16 devices in a mesh: dp: 2 (over z), sp: 8 (over y, x, core).
Axes of the slice: x: 2, y: 2, z: 2, core: 2. Of those that a mesh axis runs over, the one named last changes fastest.
Arguments:
- hidden: bfloat16 [6, 2048, 512], P('dp', 'sp')
- grad_out: bfloat16 [6, 2048, 512], P('dp', 'sp')
- ln1_gain: float32 [512], replicated
- ln1_bias: float32 [512], replicated
- ln2_gain: float32 [512], replicated
- ln2_bias: float32 [512], replicated
- w_qkv: bfloat16 [512, 8, 3, 64], replicated
- b_qkv: float32 [1536], replicated
- w_dense: bfloat16 [512, 512], replicated
- b_dense: float32 [512], replicated
- w_in: bfloat16 [512, 2048], replicated
- b_in: float32 [2048], replicated
- w_out: bfloat16 [2048, 512], replicated
- b_out: float32 [512], replicated
Outputs:
- output 1: bfloat16 [6, 2048, 512], P('dp', 'sp')
- output 2: bfloat16 [6, 2048, 512], P('dp', 'sp')
- output 3: float32 [512], P(('dp', 'sp'))
- output 4: float32 [512], P(('dp', 'sp'))
- output 5: float32 [512], P(('dp', 'sp'))
- output 6: float32 [512], P(('dp', 'sp'))
- output 7: float32 [512, 8, 3, 64], P(('dp', 'sp'))
- output 8: float32 [1536], P(('dp', 'sp'))
- output 9: float32 [512, 512], P(('dp', 'sp'))
- output 10: float32 [512], P(('dp', 'sp'))
- output 11: float32 [512, 2048], P(('dp', 'sp'))
- output 12: float32 [2048], P(('dp', 'sp'))
- output 13: float32 [2048, 512], P(('dp', 'sp'))
- output 14: float32 [512], P(('dp', 'sp'))
All inputs are finite; a program needn't handle non-finite values.
Results may differ from the reference program's by a relative error of at most 0.0105531.
Values are sent between devices in bfloat16 or wider.
A program may use at most 1 GiB of HBM per device.

```python
import math
import jax
import jax.numpy as jnp
from jax import lax

D_MODEL = 512
NUM_HEADS = 8
HEAD_DIM = 64
FF_DIM = 2048
BATCH_SIZE = 6
SEQ_LEN = 2048
ROT_DIM = HEAD_DIM // 4
QUERY_BLOCK = math.gcd(SEQ_LEN, 512)
LN_EPS = 1e-5
ROPE_BASE = 10000.0


def setup_inputs(seed: int = 0) -> dict:
    key_list = jax.random.split(jax.random.key(seed), 14)

    def normal(key_index, arr_shape, std_dev):
        return std_dev * jax.random.normal(key_list[key_index], arr_shape, jnp.float32)

    part_scale = jnp.array([0.3, 0.3, 0.05], jnp.float32)[:, None]
    return {
        'hidden': normal(0, (BATCH_SIZE, SEQ_LEN, D_MODEL), 1.0).astype(jnp.bfloat16),
        'grad_out': normal(1, (BATCH_SIZE, SEQ_LEN, D_MODEL), 1.0).astype(jnp.bfloat16),
        'ln1_gain': 1.0 + normal(2, (D_MODEL,), 0.3),
        'ln1_bias': normal(3, (D_MODEL,), 0.3),
        'ln2_gain': 1.0 + normal(4, (D_MODEL,), 0.3),
        'ln2_bias': normal(5, (D_MODEL,), 0.3),
        'w_qkv': normal(6, (D_MODEL, NUM_HEADS, 3, HEAD_DIM), 1.2 * D_MODEL ** -0.5).astype(jnp.bfloat16),
        'b_qkv': (normal(7, (NUM_HEADS, 3, HEAD_DIM), 1.0) * part_scale).reshape(3 * D_MODEL),
        'w_dense': normal(8, (D_MODEL, D_MODEL), D_MODEL ** -0.5).astype(jnp.bfloat16),
        'b_dense': normal(9, (D_MODEL,), 0.3),
        'w_in': normal(10, (D_MODEL, FF_DIM), D_MODEL ** -0.5).astype(jnp.bfloat16),
        'b_in': normal(11, (FF_DIM,), 0.3),
        'w_out': normal(12, (FF_DIM, D_MODEL), FF_DIM ** -0.5).astype(jnp.bfloat16),
        'b_out': normal(13, (D_MODEL,), 0.3),
    }


def as_bf16(tensor):
    return tensor.astype(jnp.bfloat16).astype(jnp.float32)


def layer_norm(x_f32, ln_gain, ln_shift):
    mean_val = jnp.mean(x_f32, axis=-1, keepdims=True)
    centered = x_f32 - mean_val
    var_val = jnp.mean(centered * centered, axis=-1, keepdims=True)
    return as_bf16(centered * lax.rsqrt(var_val + LN_EPS) * ln_gain + ln_shift)


def rotate(x_f32, cos_t, sin_t):
    half_rot = ROT_DIM // 2
    x_rot = x_f32[..., :ROT_DIM]
    turned = jnp.concatenate([-x_rot[..., half_rot:], x_rot[..., :half_rot]], axis=-1)
    return jnp.concatenate([x_rot * cos_t + turned * sin_t, x_f32[..., ROT_DIM:]], axis=-1)


def head_attention(q_head, k_head, v_head):
    attn_scale = 1.0 / math.sqrt(HEAD_DIM)
    key_pos = jnp.arange(SEQ_LEN)
    n_blocks = SEQ_LEN // QUERY_BLOCK

    def one_block(block_in):
        q_part, q_start = block_in
        scores = jnp.dot(q_part, k_head.T, preferred_element_type=jnp.float32) * attn_scale
        causal = key_pos[None, :] <= (q_start + jnp.arange(QUERY_BLOCK))[:, None]
        attn_prob = as_bf16(jax.nn.softmax(jnp.where(causal, scores, -1e30), axis=-1))
        return as_bf16(jnp.dot(attn_prob, v_head, preferred_element_type=jnp.float32))

    ctx_blocks = lax.map(jax.checkpoint(one_block), (q_head.reshape(n_blocks, QUERY_BLOCK, HEAD_DIM), jnp.arange(n_blocks) * QUERY_BLOCK))
    return ctx_blocks.reshape(SEQ_LEN, HEAD_DIM)


def head_entry(head_trio):
    return head_attention(head_trio[0], head_trio[1], head_trio[2])


def seq_forward(x_seq, ln1_gain, ln1_bias, ln2_gain, ln2_bias, w_qkv, b_qkv, w_dense, b_dense, w_in, b_in, w_out, b_out):
    h_attn = layer_norm(x_seq, ln1_gain, ln1_bias)
    h_mlp = layer_norm(x_seq, ln2_gain, ln2_bias)
    qkv_proj = jnp.einsum('sd,dhce->shce', h_attn, w_qkv) + b_qkv.reshape(NUM_HEADS, 3, HEAD_DIM)
    inv_freq = ROPE_BASE ** (-jnp.arange(0, ROT_DIM, 2, dtype=jnp.float32) / ROT_DIM)
    angles = jnp.arange(SEQ_LEN).astype(jnp.float32)[:, None] * inv_freq[None, :]
    angles = jnp.concatenate([angles, angles], axis=-1)[:, None, :]
    cos_t = jnp.cos(angles)
    sin_t = jnp.sin(angles)
    q_all = as_bf16(rotate(qkv_proj[:, :, 0], cos_t, sin_t))
    k_all = as_bf16(rotate(qkv_proj[:, :, 1], cos_t, sin_t))
    v_all = as_bf16(qkv_proj[:, :, 2])
    context = lax.map(jax.checkpoint(head_entry), (q_all.transpose(1, 0, 2), k_all.transpose(1, 0, 2), v_all.transpose(1, 0, 2)))
    context = context.transpose(1, 0, 2).reshape(SEQ_LEN, D_MODEL)
    attn_out = jnp.dot(context, w_dense, preferred_element_type=jnp.float32) + b_dense
    act_bf = as_bf16(jax.nn.gelu(jnp.dot(h_mlp, w_in, preferred_element_type=jnp.float32) + b_in, approximate=False))
    mlp_out = jnp.dot(act_bf, w_out, preferred_element_type=jnp.float32) + b_out
    return x_seq + attn_out + mlp_out


def reference(hidden, grad_out, ln1_gain, ln1_bias, ln2_gain, ln2_bias, w_qkv, b_qkv, w_dense, b_dense, w_in, b_in, w_out, b_out):
    params = (ln1_gain, ln1_bias, ln2_gain, ln2_bias, w_qkv.astype(jnp.float32), b_qkv, w_dense.astype(jnp.float32), b_dense, w_in.astype(jnp.float32), b_in, w_out.astype(jnp.float32), b_out)

    def one_seq(grad_acc, seq_in):
        out_seq, pullback = jax.vjp(seq_forward, seq_in[0].astype(jnp.float32), *params)
        seq_grads = pullback(seq_in[1].astype(jnp.float32))
        new_acc = tuple(acc_val + seq_val for acc_val, seq_val in zip(grad_acc, seq_grads[1:]))
        return new_acc, (out_seq.astype(jnp.bfloat16), seq_grads[0].astype(jnp.bfloat16))

    zero_acc = tuple(jnp.zeros_like(weight) for weight in params)
    grad_sums, seq_outs = lax.scan(one_seq, zero_acc, (hidden, grad_out))
    return (seq_outs[0], seq_outs[1], grad_sums[0], grad_sums[1], grad_sums[2], grad_sums[3], grad_sums[4], grad_sums[5], grad_sums[6], grad_sums[7], grad_sums[8], grad_sums[9], grad_sums[10], grad_sums[11])
```

```python
import math
import jax
import jax.numpy as jnp
from jax import lax
from jax.experimental import pallas as pl
from jax.experimental.pallas import tpu as pltpu
from jax.sharding import PartitionSpec as P

LN_EPS = 1e-5
ROPE_BASE = 10000.0
F32 = jnp.float32
BF16 = jnp.bfloat16
VMEM_LIMIT = 62 * 1024 * 1024

NB, NT, D, NH, HD, FF = 3, 256, 512, 8, 64, 2048
ROWS = NB * NT
SP = 8
SEQ = SP * NT
CHUNK = 512


def dot(a, b):
    return lax.dot_general(a, b, (((1,), (0,)), ((), ())), preferred_element_type=F32)


def dot_tb(a, b):
    return lax.dot_general(a, b, (((1,), (1,)), ((), ())), preferred_element_type=F32)


def lane_iota(rows, cols):
    return lax.broadcasted_iota(jnp.int32, (rows, cols), 1)


def row(ref):
    return ref[...].reshape(1, ref.shape[0])


def layer_hat(x):
    mean_val = jnp.mean(x, axis=-1, keepdims=True)
    centered = x - mean_val
    var_val = jnp.mean(centered * centered, axis=-1, keepdims=True)
    inv_std = lax.rsqrt(var_val + LN_EPS)
    return centered * inv_std, inv_std


def fold_weights(wt_ref, wp_ref):
    for h in range(NH):
        wp_ref[2 * HD * h:2 * HD * (h + 1), :] = wt_ref[3 * HD * h:3 * HD * h + 2 * HD, :]
        wp_ref[2 * D + HD * h:2 * D + HD * (h + 1), :] = wt_ref[3 * HD * h + 2 * HD:3 * HD * (h + 1), :]


def pair_lanes(row_qk, row_v):
    low = lane_iota(row_qk.shape[0], 128) < HD
    tiles = []
    for p in range(NH // 2):
        first = row_qk[:, 256 * p:256 * p + 128]
        second = pltpu.roll(row_qk[:, 256 * p + 128:256 * p + 256], HD, 1)
        v_pair = row_v[:, 128 * p:128 * p + 128]
        tiles += [first, jnp.where(low, v_pair, second), jnp.where(low, second, v_pair)]
    return jnp.concatenate(tiles, axis=1)


def tokens_a(x_ref, g_ref, g1_ref, s1_ref, g2_ref, s2_ref, wt_ref, bqkv_ref, wd_ref, bd_ref, wi_ref, bi_ref, wo_ref, bo_ref,
             cos_ref, sa_ref, sb_ref,
             send_ref, res_ref, dh2_ref, gwot_ref, gwi_ref, gbi_ref, small_ref,
             wp_ref, h2_ref, h2t_ref, gt_ref):
    x = x_ref[...].astype(F32)
    hat, _ = layer_hat(x)
    h1 = (hat * row(g1_ref) + row(s1_ref)).astype(BF16)
    h2_ref[...] = (hat * row(g2_ref) + row(s2_ref)).astype(BF16)
    fold_weights(wt_ref, wp_ref)

    low = lane_iota(NT, 128) < HD
    b_all = row(bqkv_ref)
    for b in range(NB):
        rows = slice(NT * b, NT * (b + 1))
        h_b = h1[rows]
        qk = dot_tb(h_b, wp_ref[:2 * D, :])
        vv = dot_tb(h_b, wp_ref[2 * D:, :])
        dc = dot_tb(g_ref[rows, :], wd_ref[...])
        for p in range(NH // 2):
            bias_a = b_all[:, 384 * p:384 * p + 128]
            bias_m = b_all[:, 384 * p + 128:384 * p + 256]
            bias_c = b_all[:, 384 * p + 256:384 * p + 384]
            low_row = low[:1]
            bias_b = pltpu.roll(jnp.where(low_row, bias_c, bias_m), HD, 1)
            bias_v = jnp.where(low_row, bias_m, bias_c)
            v_pair = vv[:, 128 * p:128 * p + 128] + bias_v
            d_pair = dc[:, 128 * p:128 * p + 128]
            v_turn = pltpu.roll(v_pair, HD, 1)
            d_turn = pltpu.roll(d_pair, HD, 1)
            for h, bias, second in ((2 * p, bias_a, jnp.where(low, v_pair, d_turn)), (2 * p + 1, bias_b, jnp.where(low, v_turn, d_pair))):
                t = qk[:, 128 * h:128 * h + 128] + bias
                t = t * cos_ref[...] + pltpu.roll(t, 120, 1) * sa_ref[...] + pltpu.roll(t, 8, 1) * sb_ref[...]
                send_ref[h, b, :, 0:128] = t.astype(BF16)
                send_ref[h, b, :, 128:256] = second.astype(BF16)

    h2t_ref[...] = h2_ref[...].T
    gt_ref[...] = g_ref[...].T
    g32 = g_ref[...].astype(F32)
    g_b_dense = jnp.sum(g32, axis=0, keepdims=True)
    res_ref[...] = x + row(bd_ref) + row(bo_ref)
    b_in = row(bi_ref)
    for c in range(FF // CHUNK):
        cols = slice(CHUNK * c, CHUNK * (c + 1))
        pre = dot(h2_ref[...], wi_ref[:, cols]) + b_in[:, cols]
        d_act = dot_tb(g_ref[...], wo_ref[cols, :])
        cdf = 0.5 * (1.0 + lax.erf(pre * math.sqrt(0.5)))
        pdf = jnp.exp(-0.5 * pre * pre) * (1.0 / math.sqrt(2.0 * math.pi))
        act = (pre * cdf).astype(BF16)
        d_pre = d_act * (cdf + pre * pdf)
        d_pre_bf = d_pre.astype(BF16)
        gbi_ref[:, cols] = jnp.broadcast_to(jnp.sum(d_pre, axis=0, keepdims=True), (8, CHUNK))
        gwot_ref[:, cols] = dot(gt_ref[...], act)
        gwi_ref[:, cols] = dot(h2t_ref[...], d_pre_bf)
        res_ref[...] += dot(act, wo_ref[cols, :])
        d_h = dot_tb(d_pre_bf, wi_ref[:, cols])
        if c == 0:
            dh2_ref[...] = d_h
        else:
            dh2_ref[...] += d_h
    d_h2 = dh2_ref[...]
    small_ref[...] = jnp.concatenate([jnp.sum(d_h2 * hat, axis=0, keepdims=True), jnp.sum(d_h2, axis=0, keepdims=True), g_b_dense, jnp.zeros((5, D), F32)], axis=0)


def heads_body(in_ref, out_ref, xt_ref, s_ref, dp_ref, acc_ref):
    scale = 1.0 / math.sqrt(HD)
    for j in range(SP):
        xt_ref[:, NT * j:NT * (j + 1)] = in_ref[j, 0].T
    low = lane_iota(NT, 128) < HD
    keep = lax.broadcasted_iota(jnp.int32, (NT, NT), 0) <= lane_iota(NT, NT)
    zero_t = jnp.zeros((HD, NT), BF16)
    for i in reversed(range(SP)):
        cols = slice(NT * i, NT * (i + 1))
        q_t = xt_ref[0:HD, cols] * BF16(scale)
        dc_t = xt_ref[3 * HD:4 * HD, cols]
        w_s = jnp.concatenate([zero_t, q_t, zero_t, zero_t], axis=0)
        w_p = jnp.concatenate([zero_t, zero_t, dc_t, zero_t], axis=0)
        w_sp = jnp.concatenate([w_s, w_p], axis=1)
        q_n = jnp.where(low, in_ref[i, 0, :, 0:128] * BF16(scale), BF16(0.0))
        dc_n = jnp.where(low, BF16(0.0), in_ref[i, 0, :, 128:256])
        w_acc = jnp.concatenate([q_n, dc_n], axis=0)
        top = None
        for j in range(i + 1):
            kv = slice(NT * j, NT * (j + 1))
            both = dot(in_ref[j, 0], w_sp)
            s = both[:, :NT]
            if j == i:
                s = jnp.where(keep, s, -1e30)
            s_ref[kv, :] = s
            dp_ref[kv, :] = both[:, NT:]
            part = jnp.max(s.reshape(NT // 8, 8, NT), axis=0)
            top = part if top is None else jnp.maximum(top, part)
        top = jnp.max(top, axis=0, keepdims=True)
        total = jnp.zeros((8, NT), F32)
        inner = jnp.zeros((8, NT), F32)
        for j in range(i + 1):
            kv = slice(NT * j, NT * (j + 1))
            e = jnp.exp(s_ref[kv, :] - top)
            s_ref[kv, :] = e
            total += jnp.sum(e.reshape(NT // 8, 8, NT), axis=0)
            inner += jnp.sum((e * dp_ref[kv, :]).reshape(NT // 8, 8, NT), axis=0)
        inv = 1.0 / jnp.sum(total, axis=0, keepdims=True)
        delta = jnp.sum(inner, axis=0, keepdims=True) * inv
        ctx_t = jnp.zeros((HD, NT), F32)
        dq_t = jnp.zeros((HD, NT), F32)
        for j in range(i + 1):
            kv = slice(NT * j, NT * (j + 1))
            prob = s_ref[kv, :] * inv
            prob_bf = prob.astype(BF16)
            ds_bf = (prob * (dp_ref[kv, :] - delta)).astype(BF16)
            ctx_t += dot(xt_ref[2 * HD:3 * HD, kv], prob_bf)
            dq_t += dot(xt_ref[HD:2 * HD, kv], ds_bf)
            step = dot(jnp.concatenate([ds_bf, prob_bf], axis=1), w_acc)
            if i == SP - 1:
                acc_ref[kv, :] = step
            else:
                acc_ref[kv, :] += step
        nat = jnp.concatenate([dq_t * scale, ctx_t], axis=0).T
        acc = acc_ref[cols, :]
        out_ref[i, 0, :, 0:128] = jnp.where(low, nat, pltpu.roll(acc, HD, 1)).astype(BF16)
        out_ref[i, 0, :, 128:256] = jnp.where(low, pltpu.roll(nat, HD, 1), acc).astype(BF16)


def tokens_b(z_ref, x_ref, g_ref, res_ref, dh2_ref, gbi_ref, small_ref, g1_ref, s1_ref, g2_ref, wt_ref, wd_ref, cos_ref, sa_ref, sb_ref,
             out_ref, gx_ref, pack_ref,
             wp_ref, ctx_ref, dqkv_ref):
    fold_weights(wt_ref, wp_ref)
    low = lane_iota(NT, 128) < HD
    gb_qk = [None] * NH
    gb_v = [None] * (NH // 2)
    for b in range(NB):
        rows = slice(NT * b, NT * (b + 1))
        for p in range(NH // 2):
            seconds = []
            for h in (2 * p, 2 * p + 1):
                t = z_ref[h, b, :, 0:128].astype(F32)
                t = t * cos_ref[...] - pltpu.roll(t, 120, 1) * sa_ref[...] - pltpu.roll(t, 8, 1) * sb_ref[...]
                part = jnp.sum(t, axis=0, keepdims=True)
                gb_qk[h] = part if b == 0 else gb_qk[h] + part
                dqkv_ref[rows, 128 * h:128 * h + 128] = t.astype(BF16)
                seconds.append(z_ref[h, b, :, 128:256].astype(F32))
            ctx_pair = jnp.where(low, seconds[0], pltpu.roll(seconds[1], HD, 1))
            dv_pair = jnp.where(low, pltpu.roll(seconds[0], HD, 1), seconds[1])
            ctx_ref[rows, 128 * p:128 * p + 128] = ctx_pair.astype(BF16)
            dqkv_ref[rows, 2 * D + 128 * p:2 * D + 128 * p + 128] = dv_pair.astype(BF16)
            part = jnp.sum(dv_pair, axis=0, keepdims=True)
            gb_v[p] = part if b == 0 else gb_v[p] + part
    out_ref[...] = (res_ref[...] + dot(ctx_ref[...], wd_ref[...])).astype(BF16)
    x = x_ref[...].astype(F32)
    hat, inv_std = layer_hat(x)
    h1_t = (hat * row(g1_ref) + row(s1_ref)).astype(BF16).T
    for k in range(3):
        g_qkv = dot(h1_t, dqkv_ref[:, D * k:D * (k + 1)])
        for q in range(16):
            pack_ref[q, 32 * k:32 * k + 32, :] = g_qkv[32 * q:32 * q + 32]
    g_dense = dot(ctx_ref[...].T, g_ref[...])
    for q in range(16):
        pack_ref[q, 96:128, :] = g_dense[32 * q:32 * q + 32]
    d_h1 = dot(dqkv_ref[...], wp_ref[...])
    g_ln1 = jnp.sum(d_h1 * hat, axis=0, keepdims=True)
    g_ln1_b = jnp.sum(d_h1, axis=0, keepdims=True)
    d_hat = d_h1 * row(g1_ref) + dh2_ref[...] * row(g2_ref)
    d_x = inv_std * (d_hat - jnp.mean(d_hat, axis=-1, keepdims=True) - hat * jnp.mean(d_hat * hat, axis=-1, keepdims=True))
    gx_ref[...] = (g_ref[...].astype(F32) + d_x).astype(BF16)

    five = jnp.concatenate([g_ln1, g_ln1_b, small_ref[...][0:3], jnp.zeros((3, D), F32)], axis=0)
    g_bqkv = jnp.broadcast_to(pair_lanes(jnp.concatenate(gb_qk, axis=1), jnp.concatenate(gb_v, axis=1)), (8, 3 * D))
    for q in range(16):
        part = pltpu.roll(five, (D - 32 * q) % D, 1)[:, 0:128] if q else five[:, 0:128]
        bq = pltpu.roll(g_bqkv, (3 * D - 96 * q) % (3 * D), 1)[:, 0:128] if q else g_bqkv[:, 0:128]
        pack_ref[q, 128:136, 0:128] = part
        pack_ref[q, 128:136, 128:256] = gbi_ref[:, 128 * q:128 * q + 128]
        pack_ref[q, 128:136, 256:384] = bq
        pack_ref[q, 128:136, 384:512] = jnp.zeros((8, 128), F32)


def sds(shape, dtype):
    return jax.ShapeDtypeStruct(shape, dtype)


def vmem_specs(count):
    return [pl.BlockSpec(memory_space=pltpu.VMEM)] * count


def solution(mesh):
    grad_axes = ('dp', 'sp')

    def device_step(hidden, grad_out, ln1_gain, ln1_bias, ln2_gain, ln2_bias, w_qkv, b_qkv, w_dense, b_dense, w_in, b_in, w_out, b_out):
        x = hidden.reshape(ROWS, D)
        g = grad_out.reshape(ROWS, D)
        wt = jnp.transpose(w_qkv, (1, 2, 3, 0)).reshape(3 * D, D)
        rot = HD // 4
        half = rot // 2
        lane = jnp.arange(128)
        in_head = lane % HD
        inv_freq = ROPE_BASE ** (-(2.0 * (in_head % half)).astype(F32) / rot)
        pos = (lax.axis_index('sp') * NT + jnp.arange(NT)).astype(F32)
        angles = pos[:, None] * inv_freq[None, :]
        cos_t = jnp.where(in_head[None, :] < rot, jnp.cos(angles), 1.0)
        sin_t = jnp.sin(angles)
        sin_a = jnp.where(in_head[None, :] < half, -sin_t, 0.0)
        sin_b = jnp.where((in_head[None, :] >= half) & (in_head[None, :] < rot), sin_t, 0.0)

        send, res, dh2, gwot, gwi, gbi, small = pl.pallas_call(
            tokens_a,
            out_shape=(sds((SP, NB, NT, 256), BF16), sds((ROWS, D), F32), sds((ROWS, D), F32), sds((D, FF), F32), sds((D, FF), F32), sds((8, FF), F32), sds((8, D), F32)),
            in_specs=vmem_specs(17),
            out_specs=tuple(vmem_specs(7)),
            scratch_shapes=[pltpu.VMEM((3 * D, D), BF16), pltpu.VMEM((ROWS, D), BF16), pltpu.VMEM((D, ROWS), BF16), pltpu.VMEM((D, ROWS), BF16)],
            compiler_params=pltpu.CompilerParams(vmem_limit_bytes=VMEM_LIMIT),
            cost_estimate=pl.CostEstimate(flops=12_000_000_000, bytes_accessed=22_000_000, transcendentals=3_000_000),
            name='tokens_a',
        )(x, g, ln1_gain, ln1_bias, ln2_gain, ln2_bias, wt, b_qkv, w_dense, b_dense, w_in, b_in, w_out, b_out, cos_t, sin_a, sin_b)

        heads = lax.all_to_all(send, 'sp', 0, 0, tiled=True)
        block = pl.BlockSpec((SP, 1, NT, 256), lambda b: (0, b, 0, 0))
        back = pl.pallas_call(
            heads_body,
            grid=(NB,),
            out_shape=sds((SP, NB, NT, 256), BF16),
            in_specs=[block],
            out_specs=block,
            scratch_shapes=[pltpu.VMEM((256, SEQ), BF16), pltpu.VMEM((SEQ, NT), F32), pltpu.VMEM((SEQ, NT), F32), pltpu.VMEM((SEQ, 128), F32)],
            compiler_params=pltpu.CompilerParams(vmem_limit_bytes=40 * 1024 * 1024),
            cost_estimate=pl.CostEstimate(flops=40_000_000_000, bytes_accessed=6_400_000, transcendentals=7_000_000),
            name='heads',
        )(heads)
        tok = lax.all_to_all(back, 'sp', 0, 0, tiled=True)

        g_wot = lax.psum_scatter(gwot.reshape(D, FF // 128, 128).transpose(1, 0, 2), grad_axes, scatter_dimension=0, tiled=True)
        g_wi = lax.psum_scatter(gwi, grad_axes, scatter_dimension=0, tiled=True)

        out, gx, pack = pl.pallas_call(
            tokens_b,
            out_shape=(sds((ROWS, D), BF16), sds((ROWS, D), BF16), sds((16, 136, D), F32)),
            in_specs=vmem_specs(15),
            out_specs=tuple(vmem_specs(3)),
            scratch_shapes=[pltpu.VMEM((3 * D, D), BF16), pltpu.VMEM((ROWS, D), BF16), pltpu.VMEM((ROWS, 3 * D), BF16)],
            compiler_params=pltpu.CompilerParams(vmem_limit_bytes=VMEM_LIMIT),
            cost_estimate=pl.CostEstimate(flops=4_000_000_000, bytes_accessed=20_000_000, transcendentals=0),
            name='tokens_b',
        )(tok, x, g, res, dh2, gbi, small, ln1_gain, ln1_bias, ln2_gain, wt, w_dense, cos_t, sin_a, sin_b)

        mine = lax.psum_scatter(pack.reshape(16 * 136, D), grad_axes, scatter_dimension=0, tiled=True)
        qkv = jnp.concatenate([mine[0:32], mine[32:64], mine[64:96]], axis=1)
        g_qk = qkv[:, :2 * D].reshape(32, NH, 2, HD)
        g_v = qkv[:, 2 * D:].reshape(32, NH, 1, HD)
        g_w_qkv = jnp.concatenate([g_qk, g_v], axis=2)
        tail = mine[128:136]
        return (out.reshape(hidden.shape), gx.reshape(hidden.shape), tail[0, 0:32], tail[1, 0:32], tail[2, 0:32], tail[3, 0:32], g_w_qkv,
                tail[0, 256:352], mine[96:128], tail[4, 0:32], g_wi, tail[0, 128:256], g_wot[0].T, tail[4, 0:32])

    tok_spec = P('dp', 'sp', None)
    grad_spec = P(grad_axes)
    return jax.shard_map(device_step, mesh=mesh, in_specs=(tok_spec, tok_spec) + (P(),) * 12, out_specs=(tok_spec, tok_spec) + (grad_spec,) * 12, check_vma=False)
```

```python
import math
import jax
import jax.numpy as jnp
from jax import lax
from jax.experimental import pallas as pl
from jax.experimental.pallas import tpu as pltpu
from jax.sharding import PartitionSpec as P

LN_EPS = 1e-5
ROPE_BASE = 10000.0
F32 = jnp.float32
BF16 = jnp.bfloat16
VMEM_LIMIT = 67_043_328
MESH = pl.DeviceIdType.MESH

NB, NT, D, NH, HD, FF = 3, 256, 512, 8, 64, 2048
ROWS = NB * NT
SP = 8
SEQ = SP * NT
CHUNK = 512


def dot(a, b):
    return lax.dot_general(a, b, (((1,), (0,)), ((), ())), preferred_element_type=F32)


def dot_tb(a, b):
    return lax.dot_general(a, b, (((1,), (1,)), ((), ())), preferred_element_type=F32)


def lane_iota(rows, cols):
    return lax.broadcasted_iota(jnp.int32, (rows, cols), 1)


def row(ref):
    return ref[...].reshape(1, ref.shape[0])


def layer_hat(x):
    mean_val = jnp.mean(x, axis=-1, keepdims=True)
    centered = x - mean_val
    var_val = jnp.mean(centered * centered, axis=-1, keepdims=True)
    inv_std = lax.rsqrt(var_val + LN_EPS)
    return centered * inv_std, inv_std


def fold_weights(wt_ref, wp_ref):
    for h in range(NH):
        wp_ref[2 * HD * h:2 * HD * (h + 1), :] = wt_ref[3 * HD * h:3 * HD * h + 2 * HD, :]
        wp_ref[2 * D + HD * h:2 * D + HD * (h + 1), :] = wt_ref[3 * HD * h + 2 * HD:3 * HD * (h + 1), :]


def pair_lanes(row_qk, row_v):
    low = lane_iota(row_qk.shape[0], 128) < HD
    tiles = []
    for p in range(NH // 2):
        first = row_qk[:, 256 * p:256 * p + 128]
        second = pltpu.roll(row_qk[:, 256 * p + 128:256 * p + 256], HD, 1)
        v_pair = row_v[:, 128 * p:128 * p + 128]
        tiles += [first, jnp.where(low, v_pair, second), jnp.where(low, second, v_pair)]
    return jnp.concatenate(tiles, axis=1)


def part_bits(p):
    return p % 2, p // 8, (p // 2) % 2, (p // 4) % 2


class Where:
    def __init__(self):
        self.z = lax.axis_index('dp')
        self.me = lax.axis_index('sp')
        self.bit = {'c': self.me % 2, 'x': (self.me // 2) % 2, 'y': self.me // 4, 'z': self.z}

    def flip(self, names):
        step = {'c': 1, 'x': 2, 'y': 4}
        sp = self.me
        z = self.z
        for n in names:
            if n == 'z':
                z = 1 - z
            else:
                sp = sp + step[n] * (1 - 2 * self.bit[n])
        return z, sp


class Summed:
    def __init__(self, at, order, buf, lands, send_sem, recv_sem):
        self.at, self.order, self.buf, self.lands, self.send_sem, self.recv_sem = at, order, buf, lands, send_sem, recv_sem

    def copy(self, k):
        mine = [self.at.bit[n] for n in self.order]
        index = tuple(mine[:k]) + (1 - mine[k],)
        z, sp = self.at.flip(self.order[k])
        return pltpu.make_async_remote_copy(src_ref=self.buf.at[index], dst_ref=self.lands[k], send_sem=self.send_sem.at[k], recv_sem=self.recv_sem.at[k],
                                            device_id=(z, sp), device_id_type=MESH)

    def start(self, k):
        self.copy(k).start()

    def land(self, k):
        self.copy(k).wait_recv()
        mine = tuple(self.at.bit[n] for n in self.order[:k + 1])
        rest = 3 - k
        for n in range(2 ** rest):
            sub = tuple((n >> (rest - 1 - m)) % 2 for m in range(rest))
            full = mine + sub
            self.buf[full] = self.buf[full] + self.lands[k][sub if sub else ...]

    def result(self):
        return self.buf[tuple(self.at.bit[n] for n in self.order)]

    def drain(self):
        for k in range(4):
            self.copy(k).wait_send()


PEERS = ('x', 'y', 'xy', 'xc', 'yc', 'xyc', 'c')


def exchange(at, b, src, dst, send_sem, recv_sem):
    out = []
    for k, names in enumerate(PEERS):
        z, sp = at.flip(names)
        out.append(pltpu.make_async_remote_copy(src_ref=src.at[b, sp], dst_ref=dst.at[b, at.me], send_sem=send_sem.at[b, k], recv_sem=recv_sem.at[b, k],
                                                device_id=(z, sp), device_id_type=MESH))
    return out


def layer(x_ref, g_ref, g1_ref, s1_ref, g2_ref, s2_ref, wt_ref, bqkv_ref, wd_ref, bd_ref, wi_ref, bi_ref, wo_ref, bo_ref, cos_ref, sa_ref, sb_ref,
          out_ref, gx_ref, gwi_ref, gwo_ref, gqkv_ref, gwd_ref, tail_ref,
          wp_ref, ctx_ref, dqkv_ref, h2t_ref, gt_ref, buf_ref, in_ref, z_ref, res_ref, dh2_ref, gbi_ref,
          xt_ref, sdp_ref, acc_ref,
          wi_buf, wi_c, wi_1, wi_2, wi_3, wo_buf, wo_c, wo_1, wo_2, wo_3,
          t0_buf, t0_c, t0_1, t0_2, t0_3, t1_buf, t1_c, t1_1, t1_2, t1_3, t2_buf, t2_c, t2_1, t2_2, t2_3,
          s1_sem, r1_sem, s2_sem, r2_sem, sum_send, sum_recv):
    at = Where()
    me = at.me
    sum_wi = Summed(at, 'czxy', wi_buf, (wi_c, wi_1, wi_2, wi_3), sum_send.at[0], sum_recv.at[0])
    sum_wo = Summed(at, 'czyx', wo_buf, (wo_c, wo_1, wo_2, wo_3), sum_send.at[1], sum_recv.at[1])
    sum_t = (Summed(at, 'czxy', t0_buf, (t0_c, t0_1, t0_2, t0_3), sum_send.at[2], sum_recv.at[2]),
             Summed(at, 'cxyz', t1_buf, (t1_c, t1_1, t1_2, t1_3), sum_send.at[3], sum_recv.at[3]),
             Summed(at, 'cyzx', t2_buf, (t2_c, t2_1, t2_2, t2_3), sum_send.at[4], sum_recv.at[4]))
    low = lane_iota(NT, 128) < HD
    fold_weights(wt_ref, wp_ref)
    b_all = row(bqkv_ref)

    for b in range(NB):
        rows = slice(NT * b, NT * (b + 1))
        x = x_ref[rows, :].astype(F32)
        hat, _ = layer_hat(x)
        h_b = (hat * row(g1_ref) + row(s1_ref)).astype(BF16)
        ctx_ref[rows, :] = (hat * row(g2_ref) + row(s2_ref)).astype(BF16)
        res_ref[rows, :] = x + row(bd_ref) + row(bo_ref)
        qk = dot_tb(h_b, wp_ref[:2 * D, :])
        vv = dot_tb(h_b, wp_ref[2 * D:, :])
        dc = dot_tb(g_ref[rows, :], wd_ref[...])
        for p in range(NH // 2):
            bias_a = b_all[:, 384 * p:384 * p + 128]
            bias_m = b_all[:, 384 * p + 128:384 * p + 256]
            bias_c = b_all[:, 384 * p + 256:384 * p + 384]
            low_row = low[:1]
            bias_b = pltpu.roll(jnp.where(low_row, bias_c, bias_m), HD, 1)
            bias_v = jnp.where(low_row, bias_m, bias_c)
            v_pair = vv[:, 128 * p:128 * p + 128] + bias_v
            d_pair = dc[:, 128 * p:128 * p + 128]
            v_turn = pltpu.roll(v_pair, HD, 1)
            d_turn = pltpu.roll(d_pair, HD, 1)
            for h, bias, second in ((2 * p, bias_a, jnp.where(low, v_pair, d_turn)), (2 * p + 1, bias_b, jnp.where(low, v_turn, d_pair))):
                t = qk[:, 128 * h:128 * h + 128] + bias
                t = t * cos_ref[...] + pltpu.roll(t, 120, 1) * sa_ref[...] + pltpu.roll(t, 8, 1) * sb_ref[...]
                buf_ref[b, h, :, 0:128] = t.astype(BF16)
                buf_ref[b, h, :, 128:256] = second.astype(BF16)
        if b == 0:
            barrier = pltpu.get_barrier_semaphore()
            for names in PEERS + ('z',):
                pl.semaphore_signal(barrier, inc=1, device_id=at.flip(names), device_id_type=MESH)
            pl.semaphore_wait(barrier, len(PEERS) + 1)
        for copy in exchange(at, b, buf_ref, in_ref, s1_sem, r1_sem):
            copy.start()
        in_ref[b, me] = buf_ref[b, me]

    h2t_ref[...] = ctx_ref[...].T
    gt_ref[...] = g_ref[...].T
    b_in = row(bi_ref)
    for c in range(FF // CHUNK):
        cols = slice(CHUNK * c, CHUNK * (c + 1))
        pre = dot(ctx_ref[...], wi_ref[:, cols]) + b_in[:, cols]
        d_act = dot_tb(g_ref[...], wo_ref[cols, :])
        cdf = 0.5 * (1.0 + lax.erf(pre * math.sqrt(0.5)))
        pdf = jnp.exp(-0.5 * pre * pre) * (1.0 / math.sqrt(2.0 * math.pi))
        act = (pre * cdf).astype(BF16)
        d_pre = d_act * (cdf + pre * pdf)
        d_pre_bf = d_pre.astype(BF16)
        gbi_ref[:, cols] = jnp.broadcast_to(jnp.sum(d_pre, axis=0, keepdims=True), (8, CHUNK))
        g_wo = dot(gt_ref[...], act)
        g_wi = dot(h2t_ref[...], d_pre_bf)
        for p in range(16):
            cc, zz, xx, yy = part_bits(p)
            wi_buf[cc, zz, xx, yy, 32 * c:32 * c + 32, :] = g_wi[32 * p:32 * p + 32]
        for q in range(4):
            cc, zz, xx, yy = part_bits(4 * c + q)
            for k in range(4):
                wo_buf[cc, zz, yy, xx, :, 128 * k:128 * k + 128] = g_wo[128 * k:128 * k + 128, 128 * q:128 * q + 128]
        res_ref[...] += dot(act, wo_ref[cols, :])
        d_h = dot_tb(d_pre_bf, wi_ref[:, cols])
        if c == 0:
            dh2_ref[...] = d_h
        else:
            dh2_ref[...] += d_h
    sum_wi.start(0)
    sum_wo.start(0)
    g_ln2 = jnp.zeros((1, D), F32)
    g_ln2_b = jnp.zeros((1, D), F32)
    g_b_dense = jnp.zeros((1, D), F32)
    for b in range(NB):
        rows = slice(NT * b, NT * (b + 1))
        hat, _ = layer_hat(x_ref[rows, :].astype(F32))
        d_h = dh2_ref[rows, :]
        g_ln2 += jnp.sum(d_h * hat, axis=0, keepdims=True)
        g_ln2_b += jnp.sum(d_h, axis=0, keepdims=True)
        g_b_dense += jnp.sum(g_ref[rows, :].astype(F32), axis=0, keepdims=True)
        dh2_ref[rows, :] = d_h * row(g2_ref)

    scale = 1.0 / math.sqrt(HD)
    keep = lax.broadcasted_iota(jnp.int32, (NT, NT), 0) <= lane_iota(NT, NT)
    zero_t = jnp.zeros((HD, NT), BF16)

    def one_sequence(b, carry):
        for copy in exchange(at, b, buf_ref, in_ref, s1_sem, r1_sem):
            copy.wait()
        for j in range(SP):
            xt_ref[:, NT * j:NT * (j + 1)] = in_ref[b, j].T
        for i in reversed(range(SP)):
            cols = slice(NT * i, NT * (i + 1))
            q_t = xt_ref[0:HD, cols] * BF16(scale)
            dc_t = xt_ref[3 * HD:4 * HD, cols]
            w_s = jnp.concatenate([zero_t, q_t, zero_t, zero_t], axis=0)
            w_p = jnp.concatenate([zero_t, zero_t, dc_t, zero_t], axis=0)
            w_sp = jnp.concatenate([w_s, w_p], axis=1)
            q_n = jnp.where(low, in_ref[b, i, :, 0:128] * BF16(scale), BF16(0.0))
            dc_n = jnp.where(low, BF16(0.0), in_ref[b, i, :, 128:256])
            w_acc = jnp.concatenate([q_n, dc_n], axis=0)
            top = None
            for j in range(i + 1):
                kv = slice(NT * j, NT * (j + 1))
                both = dot(in_ref[b, j], w_sp)
                s = both[:, :NT]
                if j == i:
                    s = jnp.where(keep, s, -1e30)
                sdp_ref[kv, 0:NT] = s
                sdp_ref[kv, NT:2 * NT] = both[:, NT:]
                part = jnp.max(s.reshape(NT // 8, 8, NT), axis=0)
                top = part if top is None else jnp.maximum(top, part)
            top = jnp.max(top, axis=0, keepdims=True)
            total = jnp.zeros((8, NT), F32)
            inner = jnp.zeros((8, NT), F32)
            for j in range(i + 1):
                kv = slice(NT * j, NT * (j + 1))
                e = jnp.exp(sdp_ref[kv, 0:NT] - top)
                sdp_ref[kv, 0:NT] = e
                total += jnp.sum(e.reshape(NT // 8, 8, NT), axis=0)
                inner += jnp.sum((e * sdp_ref[kv, NT:2 * NT]).reshape(NT // 8, 8, NT), axis=0)
            inv = 1.0 / jnp.sum(total, axis=0, keepdims=True)
            delta = jnp.sum(inner, axis=0, keepdims=True) * inv
            ctx_t = jnp.zeros((HD, NT), F32)
            dq_t = jnp.zeros((HD, NT), F32)
            for j in range(i + 1):
                kv = slice(NT * j, NT * (j + 1))
                prob = sdp_ref[kv, 0:NT] * inv
                prob_bf = prob.astype(BF16)
                ds_bf = (prob * (sdp_ref[kv, NT:2 * NT] - delta)).astype(BF16)
                ctx_t += dot(xt_ref[2 * HD:3 * HD, kv], prob_bf)
                dq_t += dot(xt_ref[HD:2 * HD, kv], ds_bf)
                step = dot(jnp.concatenate([ds_bf, prob_bf], axis=1), w_acc)
                if i == SP - 1:
                    acc_ref[kv, :] = step
                else:
                    acc_ref[kv, :] += step
            nat = jnp.concatenate([dq_t * scale, ctx_t], axis=0).T
            acc = acc_ref[cols, :]
            buf_ref[b, i, :, 0:128] = jnp.where(low, nat, pltpu.roll(acc, HD, 1)).astype(BF16)
            buf_ref[b, i, :, 128:256] = jnp.where(low, pltpu.roll(nat, HD, 1), acc).astype(BF16)
        for copy in exchange(at, b, buf_ref, z_ref, s2_sem, r2_sem):
            copy.start()
        z_ref[b, me] = buf_ref[b, me]

        @pl.when(b == 0)
        def _():
            for s in (sum_wi, sum_wo):
                s.land(0)
                s.start(1)
        return carry

    lax.fori_loop(0, NB, one_sequence, 0)

    g_ln1 = jnp.zeros((1, D), F32)
    g_ln1_b = jnp.zeros((1, D), F32)
    gb_qk = [None] * NH
    gb_v = [None] * (NH // 2)
    for b in range(NB):
        rows = slice(NT * b, NT * (b + 1))
        for copy in exchange(at, b, buf_ref, z_ref, s2_sem, r2_sem):
            copy.wait()
        for p in range(NH // 2):
            seconds = []
            for h in (2 * p, 2 * p + 1):
                t = z_ref[b, h, :, 0:128].astype(F32)
                t = t * cos_ref[...] - pltpu.roll(t, 120, 1) * sa_ref[...] - pltpu.roll(t, 8, 1) * sb_ref[...]
                part = jnp.sum(t, axis=0, keepdims=True)
                gb_qk[h] = part if b == 0 else gb_qk[h] + part
                dqkv_ref[rows, 128 * h:128 * h + 128] = t.astype(BF16)
                seconds.append(z_ref[b, h, :, 128:256].astype(F32))
            ctx_pair = jnp.where(low, seconds[0], pltpu.roll(seconds[1], HD, 1))
            dv_pair = jnp.where(low, pltpu.roll(seconds[0], HD, 1), seconds[1])
            ctx_ref[rows, 128 * p:128 * p + 128] = ctx_pair.astype(BF16)
            dqkv_ref[rows, 2 * D + 128 * p:2 * D + 128 * p + 128] = dv_pair.astype(BF16)
            part = jnp.sum(dv_pair, axis=0, keepdims=True)
            gb_v[p] = part if b == 0 else gb_v[p] + part
        out_ref[rows, :] = (res_ref[rows, :] + dot(ctx_ref[rows, :], wd_ref[...])).astype(BF16)
        hat, inv_std = layer_hat(x_ref[rows, :].astype(F32))
        h2t_ref[:, rows] = (hat * row(g1_ref) + row(s1_ref)).astype(BF16).T
        d_h1 = dot(dqkv_ref[rows, :], wp_ref[...])
        g_ln1 += jnp.sum(d_h1 * hat, axis=0, keepdims=True)
        g_ln1_b += jnp.sum(d_h1, axis=0, keepdims=True)
        d_hat = d_h1 * row(g1_ref) + dh2_ref[rows, :]
        d_x = inv_std * (d_hat - jnp.mean(d_hat, axis=-1, keepdims=True) - hat * jnp.mean(d_hat * hat, axis=-1, keepdims=True))
        gx_ref[rows, :] = (g_ref[rows, :].astype(F32) + d_x).astype(BF16)

    g_q = [dot(h2t_ref[...], dqkv_ref[:, D * k:D * (k + 1)]) for k in range(3)]
    g_dense = dot(ctx_ref[...].T, g_ref[...])
    five = jnp.concatenate([g_ln1, g_ln1_b, g_ln2, g_ln2_b, g_b_dense, jnp.zeros((3, D), F32)], axis=0)
    g_bqkv = jnp.broadcast_to(pair_lanes(jnp.concatenate(gb_qk, axis=1), jnp.concatenate(gb_v, axis=1)), (8, 3 * D))
    for p in range(16):
        cc, zz, xx, yy = part_bits(p)
        d0 = 32 * p
        t0_buf[cc, zz, xx, yy, 0:32, :] = g_q[0][d0:d0 + 32]
        t0_buf[cc, zz, xx, yy, 32:48, :] = g_q[1][d0:d0 + 16]
        t1_buf[cc, xx, yy, zz, 0:16, :] = g_q[1][d0 + 16:d0 + 32]
        t1_buf[cc, xx, yy, zz, 16:48, :] = g_q[2][d0:d0 + 32]
        t2_buf[cc, yy, zz, xx, 0:32, :] = g_dense[d0:d0 + 32]
        t2_buf[cc, yy, zz, xx, 32:40, 0:128] = pltpu.roll(five, (D - 32 * p) % D, 1)[:, 0:128] if p else five[:, 0:128]
        t2_buf[cc, yy, zz, xx, 32:40, 128:256] = gbi_ref[:, 128 * p:128 * p + 128]
        t2_buf[cc, yy, zz, xx, 32:40, 256:384] = pltpu.roll(g_bqkv, (3 * D - 96 * p) % (3 * D), 1)[:, 0:128] if p else g_bqkv[:, 0:128]
        t2_buf[cc, yy, zz, xx, 32:40, 384:512] = jnp.zeros((8, 128), F32)

    for s in sum_t:
        s.start(0)
    for s in (sum_wi, sum_wo):
        s.land(1)
        s.start(2)
    for k in range(3):
        for s in sum_t:
            s.land(k)
            s.start(k + 1)
        if k == 0:
            for s in (sum_wi, sum_wo):
                s.land(2)
                s.start(3)
        if k == 1:
            for s in (sum_wi, sum_wo):
                s.land(3)
    g_wi = sum_wi.result()
    for c in range(FF // CHUNK):
        gwi_ref[:, CHUNK * c:CHUNK * (c + 1)] = g_wi[32 * c:32 * c + 32]
    g_wo = sum_wo.result()
    for k in range(4):
        gwo_ref[:, 128 * k:128 * k + 128] = g_wo[:, 128 * k:128 * k + 128].T
    for s in sum_t:
        s.land(3)
    first, second, third = (s.result() for s in sum_t)
    gqkv_ref[:, 0:D] = first[0:32]
    gqkv_ref[0:16, D:2 * D] = first[32:48]
    gqkv_ref[16:32, D:2 * D] = second[0:16]
    gqkv_ref[:, 2 * D:3 * D] = second[16:48]
    gwd_ref[...] = third[0:32]
    tail_ref[...] = third[32:40]
    for s in (sum_wi, sum_wo) + sum_t:
        s.drain()


def sds(shape, dtype):
    return jax.ShapeDtypeStruct(shape, dtype)


def halving(rows):
    return [pltpu.VMEM((2,) * n + (rows, D), F32) for n in (4, 3, 2, 1, 0)]


def solution(mesh):
    grad_axes = ('dp', 'sp')

    def device_step(hidden, grad_out, ln1_gain, ln1_bias, ln2_gain, ln2_bias, w_qkv, b_qkv, w_dense, b_dense, w_in, b_in, w_out, b_out):
        x = hidden.reshape(ROWS, D)
        g = grad_out.reshape(ROWS, D)
        wt = jnp.transpose(w_qkv, (1, 2, 3, 0)).reshape(3 * D, D)
        rot = HD // 4
        half = rot // 2
        lane = jnp.arange(128)
        in_head = lane % HD
        inv_freq = ROPE_BASE ** (-(2.0 * (in_head % half)).astype(F32) / rot)
        pos = (lax.axis_index('sp') * NT + jnp.arange(NT)).astype(F32)
        angles = pos[:, None] * inv_freq[None, :]
        cos_t = jnp.where(in_head[None, :] < rot, jnp.cos(angles), 1.0)
        sin_t = jnp.sin(angles)
        sin_a = jnp.where(in_head[None, :] < half, -sin_t, 0.0)
        sin_b = jnp.where((in_head[None, :] >= half) & (in_head[None, :] < rot), sin_t, 0.0)

        dma = pltpu.SemaphoreType.DMA
        out, gx, g_wi, g_wo, qkv, g_wd, tail = pl.pallas_call(
            layer,
            out_shape=(sds((ROWS, D), BF16), sds((ROWS, D), BF16), sds((32, FF), F32), sds((128, D), F32), sds((32, 3 * D), F32), sds((32, D), F32), sds((8, D), F32)),
            in_specs=[pl.BlockSpec(memory_space=pltpu.VMEM)] * 17,
            out_specs=(pl.BlockSpec(memory_space=pltpu.VMEM),) * 7,
            scratch_shapes=[
                pltpu.VMEM((3 * D, D), BF16), pltpu.VMEM((ROWS, D), BF16), pltpu.VMEM((ROWS, 3 * D), BF16), pltpu.VMEM((D, ROWS), BF16), pltpu.VMEM((D, ROWS), BF16),
                pltpu.VMEM((NB, SP, NT, 256), BF16), pltpu.VMEM((NB, SP, NT, 256), BF16), pltpu.VMEM((NB, SP, NT, 256), BF16),
                pltpu.VMEM((ROWS, D), F32), pltpu.VMEM((ROWS, D), F32), pltpu.VMEM((8, FF), F32),
                pltpu.VMEM((256, SEQ), BF16), pltpu.VMEM((SEQ, 2 * NT), F32), pltpu.VMEM((SEQ, 128), F32),
                *halving(128), *halving(128), *halving(48), *halving(48), *halving(40),
                dma((NB, 7)), dma((NB, 7)), dma((NB, 7)), dma((NB, 7)), dma((5, 4)), dma((5, 4)),
            ],
            compiler_params=pltpu.CompilerParams(vmem_limit_bytes=VMEM_LIMIT, collective_id=0, has_side_effects=True),
            cost_estimate=pl.CostEstimate(flops=56_000_000_000, bytes_accessed=12_000_000, transcendentals=10_000_000),
            name='layer',
        )(x, g, ln1_gain, ln1_bias, ln2_gain, ln2_bias, wt, b_qkv, w_dense, b_dense, w_in, b_in, w_out, b_out, cos_t, sin_a, sin_b)

        g_qk = qkv[:, :2 * D].reshape(32, NH, 2, HD)
        g_v = qkv[:, 2 * D:].reshape(32, NH, 1, HD)
        g_w_qkv = jnp.concatenate([g_qk, g_v], axis=2)
        return (out.reshape(hidden.shape), gx.reshape(hidden.shape), tail[0, 0:32], tail[1, 0:32], tail[2, 0:32], tail[3, 0:32], g_w_qkv,
                tail[0, 256:352], g_wd, tail[4, 0:32], g_wi, tail[0, 128:256], g_wo, tail[4, 0:32])

    tok_spec = P('dp', 'sp', None)
    grad_spec = P(grad_axes)
    return jax.shard_map(device_step, mesh=mesh, in_specs=(tok_spec, tok_spec) + (P(),) * 12, out_specs=(tok_spec, tok_spec) + (grad_spec,) * 12, check_vma=False)
```

```python
import math
import jax
import jax.numpy as jnp
from jax import lax
from jax.experimental import pallas as pl
from jax.experimental.pallas import tpu as pltpu
from jax.sharding import PartitionSpec as P

LN_EPS = 1e-5
ROPE_BASE = 10000.0
F32 = jnp.float32
BF16 = jnp.bfloat16
MESH = pl.DeviceIdType.MESH
VMEM_LIMIT = 67_043_328

NB, NT, D, NH, HD, FF = 3, 256, 512, 8, 64, 2048
ROWS = NB * NT
SP = 8
PARTS = 16
SEQ = SP * NT
CHUNK = 512
N_CHUNK = FF // CHUNK
SUB = 8
LANES = 2 * HD
PAIRS = NH // 2
SLICE = D // PARTS
HALF = SLICE // 2
QKV = 3 * D
ROT = HD // 4
TURN = ROT // 2
TURN_BACK = LANES - TURN
LO = slice(0, LANES)
HI = slice(LANES, 2 * LANES)
SCALE = 1.0 / math.sqrt(HD)


def dot(a, b):
    return lax.dot_general(a, b, (((1,), (0,)), ((), ())), preferred_element_type=F32)


def dot_tb(a, b):
    return lax.dot_general(a, b, (((1,), (1,)), ((), ())), preferred_element_type=F32)


def span(index, size):
    return slice(size * index, size * (index + 1))


def lane_iota(rows, cols):
    return lax.broadcasted_iota(jnp.int32, (rows, cols), 1)


def swap(x):
    return pltpu.roll(x, HD, 1)


def row(ref):
    return ref[...].reshape(1, ref.shape[0])


def col_sum(x):
    return jnp.sum(x, axis=0, keepdims=True)


def fold(x, op):
    return op(x.reshape(NT // SUB, SUB, NT), axis=0)


def layer_hat(x):
    mean_val = jnp.mean(x, axis=-1, keepdims=True)
    centered = x - mean_val
    var_val = jnp.mean(centered * centered, axis=-1, keepdims=True)
    inv_std = lax.rsqrt(var_val + LN_EPS)
    return centered * inv_std, inv_std


def fold_weights(wt_ref, wp_ref):
    for h in range(NH):
        base = 3 * HD * h
        wp_ref[span(h, LANES), :] = wt_ref[base:base + LANES, :]
        wp_ref[span(2 * NH + h, HD), :] = wt_ref[base + LANES:base + LANES + HD, :]


def pair_lanes(row_qk, row_v):
    low = lane_iota(1, LANES) < HD
    tiles = []
    for p in range(PAIRS):
        second = swap(row_qk[:, span(2 * p + 1, LANES)])
        v_pair = row_v[:, span(p, LANES)]
        tiles += [row_qk[:, span(2 * p, LANES)], jnp.where(low, v_pair, second), jnp.where(low, second, v_pair)]
    return jnp.concatenate(tiles, axis=1)


def pair_bias(b_all, p):
    low = lane_iota(1, LANES) < HD
    first, mid, last = (b_all[:, span(3 * p + n, LANES)] for n in range(3))
    return first, swap(jnp.where(low, last, mid)), jnp.where(low, mid, last)


def cut(x, shift):
    width = x.shape[1]
    return pltpu.roll(x, (width - shift) % width, 1)[:, LO]


def part_bits(p):
    return {'c': p % 2, 'x': p // 2 % 2, 'y': p // 4 % 2, 'z': p // 8}


class Where:
    def __init__(self):
        self.z = lax.axis_index('dp')
        self.me = lax.axis_index('sp')
        self.bit = part_bits(self.z * SP + self.me)

    def flip(self, names):
        step = {'c': 1, 'x': 2, 'y': 4}
        z, sp = self.z, self.me
        for n in names:
            if n == 'z':
                z = 1 - z
            else:
                sp = sp + step[n] * (1 - 2 * self.bit[n])
        return z, sp


class Summed:
    def __init__(self, at, order, refs, send_sem, recv_sem):
        self.at, self.order, self.buf, self.lands, self.send_sem, self.recv_sem = at, order, refs[0], refs[1:], send_sem, recv_sem

    def place(self, p):
        bits = part_bits(p)
        return tuple(bits[n] for n in self.order)

    def put(self, p, rows, value):
        self.buf[self.place(p) + (rows,)] = value

    def copy(self, k):
        mine = [self.at.bit[n] for n in self.order]
        return pltpu.make_async_remote_copy(src_ref=self.buf.at[tuple(mine[:k]) + (1 - mine[k],)], dst_ref=self.lands[k],
                                            send_sem=self.send_sem.at[k], recv_sem=self.recv_sem.at[k],
                                            device_id=self.at.flip(self.order[k]), device_id_type=MESH)

    def start(self, k):
        self.copy(k).start()

    def land(self, k):
        self.copy(k).wait_recv()
        mine = tuple(self.at.bit[n] for n in self.order[:k + 1])
        rest = len(self.order) - 1 - k
        for n in range(2 ** rest):
            sub = tuple((n >> m) % 2 for m in reversed(range(rest)))
            self.buf[mine + sub] = self.buf[mine + sub] + self.lands[k][sub if sub else ...]

    def step(self, k):
        self.land(k)
        self.start(k + 1)

    def result(self):
        return self.buf[tuple(self.at.bit[n] for n in self.order)]

    def drain(self):
        for k in range(len(self.order)):
            self.copy(k).wait_send()


PEERS = ('x', 'y', 'xy', 'xc', 'yc', 'xyc', 'c')
ORDERS = ('czxy', 'czxy', 'czyx', 'czxy', 'cxyz', 'cyzx')
SUM_ROWS = (2 * SLICE, 2 * SLICE, LANES, SLICE + HALF, SLICE + HALF, SLICE + SUB)


def exchange(at, b, src, dst, sems):
    out = []
    for k, names in enumerate(PEERS):
        z, sp = at.flip(names)
        out.append(pltpu.make_async_remote_copy(src_ref=src.at[b, sp], dst_ref=dst.at[b, at.me], send_sem=sems[0].at[b, k], recv_sem=sems[1].at[b, k],
                                                device_id=(z, sp), device_id_type=MESH))
    return out


def layer(x_ref, g_ref, g1_ref, s1_ref, g2_ref, s2_ref, wt_ref, bqkv_ref, wd_ref, bd_ref, wi_hbm, bi_ref, wo_hbm, bo_ref, cos_ref, sa_ref, sb_ref,
          out_ref, gx_ref, gwi_ref, gwo_ref, gqkv_ref, gwd_ref, tail_ref,
          wi_ref, wo_ref, wp_ref, ctx_ref, dqkv_ref, h2t_ref, gt_ref, buf_ref, in_ref, z_ref, res_ref, dh2_ref, gbi_ref, xt_ref, sdp_ref, acc_ref,
          sums_refs, load_sem, out_sems, back_sems, sum_send, sum_recv):
    at = Where()
    me = at.me
    loads = [pltpu.make_async_copy(src, dst, load_sem.at[n]) for n, (src, dst) in enumerate(((wi_hbm, wi_ref), (wo_hbm, wo_ref)))]
    for load in loads:
        load.start()
    barrier = pltpu.get_barrier_semaphore()
    for names in PEERS + ('z',):
        pl.semaphore_signal(barrier, inc=1, device_id=at.flip(names), device_id_type=MESH)
    sums = [Summed(at, order, refs, sum_send.at[n], sum_recv.at[n]) for n, (order, refs) in enumerate(zip(ORDERS, sums_refs))]
    early, tail = sums[:3], sums[3:]
    sum_w = sums[:2]
    sum_wo = sums[2]
    low = lane_iota(NT, LANES) < HD
    fold_weights(wt_ref, wp_ref)
    b_all = row(bqkv_ref)

    for b in range(NB):
        rows = span(b, NT)
        x = x_ref[rows, :].astype(F32)
        hat, _ = layer_hat(x)
        h_b = (hat * row(g1_ref) + row(s1_ref)).astype(BF16)
        qk = dot_tb(h_b, wp_ref[:2 * D, :])
        vv = dot_tb(h_b, wp_ref[2 * D:, :])
        dc = dot_tb(g_ref[rows, :], wd_ref[...])
        for p in range(PAIRS):
            bias_a, bias_b, bias_v = pair_bias(b_all, p)
            v_pair = vv[:, span(p, LANES)] + bias_v
            d_pair = dc[:, span(p, LANES)]
            for h, bias, second in ((2 * p, bias_a, jnp.where(low, v_pair, swap(d_pair))), (2 * p + 1, bias_b, jnp.where(low, swap(v_pair), d_pair))):
                t = qk[:, span(h, LANES)] + bias
                t = t * cos_ref[...] + pltpu.roll(t, TURN_BACK, 1) * sa_ref[...] + pltpu.roll(t, TURN, 1) * sb_ref[...]
                buf_ref[b, h, :, LO] = t.astype(BF16)
                buf_ref[b, h, :, HI] = second.astype(BF16)
        if b == 0:
            pl.semaphore_wait(barrier, len(PEERS) + 1)
        for copy in exchange(at, b, buf_ref, in_ref, out_sems):
            copy.start()
        in_ref[b, me] = buf_ref[b, me]
        ctx_ref[rows, :] = (hat * row(g2_ref) + row(s2_ref)).astype(BF16)
        res_ref[rows, :] = x + row(bd_ref) + row(bo_ref)

    h2t_ref[...] = ctx_ref[...].T
    gt_ref[...] = g_ref[...].T
    b_in = row(bi_ref)
    for load in loads:
        load.wait()
    for c in range(N_CHUNK):
        cols = span(c, CHUNK)
        pre = dot(ctx_ref[...], wi_ref[:, cols]) + b_in[:, cols]
        d_act = dot_tb(g_ref[...], wo_ref[cols, :])
        cdf = 0.5 * (1.0 + lax.erf(pre * math.sqrt(0.5)))
        pdf = jnp.exp(-0.5 * pre * pre) * (1.0 / math.sqrt(2.0 * math.pi))
        act = (pre * cdf).astype(BF16)
        d_pre = d_act * (cdf + pre * pdf)
        d_pre_bf = d_pre.astype(BF16)
        gbi_ref[:, cols] = jnp.broadcast_to(col_sum(d_pre), (SUB, CHUNK))
        g_wi = dot(h2t_ref[...], d_pre_bf)
        for p in range(PARTS):
            sum_w[c // 2].put(p, span(c % 2, SLICE), g_wi[span(p, SLICE)])
        if c % 2:
            sum_w[c // 2].start(0)
        g_wo = dot(gt_ref[...], act)
        for q in range(CHUNK // LANES):
            where = sum_wo.place(PARTS // N_CHUNK * c + q)
            for k in range(D // LANES):
                sum_wo.buf[where + (slice(None), span(k, LANES))] = g_wo[span(k, LANES), span(q, LANES)]
        res_ref[...] += dot(act, wo_ref[cols, :])
        d_h = dot_tb(d_pre_bf, wi_ref[:, cols])
        if c == 0:
            dh2_ref[...] = d_h
        else:
            dh2_ref[...] += d_h
    sum_wo.start(0)
    sum_w[0].step(0)
    zero_row = jnp.zeros((1, D), F32)
    g_ln2 = g_ln2_b = g_b_dense = zero_row
    for b in range(NB):
        rows = span(b, NT)
        hat, _ = layer_hat(x_ref[rows, :].astype(F32))
        d_h = dh2_ref[rows, :]
        g_ln2 += col_sum(d_h * hat)
        g_ln2_b += col_sum(d_h)
        g_b_dense += col_sum(g_ref[rows, :].astype(F32))
        dh2_ref[rows, :] = d_h * row(g2_ref)

    keep = lax.broadcasted_iota(jnp.int32, (NT, NT), 0) <= lane_iota(NT, NT)
    zero_t = jnp.zeros((HD, NT), BF16)
    s_cols, p_cols = span(0, NT), span(1, NT)

    def one_sequence(b, carry):
        for copy in exchange(at, b, buf_ref, in_ref, out_sems):
            copy.wait()
        for j in range(SP):
            xt_ref[:, span(j, NT)] = in_ref[b, j].T
        for i in reversed(range(SP)):
            cols = span(i, NT)
            q_t = xt_ref[span(0, HD), cols] * BF16(SCALE)
            dc_t = xt_ref[span(3, HD), cols]
            w_s = jnp.concatenate([zero_t, q_t, zero_t, zero_t], axis=0)
            w_p = jnp.concatenate([zero_t, zero_t, dc_t, zero_t], axis=0)
            w_sp = jnp.concatenate([w_s, w_p], axis=1)
            q_n = jnp.where(low, in_ref[b, i, :, LO] * BF16(SCALE), BF16(0.0))
            dc_n = jnp.where(low, BF16(0.0), in_ref[b, i, :, HI])
            w_acc = jnp.concatenate([q_n, dc_n], axis=0)
            tops = []
            for j in range(i + 1):
                kv = span(j, NT)
                both = dot(in_ref[b, j], w_sp)
                s = both[:, s_cols]
                if j == i:
                    s = jnp.where(keep, s, -1e30)
                sdp_ref[kv, s_cols] = s
                sdp_ref[kv, p_cols] = both[:, p_cols]
                part = fold(s, jnp.max)
                tops = [jnp.maximum(tops[0], part)] if tops else [part]
            top = jnp.max(tops[0], axis=0, keepdims=True)
            total = jnp.zeros((SUB, NT), F32)
            inner = jnp.zeros((SUB, NT), F32)
            for j in range(i + 1):
                kv = span(j, NT)
                e = jnp.exp(sdp_ref[kv, s_cols] - top)
                sdp_ref[kv, s_cols] = e
                total += fold(e, jnp.sum)
                inner += fold(e * sdp_ref[kv, p_cols], jnp.sum)
            inv = 1.0 / col_sum(total)
            delta = col_sum(inner) * inv
            ctx_t = jnp.zeros((HD, NT), F32)
            dq_t = jnp.zeros((HD, NT), F32)
            for j in range(i + 1):
                kv = span(j, NT)
                prob = sdp_ref[kv, s_cols] * inv
                prob_bf = prob.astype(BF16)
                ds_bf = (prob * (sdp_ref[kv, p_cols] - delta)).astype(BF16)
                ctx_t += dot(xt_ref[span(2, HD), kv], prob_bf)
                dq_t += dot(xt_ref[span(1, HD), kv], ds_bf)
                step = dot(jnp.concatenate([ds_bf, prob_bf], axis=1), w_acc)
                if i == SP - 1:
                    acc_ref[kv, :] = step
                else:
                    acc_ref[kv, :] += step
            nat = jnp.concatenate([dq_t * SCALE, ctx_t], axis=0).T
            acc = acc_ref[cols, :]
            buf_ref[b, i, :, LO] = jnp.where(low, nat, swap(acc)).astype(BF16)
            buf_ref[b, i, :, HI] = jnp.where(low, swap(nat), acc).astype(BF16)
            if i == SP - 3:
                @pl.when(b == 0)
                def _():
                    for s in early[1:]:
                        s.step(0)
        for copy in exchange(at, b, buf_ref, z_ref, back_sems):
            copy.start()
        z_ref[b, me] = buf_ref[b, me]
        return carry

    lax.fori_loop(0, NB, one_sequence, 0)

    def arrive(b):
        rows = span(b, NT)
        for copy in exchange(at, b, buf_ref, z_ref, back_sems):
            copy.wait()
        if b == NB - 1:
            for s in early:
                s.step(1)
        sums_qk, sums_v = [], []
        for p in range(PAIRS):
            seconds = []
            for h in (2 * p, 2 * p + 1):
                t = z_ref[b, h, :, LO].astype(F32)
                t = t * cos_ref[...] - pltpu.roll(t, TURN_BACK, 1) * sa_ref[...] - pltpu.roll(t, TURN, 1) * sb_ref[...]
                sums_qk.append(col_sum(t))
                dqkv_ref[rows, span(h, LANES)] = t.astype(BF16)
                seconds.append(z_ref[b, h, :, HI].astype(F32))
            ctx_ref[rows, span(p, LANES)] = jnp.where(low, seconds[0], swap(seconds[1])).astype(BF16)
            dv_pair = jnp.where(low, swap(seconds[0]), seconds[1])
            dqkv_ref[rows, span(2 * NH // 2 + p, LANES)] = dv_pair.astype(BF16)
            sums_v.append(col_sum(dv_pair))
        hat, inv_std = layer_hat(x_ref[rows, :].astype(F32))
        h1_t = (hat * row(g1_ref) + row(s1_ref)).astype(BF16).T
        ctx_t = ctx_ref[rows, :].T
        for k in range(4):
            block = span(k, D)
            term = dot(h1_t, dqkv_ref[rows, block]) if k < 3 else dot(ctx_t, g_ref[rows, :])
            if b:
                sdp_ref[block, :] += term
            else:
                sdp_ref[block, :] = term
        return hat, inv_std, jnp.concatenate(sums_qk, axis=1), jnp.concatenate(sums_v, axis=1)

    def finish(b, hat, inv_std):
        rows = span(b, NT)
        d_h1 = dot(dqkv_ref[rows, :], wp_ref[...])
        d_hat = d_h1 * row(g1_ref) + dh2_ref[rows, :]
        d_x = inv_std * (d_hat - jnp.mean(d_hat, axis=-1, keepdims=True) - hat * jnp.mean(d_hat * hat, axis=-1, keepdims=True))
        gx_ref[rows, :] = (g_ref[rows, :].astype(F32) + d_x).astype(BF16)
        return col_sum(d_h1 * hat), col_sum(d_h1)

    def forward(b):
        rows = span(b, NT)
        out_ref[rows, :] = (res_ref[rows, :] + dot(ctx_ref[rows, :], wd_ref[...])).astype(BF16)

    g_ln1 = g_ln1_b = zero_row
    gb_qk, gb_v = jnp.zeros((1, 2 * D), F32), zero_row
    for b in range(NB):
        hat, inv_std, part_qk, part_v = arrive(b)
        gb_qk += part_qk
        gb_v += part_v
        if b == NB - 1:
            for p in range(PARTS):
                first = SLICE * p
                tail[0].put(p, span(0, SLICE), sdp_ref[first:first + SLICE, :])
                tail[0].put(p, slice(SLICE, SLICE + HALF), sdp_ref[D + first:D + first + HALF, :])
                tail[1].put(p, span(0, HALF), sdp_ref[D + first + HALF:D + first + SLICE, :])
                tail[1].put(p, slice(HALF, HALF + SLICE), sdp_ref[2 * D + first:2 * D + first + SLICE, :])
            for s in tail[:2]:
                s.start(0)
        part_g, part_b = finish(b, hat, inv_std)
        g_ln1 += part_g
        g_ln1_b += part_b
        if b < NB - 1:
            forward(b)

    five = jnp.concatenate([g_ln1, g_ln1_b, g_ln2, g_ln2_b, g_b_dense] + [zero_row] * 3, axis=0)
    g_bqkv = jnp.broadcast_to(pair_lanes(gb_qk, gb_v), (SUB, QKV))
    small = slice(SLICE, SLICE + SUB)
    for p in range(PARTS):
        tail[2].put(p, span(0, SLICE), sdp_ref[QKV + SLICE * p:QKV + SLICE * p + SLICE, :])
        line = [cut(five, SLICE * p), gbi_ref[:, span(p, LANES)], cut(g_bqkv, 3 * SLICE * p), jnp.zeros((SUB, LANES), F32)]
        tail[2].put(p, small, jnp.concatenate(line, axis=1))
    tail[2].start(0)
    forward(NB - 1)

    for s in tail:
        s.step(0)
    for s in early:
        s.step(2)
    for s in tail:
        s.step(1)
    for s in early:
        s.land(3)
    for c in range(N_CHUNK):
        gwi_ref[:, span(c, CHUNK)] = sum_w[c // 2].result()[span(c % 2, SLICE)]
    g_wo = sum_wo.result()
    for k in range(D // LANES):
        gwo_ref[:, span(k, LANES)] = g_wo[:, span(k, LANES)].T
    for s in tail:
        s.step(2)
    for s in tail:
        s.land(3)
    first, second, third = (s.result() for s in tail)
    gqkv_ref[:, span(0, D)] = first[:SLICE]
    gqkv_ref[:HALF, span(1, D)] = first[SLICE:]
    gqkv_ref[HALF:, span(1, D)] = second[:HALF]
    gqkv_ref[:, span(2, D)] = second[HALF:]
    gwd_ref[...] = third[:SLICE]
    tail_ref[...] = third[SLICE:]
    for s in sums:
        s.drain()


def write_out(out_in, gx_in, gwi_in, gwo_in, gqkv_in, gwd_in, tail_in,
              out_ref, gx_ref, g1_ref, s1_ref, g2_ref, s2_ref, gqkv_ref, gbqkv_ref, gwd_ref, gbd_ref, gwi_ref, gbi_ref, gwo_ref, gbo_ref):
    out_ref[...] = out_in[...]
    gx_ref[...] = gx_in[...]
    gwi_ref[...] = gwi_in[...]
    gwo_ref[...] = gwo_in[...]
    gwd_ref[...] = gwd_in[...]
    for h in range(NH):
        tile = gqkv_in[:, span(h, LANES)]
        gqkv_ref[:, 0, h, :] = tile[:, :HD]
        gqkv_ref[:, 1, h, :] = tile[:, HD:]
        gqkv_ref[:, 2, h, :] = gqkv_in[:, span(2 * NH + h, HD)]
    for n, ref in enumerate((g1_ref, s1_ref, g2_ref, s2_ref, gbd_ref)):
        ref[...] = tail_in[n, :SLICE]
    gbo_ref[...] = tail_in[n, :SLICE]
    gbi_ref[...] = tail_in[0, span(1, LANES)]
    gbqkv_ref[...] = tail_in[0, 2 * LANES:2 * LANES + 3 * SLICE]


def sds(shape, dtype):
    return jax.ShapeDtypeStruct(shape, dtype)


def halving(rows):
    return tuple(pltpu.VMEM((2,) * n + (rows, D), F32) for n in reversed(range(5)))


def vmem(rows, cols, dtype):
    return pltpu.VMEM((rows, cols), dtype)


def solution(mesh):
    grad_axes = ('dp', 'sp')

    def device_step(hidden, grad_out, ln1_gain, ln1_bias, ln2_gain, ln2_bias, w_qkv, b_qkv, w_dense, b_dense, w_in, b_in, w_out, b_out):
        x = hidden.reshape(ROWS, D)
        g = grad_out.reshape(ROWS, D)
        wt = jnp.moveaxis(w_qkv, 0, -1).reshape(QKV, D)
        in_head = (jnp.arange(LANES) % HD)[None, :]
        inv_freq = ROPE_BASE ** (-(2.0 * (in_head % TURN)).astype(F32) / ROT)
        pos = (lax.axis_index('sp') * NT + jnp.arange(NT)).astype(F32)
        angles = pos[:, None] * inv_freq
        cos_t = jnp.where(in_head < ROT, jnp.cos(angles), 1.0)
        sin_t = jnp.sin(angles)
        sin_a = jnp.where(in_head < TURN, -sin_t, 0.0)
        sin_b = jnp.where((in_head >= TURN) & (in_head < ROT), sin_t, 0.0)

        dma = pltpu.SemaphoreType.DMA
        whole = pl.BlockSpec(memory_space=pltpu.VMEM)
        in_specs = [whole] * 17
        in_specs[10] = in_specs[12] = pl.BlockSpec(memory_space=pl.ANY)
        block = pltpu.VMEM((NB, SP, NT, 2 * LANES), BF16)
        peer_sems = (dma((NB, len(PEERS))),) * 2
        results = pl.pallas_call(
            layer,
            out_shape=(sds((ROWS, D), BF16), sds((ROWS, D), BF16), sds((SLICE, FF), F32), sds((LANES, D), F32), sds((SLICE, QKV), F32), sds((SLICE, D), F32), sds((SUB, D), F32)),
            in_specs=in_specs,
            out_specs=(whole,) * 7,
            scratch_shapes=[
                vmem(D, FF, BF16), vmem(FF, D, BF16), vmem(QKV, D, BF16), vmem(ROWS, D, BF16), vmem(ROWS, QKV, BF16), vmem(D, ROWS, BF16), vmem(D, ROWS, BF16),
                block, block, block, vmem(ROWS, D, F32), vmem(ROWS, D, F32), vmem(SUB, FF, F32),
                vmem(2 * LANES, SEQ, BF16), vmem(SEQ, 2 * NT, F32), vmem(SEQ, LANES, F32),
                tuple(halving(rows) for rows in SUM_ROWS),
                dma((2,)), peer_sems, peer_sems, dma((6, 4)), dma((6, 4)),
            ],
            compiler_params=pltpu.CompilerParams(vmem_limit_bytes=VMEM_LIMIT, collective_id=0, has_side_effects=True),
            cost_estimate=pl.CostEstimate(flops=56_000_000_000, bytes_accessed=12_000_000, transcendentals=10_000_000),
            name='layer',
        )(x, g, ln1_gain, ln1_bias, ln2_gain, ln2_bias, wt, b_qkv, w_dense, b_dense, w_in, b_in, w_out, b_out, cos_t, sin_a, sin_b)

        part = sds((SLICE,), F32)
        tokens = sds((ROWS, D), BF16)
        final = list(pl.pallas_call(
            write_out,
            out_shape=(tokens, tokens, part, part, part, part, sds((SLICE, 3, NH, HD), F32), sds((3 * SLICE,), F32), sds((SLICE, D), F32), part,
                       sds((SLICE, FF), F32), sds((LANES,), F32), sds((LANES, D), F32), part),
            in_specs=[whole] * 7,
            out_specs=(whole,) * 14,
            name='write_out',
        )(*results))
        final[0] = final[0].reshape(hidden.shape)
        final[1] = final[1].reshape(hidden.shape)
        final[6] = jnp.swapaxes(final[6], 1, 2)
        return tuple(final)

    tok_spec = P('dp', 'sp', None)
    grad_spec = P(grad_axes)
    return jax.shard_map(device_step, mesh=mesh, in_specs=(tok_spec, tok_spec) + (P(),) * 12, out_specs=(tok_spec, tok_spec) + (grad_spec,) * 12, check_vma=False)
```

```python
import math
import jax
import jax.numpy as jnp
import numpy as np
from jax import lax
from jax.experimental import pallas as pl
from jax.experimental.pallas import tpu as pltpu
from jax.sharding import PartitionSpec as P

LN_EPS = 1e-5
ROPE_BASE = 10000.0
F32 = jnp.float32
BF16 = jnp.bfloat16
MESH = pl.DeviceIdType.MESH
VMEM_LIMIT = 67_043_328

NB, NT, D, NH, HD, FF = 3, 256, 512, 8, 64, 2048
ROWS = NB * NT
SP = 8
PARTS = 16
SEQ = SP * NT
CHUNK = 512
N_CHUNK = FF // CHUNK
SUB = 8
ROW_B_IN, ROW_B_QKV = 5, 6
LANES = 2 * HD
PAIRS = NH // 2
SLICE = D // PARTS
QKV = 3 * D
ROT = HD // 4
TURN = ROT // 2
TURN_BACK = LANES - TURN
LO = slice(0, LANES)
HI = slice(LANES, 2 * LANES)
SCALE = 1.0 / math.sqrt(HD)


def dot(a, b):
    return lax.dot_general(a, b, (((1,), (0,)), ((), ())), preferred_element_type=F32)


def dot_tb(a, b):
    return lax.dot_general(a, b, (((1,), (1,)), ((), ())), preferred_element_type=F32)


def span(index, size):
    return slice(size * index, size * (index + 1))


def lane_iota(rows, cols):
    return lax.broadcasted_iota(jnp.int32, (rows, cols), 1)


def swap(x):
    return pltpu.roll(x, HD, 1)


def row(ref):
    return ref[...].reshape(1, ref.shape[0])


def col_sum(x):
    return jnp.sum(x, axis=0, keepdims=True)


def fold(x, op):
    return op(x.reshape(NT // SUB, SUB, NT), axis=0)


def layer_hat(x):
    mean_val = jnp.mean(x, axis=-1, keepdims=True)
    centered = x - mean_val
    var_val = jnp.mean(centered * centered, axis=-1, keepdims=True)
    inv_std = lax.rsqrt(var_val + LN_EPS)
    return centered * inv_std, inv_std


def fold_weights(wt_ref, wp_ref):
    for h in range(NH):
        base = 3 * HD * h
        wp_ref[span(h, LANES), :] = wt_ref[base:base + LANES, :]
        wp_ref[span(2 * NH + h, HD), :] = wt_ref[base + LANES:base + LANES + HD, :]


def pair_lanes(row_qk, row_v):
    low = lane_iota(1, LANES) < HD
    tiles = []
    for p in range(PAIRS):
        second = swap(row_qk[:, span(2 * p + 1, LANES)])
        v_pair = row_v[:, span(p, LANES)]
        tiles += [row_qk[:, span(2 * p, LANES)], jnp.where(low, v_pair, second), jnp.where(low, second, v_pair)]
    return jnp.concatenate(tiles, axis=1)


def pair_bias(b_all, p):
    low = lane_iota(1, LANES) < HD
    first, mid, last = (b_all[:, span(3 * p + n, LANES)] for n in range(3))
    return first, swap(jnp.where(low, last, mid)), jnp.where(low, mid, last)


def cut(x, shift):
    width = x.shape[1]
    return pltpu.roll(x, (width - shift) % width, 1)[:, LO]


def rotation(near_ref, far_ref, block, cos_ref, sa_ref, sb_ref):
    in_head = lane_iota(NT, LANES) % HD
    near, far = near_ref[...], far_ref[pl.ds(block, 1), :]
    near_s, far_s = pltpu.roll(near, LANES - ROT, 1), pltpu.roll(far, LANES - ROT, 1)
    sin_t = near_s * far + near * far_s
    cos_ref[...] = jnp.where(in_head < ROT, near * far - near_s * far_s, 1.0)
    sa_ref[...] = jnp.where(in_head < TURN, -sin_t, 0.0)
    sb_ref[...] = jnp.where((in_head >= TURN) & (in_head < ROT), sin_t, 0.0)


def angle_table(positions):
    lane = np.arange(LANES) % HD
    freq = ROPE_BASE ** (-(2.0 * (lane % TURN)) / ROT)
    angles = positions[:, None] * freq[None, :]
    return np.where(lane < ROT, np.cos(angles), np.sin(angles)).astype(np.float32)


def part_bits(p):
    return {'c': p % 2, 'x': p // 2 % 2, 'y': p // 4 % 2, 'z': p // 8}


class Where:
    def __init__(self):
        self.z = lax.axis_index('dp')
        self.me = lax.axis_index('sp')
        self.bit = part_bits(self.z * SP + self.me)

    def flip(self, names):
        step = {'c': 1, 'x': 2, 'y': 4}
        z, sp = self.z, self.me
        for n in names:
            if n == 'z':
                z = 1 - z
            else:
                sp = sp + step[n] * (1 - 2 * self.bit[n])
        return z, sp


class Summed:
    def __init__(self, at, order, refs, send_sem, recv_sem):
        self.at, self.order, self.buf, self.lands, self.send_sem, self.recv_sem = at, order, refs[0], refs[1:], send_sem, recv_sem

    def place(self, p):
        bits = part_bits(p)
        return tuple(bits[n] for n in self.order)

    def put(self, p, rows, value):
        self.buf[self.place(p) + (rows,)] = value

    def copy(self, k):
        mine = [self.at.bit[n] for n in self.order]
        return pltpu.make_async_remote_copy(src_ref=self.buf.at[tuple(mine[:k]) + (1 - mine[k],)], dst_ref=self.lands[k],
                                            send_sem=self.send_sem.at[k], recv_sem=self.recv_sem.at[k],
                                            device_id=self.at.flip(self.order[k]), device_id_type=MESH)

    def start(self, k):
        self.copy(k).start()

    def land(self, k):
        self.copy(k).wait_recv()
        mine = tuple(self.at.bit[n] for n in self.order[:k + 1])
        rest = len(self.order) - 1 - k
        for n in range(2 ** rest):
            sub = tuple((n >> m) % 2 for m in reversed(range(rest)))
            self.buf[mine + sub] = self.buf[mine + sub] + self.lands[k][sub if sub else ...]

    def step(self, k):
        self.land(k)
        self.start(k + 1)

    def result(self):
        return self.buf[tuple(self.at.bit[n] for n in self.order)]

    def drain(self):
        for k in range(len(self.order)):
            self.copy(k).wait_send()


PEERS = ('x', 'y', 'xy', 'xc', 'yc', 'xyc', 'c')
ORDERS = ('czxy', 'czxy', 'czyx', 'czxy', 'czyx', 'cxzy', 'cyzx', 'czxy')
SUM_SHAPES = ((2 * SLICE, D), (2 * SLICE, D), (LANES, D)) + ((SLICE, D),) * 4 + ((SUB, LANES),)


def exchange(at, b, src, dst, sems):
    out = []
    for k, names in enumerate(PEERS):
        z, sp = at.flip(names)
        out.append(pltpu.make_async_remote_copy(src_ref=src.at[b, sp], dst_ref=dst.at[b, at.me], send_sem=sems[0].at[b, k], recv_sem=sems[1].at[b, k],
                                                device_id=(z, sp), device_id_type=MESH))
    return out


def layer(x_ref, g_ref, g1_ref, s1_ref, g2_ref, s2_ref, wt_ref, bqkv_ref, wd_ref, bd_ref, wi_hbm, bi_ref, wo_hbm, bo_ref, near_ref, far_ref,
          out_hbm, gx_hbm, gwi_ref, gwo_ref, gqkv_ref, gwd_ref, tail_ref,
          out_ref, gx_ref, cos_ref, sa_ref, sb_ref, wi_ref, wo_ref, wp_ref, ctx_ref, dqkv_ref, h2t_ref, gt_ref, buf_ref, in_ref, z_ref, res_ref, dh2_ref, gbi_ref, xt_ref, sdp_ref, acc_ref,
          sums_refs, load_sem, store_sem, out_sems, back_sems, sum_send, sum_recv):
    at = Where()
    me = at.me
    loads = [pltpu.make_async_copy(src, dst, load_sem.at[n]) for n, (src, dst) in enumerate(((wi_hbm, wi_ref), (wo_hbm, wo_ref)))]
    for load in loads:
        load.start()
    barrier = pltpu.get_barrier_semaphore()
    for names in PEERS + ('z',):
        pl.semaphore_signal(barrier, inc=1, device_id=at.flip(names), device_id_type=MESH)
    sums = [Summed(at, order, refs, sum_send.at[n], sum_recv.at[n]) for n, (order, refs) in enumerate(zip(ORDERS, sums_refs))]
    early, tail = sums[:3], sums[3:]
    sum_w = sums[:2]
    sum_wo = sums[2]
    low = lane_iota(NT, LANES) < HD
    rotation(near_ref, far_ref, me, cos_ref, sa_ref, sb_ref)
    fold_weights(wt_ref, wp_ref)
    b_all = row(bqkv_ref)

    for b in range(NB):
        rows = span(b, NT)
        x = x_ref[rows, :].astype(F32)
        hat, _ = layer_hat(x)
        h_b = (hat * row(g1_ref) + row(s1_ref)).astype(BF16)
        qk = dot_tb(h_b, wp_ref[:2 * D, :])
        vv = dot_tb(h_b, wp_ref[2 * D:, :])
        dc = dot_tb(g_ref[rows, :], wd_ref[...])
        for p in range(PAIRS):
            bias_a, bias_b, bias_v = pair_bias(b_all, p)
            v_pair = vv[:, span(p, LANES)] + bias_v
            d_pair = dc[:, span(p, LANES)]
            for h, bias, second in ((2 * p, bias_a, jnp.where(low, v_pair, swap(d_pair))), (2 * p + 1, bias_b, jnp.where(low, swap(v_pair), d_pair))):
                t = qk[:, span(h, LANES)] + bias
                t = t * cos_ref[...] + pltpu.roll(t, TURN_BACK, 1) * sa_ref[...] + pltpu.roll(t, TURN, 1) * sb_ref[...]
                buf_ref[b, h, :, LO] = t.astype(BF16)
                buf_ref[b, h, :, HI] = second.astype(BF16)
        if b == 0:
            pl.semaphore_wait(barrier, len(PEERS) + 1)
        for copy in exchange(at, b, buf_ref, in_ref, out_sems):
            copy.start()
        in_ref[b, me] = buf_ref[b, me]
        ctx_ref[rows, :] = (hat * row(g2_ref) + row(s2_ref)).astype(BF16)
        res_ref[rows, :] = x + row(bd_ref) + row(bo_ref)

    h2t_ref[...] = ctx_ref[...].T
    gt_ref[...] = g_ref[...].T
    b_in = row(bi_ref)
    for load in loads:
        load.wait()
    for c in range(N_CHUNK):
        cols = span(c, CHUNK)
        pre = dot(ctx_ref[...], wi_ref[:, cols]) + b_in[:, cols]
        d_act = dot_tb(g_ref[...], wo_ref[cols, :])
        cdf = 0.5 * (1.0 + lax.erf(pre * math.sqrt(0.5)))
        pdf = jnp.exp(-0.5 * pre * pre) * (1.0 / math.sqrt(2.0 * math.pi))
        act = (pre * cdf).astype(BF16)
        d_pre = d_act * (cdf + pre * pdf)
        d_pre_bf = d_pre.astype(BF16)
        gbi_ref[:, cols] = jnp.broadcast_to(col_sum(d_pre), (SUB, CHUNK))
        g_wi = dot(h2t_ref[...], d_pre_bf)
        for p in range(PARTS):
            sum_w[c // 2].put(p, span(c % 2, SLICE), g_wi[span(p, SLICE)])
        if c % 2:
            sum_w[c // 2].start(0)
        g_wo = dot(gt_ref[...], act)
        for q in range(CHUNK // LANES):
            where = sum_wo.place(PARTS // N_CHUNK * c + q)
            for k in range(D // LANES):
                sum_wo.buf[where + (slice(None), span(k, LANES))] = g_wo[span(k, LANES), span(q, LANES)]
        res_ref[...] += dot(act, wo_ref[cols, :])
        d_h = dot_tb(d_pre_bf, wi_ref[:, cols])
        if c == 0:
            dh2_ref[...] = d_h
        else:
            dh2_ref[...] += d_h
    sum_wo.start(0)
    sum_w[0].step(0)
    zero_row = jnp.zeros((1, D), F32)
    g_ln2 = g_ln2_b = g_b_dense = zero_row
    for b in range(NB):
        rows = span(b, NT)
        hat, _ = layer_hat(x_ref[rows, :].astype(F32))
        d_h = dh2_ref[rows, :]
        g_ln2 += col_sum(d_h * hat)
        g_ln2_b += col_sum(d_h)
        g_b_dense += col_sum(g_ref[rows, :].astype(F32))
        dh2_ref[rows, :] = d_h * row(g2_ref)

    keep = lax.broadcasted_iota(jnp.int32, (NT, NT), 0) <= lane_iota(NT, NT)
    zero_t = jnp.zeros((HD, NT), BF16)
    s_cols, p_cols = span(0, NT), span(1, NT)

    def one_sequence(b, carry):
        for copy in exchange(at, b, buf_ref, in_ref, out_sems):
            copy.wait()
        for j in range(SP):
            xt_ref[:, span(j, NT)] = in_ref[b, j].T
        for i in reversed(range(SP)):
            cols = span(i, NT)
            q_t = xt_ref[span(0, HD), cols] * BF16(SCALE)
            dc_t = xt_ref[span(3, HD), cols]
            w_s = jnp.concatenate([zero_t, q_t, zero_t, zero_t], axis=0)
            w_p = jnp.concatenate([zero_t, zero_t, dc_t, zero_t], axis=0)
            w_sp = jnp.concatenate([w_s, w_p], axis=1)
            q_n = jnp.where(low, in_ref[b, i, :, LO] * BF16(SCALE), BF16(0.0))
            dc_n = jnp.where(low, BF16(0.0), in_ref[b, i, :, HI])
            w_acc = jnp.concatenate([q_n, dc_n], axis=0)
            tops = []
            for j in range(i + 1):
                kv = span(j, NT)
                both = dot(in_ref[b, j], w_sp)
                s = both[:, s_cols]
                if j == i:
                    s = jnp.where(keep, s, -1e30)
                sdp_ref[kv, s_cols] = s
                sdp_ref[kv, p_cols] = both[:, p_cols]
                part = fold(s, jnp.max)
                tops = [jnp.maximum(tops[0], part)] if tops else [part]
            top = jnp.max(tops[0], axis=0, keepdims=True)
            total = jnp.zeros((SUB, NT), F32)
            inner = jnp.zeros((SUB, NT), F32)
            for j in range(i + 1):
                kv = span(j, NT)
                e = jnp.exp(sdp_ref[kv, s_cols] - top)
                sdp_ref[kv, s_cols] = e
                total += fold(e, jnp.sum)
                inner += fold(e * sdp_ref[kv, p_cols], jnp.sum)
            inv = 1.0 / col_sum(total)
            delta = col_sum(inner) * inv
            ctx_t = jnp.zeros((HD, NT), F32)
            dq_t = jnp.zeros((HD, NT), F32)
            for j in range(i + 1):
                kv = span(j, NT)
                prob = sdp_ref[kv, s_cols] * inv
                prob_bf = prob.astype(BF16)
                ds_bf = (prob * (sdp_ref[kv, p_cols] - delta)).astype(BF16)
                ctx_t += dot(xt_ref[span(2, HD), kv], prob_bf)
                dq_t += dot(xt_ref[span(1, HD), kv], ds_bf)
                step = dot(jnp.concatenate([ds_bf, prob_bf], axis=1), w_acc)
                if i == SP - 1:
                    acc_ref[kv, :] = step
                else:
                    acc_ref[kv, :] += step
            nat = jnp.concatenate([dq_t * SCALE, ctx_t], axis=0).T
            acc = acc_ref[cols, :]
            buf_ref[b, i, :, LO] = jnp.where(low, nat, swap(acc)).astype(BF16)
            buf_ref[b, i, :, HI] = jnp.where(low, swap(nat), acc).astype(BF16)
            if i == SP - 3:
                @pl.when(b == 0)
                def _():
                    for s in early[1:]:
                        s.step(0)
        for copy in exchange(at, b, buf_ref, z_ref, back_sems):
            copy.start()
        z_ref[b, me] = buf_ref[b, me]
        return carry

    lax.fori_loop(0, NB, one_sequence, 0)

    def arrive(b):
        rows = span(b, NT)
        for copy in exchange(at, b, buf_ref, z_ref, back_sems):
            copy.wait()
        if b == NB - 1:
            for s in early:
                s.step(1)
        sums_qk, sums_v = [], []
        for p in range(PAIRS):
            seconds = []
            for h in (2 * p, 2 * p + 1):
                t = z_ref[b, h, :, LO].astype(F32)
                t = t * cos_ref[...] - pltpu.roll(t, TURN_BACK, 1) * sa_ref[...] - pltpu.roll(t, TURN, 1) * sb_ref[...]
                sums_qk.append(col_sum(t))
                dqkv_ref[rows, span(h, LANES)] = t.astype(BF16)
                seconds.append(z_ref[b, h, :, HI].astype(F32))
            ctx_ref[rows, span(p, LANES)] = jnp.where(low, seconds[0], swap(seconds[1])).astype(BF16)
            dv_pair = jnp.where(low, swap(seconds[0]), seconds[1])
            dqkv_ref[rows, span(2 * NH // 2 + p, LANES)] = dv_pair.astype(BF16)
            sums_v.append(col_sum(dv_pair))
        hat, inv_std = layer_hat(x_ref[rows, :].astype(F32))
        h1_t = (hat * row(g1_ref) + row(s1_ref)).astype(BF16).T
        ctx_t = ctx_ref[rows, :].T
        for k in range(4):
            block = span(k, D)
            term = dot(h1_t, dqkv_ref[rows, block]) if k < 3 else dot(ctx_t, g_ref[rows, :])
            if b:
                sdp_ref[block, :] += term
            else:
                sdp_ref[block, :] = term
        return hat, inv_std, jnp.concatenate(sums_qk, axis=1), jnp.concatenate(sums_v, axis=1)

    def finish(b, hat, inv_std):
        rows = span(b, NT)
        d_h1 = dot(dqkv_ref[rows, :], wp_ref[...])
        d_hat = d_h1 * row(g1_ref) + dh2_ref[rows, :]
        d_x = inv_std * (d_hat - jnp.mean(d_hat, axis=-1, keepdims=True) - hat * jnp.mean(d_hat * hat, axis=-1, keepdims=True))
        gx_ref[rows, :] = (g_ref[rows, :].astype(F32) + d_x).astype(BF16)
        return col_sum(d_h1 * hat), col_sum(d_h1)

    def forward(b):
        rows = span(b, NT)
        out_ref[rows, :] = (res_ref[rows, :] + dot(ctx_ref[rows, :], wd_ref[...])).astype(BF16)

    g_ln1 = g_ln1_b = zero_row
    gb_qk, gb_v = jnp.zeros((1, 2 * D), F32), zero_row
    for b in range(NB):
        hat, inv_std, part_qk, part_v = arrive(b)
        gb_qk += part_qk
        gb_v += part_v
        if b == NB - 1:
            for p in range(PARTS):
                for k in range(3):
                    tail[k].put(p, slice(None), sdp_ref[D * k + SLICE * p:D * k + SLICE * p + SLICE, :])
            for s in tail[:3]:
                s.start(0)
        part_g, part_b = finish(b, hat, inv_std)
        g_ln1 += part_g
        g_ln1_b += part_b
        if b < NB - 1:
            forward(b)

    store_gx = pltpu.make_async_copy(gx_ref, gx_hbm, store_sem.at[0])
    store_gx.start()
    five = jnp.concatenate([g_ln1, g_ln1_b, g_ln2, g_ln2_b, g_b_dense] + [zero_row] * 3, axis=0)
    g_bqkv = jnp.broadcast_to(pair_lanes(gb_qk, gb_v), (SUB, QKV))
    line = lax.broadcasted_iota(jnp.int32, (SUB, LANES), 0)
    for p in range(PARTS):
        tail[3].put(p, slice(None), sdp_ref[QKV + SLICE * p:QKV + SLICE * p + SLICE, :])
        small = jnp.where(line == ROW_B_IN, gbi_ref[:, span(p, LANES)], cut(five, SLICE * p))
        tail[4].put(p, slice(None), jnp.where(line == ROW_B_QKV, cut(g_bqkv, 3 * SLICE * p), small))
    for s in tail[3:]:
        s.start(0)
    forward(NB - 1)
    store_out = pltpu.make_async_copy(out_ref, out_hbm, store_sem.at[1])
    store_out.start()

    for s in tail:
        s.step(0)
    for s in early:
        s.step(2)
    for s in tail:
        s.step(1)
    for s in early:
        s.land(3)
    for c in range(N_CHUNK):
        gwi_ref[:, span(c, CHUNK)] = sum_w[c // 2].result()[span(c % 2, SLICE)]
    g_wo = sum_wo.result()
    for k in range(D // LANES):
        gwo_ref[:, span(k, LANES)] = g_wo[:, span(k, LANES)].T
    for s in tail:
        s.step(2)
    for s in tail:
        s.land(3)
    for k in range(3):
        gqkv_ref[:, span(k, D)] = tail[k].result()
    gwd_ref[...] = tail[3].result()
    tail_ref[...] = tail[4].result()
    store_gx.wait()
    store_out.wait()
    for s in sums:
        s.drain()


def write_out(out_in, gx_in, gwi_in, gwo_in, gqkv_in, gwd_in, tail_in,
              out_ref, gx_ref, g1_ref, s1_ref, g2_ref, s2_ref, gqkv_ref, gbqkv_ref, gwd_ref, gbd_ref, gwi_ref, gbi_ref, gwo_ref, gbo_ref):
    out_ref[...] = out_in[...]
    gx_ref[...] = gx_in[...]
    gwi_ref[...] = gwi_in[...]
    gwo_ref[...] = gwo_in[...]
    gwd_ref[...] = gwd_in[...]
    for h in range(NH):
        tile = gqkv_in[:, span(h, LANES)]
        gqkv_ref[:, 0, h, :] = tile[:, :HD]
        gqkv_ref[:, 1, h, :] = tile[:, HD:]
        gqkv_ref[:, 2, h, :] = gqkv_in[:, span(2 * NH + h, HD)]
    for n, ref in enumerate((g1_ref, s1_ref, g2_ref, s2_ref, gbd_ref)):
        ref[...] = tail_in[n, :SLICE]
    gbo_ref[...] = tail_in[n, :SLICE]
    gbi_ref[...] = tail_in[ROW_B_IN, :]
    gbqkv_ref[...] = tail_in[ROW_B_QKV, :3 * SLICE]


def sds(shape, dtype):
    return jax.ShapeDtypeStruct(shape, dtype)


def halving(shape):
    return tuple(pltpu.VMEM((2,) * n + shape, F32) for n in reversed(range(5)))


def vmem(rows, cols, dtype):
    return pltpu.VMEM((rows, cols), dtype)


def solution(mesh):
    grad_axes = ('dp', 'sp')

    def device_step(hidden, grad_out, ln1_gain, ln1_bias, ln2_gain, ln2_bias, w_qkv, b_qkv, w_dense, b_dense, w_in, b_in, w_out, b_out):
        x = hidden.reshape(ROWS, D)
        g = grad_out.reshape(ROWS, D)
        wt = jnp.moveaxis(w_qkv, 0, -1).reshape(QKV, D)
        near = jnp.asarray(angle_table(np.arange(NT)))
        far = jnp.asarray(angle_table(NT * np.arange(SP)))
        dma = pltpu.SemaphoreType.DMA
        whole = pl.BlockSpec(memory_space=pltpu.VMEM)
        in_specs = [whole] * 16
        in_specs[10] = in_specs[12] = pl.BlockSpec(memory_space=pl.ANY)
        block = pltpu.VMEM((NB, SP, NT, 2 * LANES), BF16)
        peer_sems = (dma((NB, len(PEERS))),) * 2
        results = pl.pallas_call(
            layer,
            out_shape=(sds((ROWS, D), BF16), sds((ROWS, D), BF16), sds((SLICE, FF), F32), sds((LANES, D), F32), sds((SLICE, QKV), F32), sds((SLICE, D), F32), sds((SUB, LANES), F32)),
            in_specs=in_specs,
            out_specs=(in_specs[10],) * 2 + (whole,) * 5,
            scratch_shapes=[
                vmem(ROWS, D, BF16), vmem(ROWS, D, BF16), vmem(NT, LANES, F32), vmem(NT, LANES, F32), vmem(NT, LANES, F32), vmem(D, FF, BF16), vmem(FF, D, BF16), vmem(QKV, D, BF16), vmem(ROWS, D, BF16), vmem(ROWS, QKV, BF16), vmem(D, ROWS, BF16), vmem(D, ROWS, BF16),
                block, block, block, vmem(ROWS, D, F32), vmem(ROWS, D, F32), vmem(SUB, FF, F32),
                vmem(2 * LANES, SEQ, BF16), vmem(SEQ, 2 * NT, F32), vmem(SEQ, LANES, F32),
                tuple(halving(shape) for shape in SUM_SHAPES),
                dma((2,)), dma((2,)), peer_sems, peer_sems, dma((8, 4)), dma((8, 4)),
            ],
            compiler_params=pltpu.CompilerParams(vmem_limit_bytes=VMEM_LIMIT, collective_id=0, has_side_effects=True),
            cost_estimate=pl.CostEstimate(flops=56_000_000_000, bytes_accessed=12_000_000, transcendentals=10_000_000),
            name='layer',
        )(x, g, ln1_gain, ln1_bias, ln2_gain, ln2_bias, wt, b_qkv, w_dense, b_dense, w_in, b_in, w_out, b_out, near, far)

        part = sds((SLICE,), F32)
        tokens = sds((ROWS, D), BF16)
        final = list(pl.pallas_call(
            write_out,
            out_shape=(tokens, tokens, part, part, part, part, sds((SLICE, 3, NH, HD), F32), sds((3 * SLICE,), F32), sds((SLICE, D), F32), part,
                       sds((SLICE, FF), F32), sds((LANES,), F32), sds((LANES, D), F32), part),
            in_specs=[whole] * 7,
            out_specs=(whole,) * 14,
            name='write_out',
        )(*results))
        final[0] = final[0].reshape(hidden.shape)
        final[1] = final[1].reshape(hidden.shape)
        final[6] = jnp.swapaxes(final[6], 1, 2)
        return tuple(final)

    tok_spec = P('dp', 'sp', None)
    grad_spec = P(grad_axes)
    return jax.shard_map(device_step, mesh=mesh, in_specs=(tok_spec, tok_spec) + (P(),) * 12, out_specs=(tok_spec, tok_spec) + (grad_spec,) * 12, check_vma=False)
```

```python
import math
import jax
import jax.numpy as jnp
import numpy as np
from jax import lax
from jax.experimental import pallas as pl
from jax.experimental.pallas import tpu as pltpu
from jax.sharding import PartitionSpec as P

LN_EPS = 1e-5
ROPE_BASE = 10000.0
F32 = jnp.float32
BF16 = jnp.bfloat16
MESH = pl.DeviceIdType.MESH
VMEM_LIMIT = 67_043_328

NB, NT, D, NH, HD, FF = 3, 256, 512, 8, 64, 2048
ROWS = NB * NT
SP = 8
PARTS = 16
SEQ = SP * NT
CHUNK = 512
N_CHUNK = FF // CHUNK
SUB = 8
ROW_B_IN, ROW_B_QKV = 5, 6
LANES = 2 * HD
PAIRS = NH // 2
SLICE = D // PARTS
QKV = 3 * D
ROT = HD // 4
TURN = ROT // 2
TURN_BACK = LANES - TURN
LO = slice(0, LANES)
HI = slice(LANES, 2 * LANES)
SCALE = 1.0 / math.sqrt(HD)


def dot(a, b):
    return lax.dot_general(a, b, (((1,), (0,)), ((), ())), preferred_element_type=F32)


def dot_tb(a, b):
    return lax.dot_general(a, b, (((1,), (1,)), ((), ())), preferred_element_type=F32)


def span(index, size):
    return slice(size * index, size * (index + 1))


def lane_iota(rows, cols):
    return lax.broadcasted_iota(jnp.int32, (rows, cols), 1)


def swap(x):
    return pltpu.roll(x, HD, 1)


def row(ref):
    return ref[...].reshape(1, ref.shape[0])


def col_sum(x):
    return jnp.sum(x, axis=0, keepdims=True)


def fold(x, op):
    return op(x.reshape(NT // SUB, SUB, NT), axis=0)


def layer_hat(x):
    mean_val = jnp.mean(x, axis=-1, keepdims=True)
    centered = x - mean_val
    var_val = jnp.mean(centered * centered, axis=-1, keepdims=True)
    inv_std = lax.rsqrt(var_val + LN_EPS)
    return centered * inv_std, inv_std


def fold_weights(wt_ref, wp_ref):
    for h in range(NH):
        base = 3 * HD * h
        wp_ref[span(h, LANES), :] = wt_ref[base:base + LANES, :]
        wp_ref[span(2 * NH + h, HD), :] = wt_ref[base + LANES:base + LANES + HD, :]


def pair_lanes(row_qk, row_v):
    low = lane_iota(1, LANES) < HD
    tiles = []
    for p in range(PAIRS):
        second = swap(row_qk[:, span(2 * p + 1, LANES)])
        v_pair = row_v[:, span(p, LANES)]
        tiles += [row_qk[:, span(2 * p, LANES)], jnp.where(low, v_pair, second), jnp.where(low, second, v_pair)]
    return jnp.concatenate(tiles, axis=1)


def pair_bias(b_all, p):
    low = lane_iota(1, LANES) < HD
    first, mid, last = (b_all[:, span(3 * p + n, LANES)] for n in range(3))
    return first, swap(jnp.where(low, last, mid)), jnp.where(low, mid, last)


def cut(x, shift):
    width = x.shape[1]
    return pltpu.roll(x, (width - shift) % width, 1)[:, LO]


def rotation(near_ref, far_ref, block, cos_ref, sa_ref, sb_ref):
    in_head = lane_iota(NT, LANES) % HD
    near, far = near_ref[...], far_ref[pl.ds(block, 1), :]
    near_s, far_s = pltpu.roll(near, LANES - ROT, 1), pltpu.roll(far, LANES - ROT, 1)
    sin_t = near_s * far + near * far_s
    cos_ref[...] = jnp.where(in_head < ROT, near * far - near_s * far_s, 1.0)
    sa_ref[...] = jnp.where(in_head < TURN, -sin_t, 0.0)
    sb_ref[...] = jnp.where((in_head >= TURN) & (in_head < ROT), sin_t, 0.0)


def angle_table(positions):
    lane = np.arange(LANES) % HD
    freq = ROPE_BASE ** (-(2.0 * (lane % TURN)) / ROT)
    angles = positions[:, None] * freq[None, :]
    return np.where(lane < ROT, np.cos(angles), np.sin(angles)).astype(np.float32)


def part_bits(p):
    return {'c': p % 2, 'x': p // 2 % 2, 'y': p // 4 % 2, 'z': p // 8}


class Where:
    def __init__(self):
        self.z = lax.axis_index('dp')
        self.me = lax.axis_index('sp')
        self.bit = part_bits(self.z * SP + self.me)

    def flip(self, names):
        step = {'c': 1, 'x': 2, 'y': 4}
        z, sp = self.z, self.me
        for n in names:
            if n == 'z':
                z = 1 - z
            else:
                sp = sp + step[n] * (1 - 2 * self.bit[n])
        return z, sp


class Summed:
    def __init__(self, at, order, refs, send_sem, recv_sem):
        self.at, self.order, self.buf, self.lands, self.send_sem, self.recv_sem = at, order, refs[0], refs[1:], send_sem, recv_sem

    def place(self, p):
        bits = part_bits(p)
        return tuple(bits[n] for n in self.order)

    def put(self, p, rows, value):
        self.buf[self.place(p) + (rows,)] = value

    def copy(self, k):
        mine = [self.at.bit[n] for n in self.order]
        return pltpu.make_async_remote_copy(src_ref=self.buf.at[tuple(mine[:k]) + (1 - mine[k],)], dst_ref=self.lands[k],
                                            send_sem=self.send_sem.at[k], recv_sem=self.recv_sem.at[k],
                                            device_id=self.at.flip(self.order[k]), device_id_type=MESH)

    def start(self, k):
        self.copy(k).start()

    def land(self, k):
        self.copy(k).wait_recv()
        mine = tuple(self.at.bit[n] for n in self.order[:k + 1])
        rest = len(self.order) - 1 - k
        for n in range(2 ** rest):
            sub = tuple((n >> m) % 2 for m in reversed(range(rest)))
            self.buf[mine + sub] = self.buf[mine + sub] + self.lands[k][sub if sub else ...]

    def step(self, k):
        self.land(k)
        self.start(k + 1)

    def result(self):
        return self.buf[tuple(self.at.bit[n] for n in self.order)]

    def drain(self):
        for k in range(len(self.order)):
            self.copy(k).wait_send()


PEERS = ('x', 'y', 'xc', 'yc', 'xy', 'xyc', 'c')
ORDERS = ('czxy', 'czxy', 'czyx', 'czxy', 'czyx', 'cxzy', 'cyzx', 'czxy')
SUM_SHAPES = ((2 * SLICE, D), (2 * SLICE, D), (LANES, D)) + ((SLICE, D),) * 4 + ((SUB, LANES),)


def exchange(at, b, src, dst, sems):
    out = []
    for k, names in enumerate(PEERS):
        z, sp = at.flip(names)
        out.append(pltpu.make_async_remote_copy(src_ref=src.at[b, sp], dst_ref=dst.at[b, at.me], send_sem=sems[0].at[b, k], recv_sem=sems[1].at[b, k],
                                                device_id=(z, sp), device_id_type=MESH))
    return out


def layer(x_ref, g_ref, g1_ref, s1_ref, g2_ref, s2_ref, wt_ref, bqkv_ref, wd_ref, bd_ref, wi_hbm, bi_ref, wo_hbm, bo_ref, near_ref, far_ref,
          out_hbm, gx_hbm, gwi_ref, gwo_ref, gqkv_ref, gwd_ref, tail_ref,
          out_ref, gx_ref, cos_ref, sa_ref, sb_ref, wi_ref, wo_ref, wp_ref, ctx_ref, dqkv_ref, h2t_ref, gt_ref, buf_ref, in_ref, z_ref, res_ref, dh2_ref, gbi_ref, xt_ref, sdp_ref, acc_ref,
          sums_refs, load_sem, store_sem, out_sems, back_sems, sum_send, sum_recv):
    at = Where()
    me = at.me
    loads = [pltpu.make_async_copy(src, dst, load_sem.at[n]) for n, (src, dst) in enumerate(((wi_hbm, wi_ref), (wo_hbm, wo_ref)))]
    for load in loads:
        load.start()
    barrier = pltpu.get_barrier_semaphore()
    for names in PEERS + ('z',):
        pl.semaphore_signal(barrier, inc=1, device_id=at.flip(names), device_id_type=MESH)
    sums = [Summed(at, order, refs, sum_send.at[n], sum_recv.at[n]) for n, (order, refs) in enumerate(zip(ORDERS, sums_refs))]
    early, tail = sums[:3], sums[3:]
    sum_w = sums[:2]
    sum_wo = sums[2]
    low = lane_iota(NT, LANES) < HD
    rotation(near_ref, far_ref, me, cos_ref, sa_ref, sb_ref)
    fold_weights(wt_ref, wp_ref)
    b_all = row(bqkv_ref)

    def send_heads(b):
        for copy in exchange(at, b, buf_ref, in_ref, out_sems):
            copy.start()

    for b in range(NB):
        rows = span(b, NT)
        x = x_ref[rows, :].astype(F32)
        hat, _ = layer_hat(x)
        h_b = (hat * row(g1_ref) + row(s1_ref)).astype(BF16)
        qk = dot_tb(h_b, wp_ref[:2 * D, :])
        vv = dot_tb(h_b, wp_ref[2 * D:, :])
        dc = dot_tb(g_ref[rows, :], wd_ref[...])
        for p in range(PAIRS):
            bias_a, bias_b, bias_v = pair_bias(b_all, p)
            v_pair = vv[:, span(p, LANES)] + bias_v
            d_pair = dc[:, span(p, LANES)]
            for h, bias, second in ((2 * p, bias_a, jnp.where(low, v_pair, swap(d_pair))), (2 * p + 1, bias_b, jnp.where(low, swap(v_pair), d_pair))):
                t = qk[:, span(h, LANES)] + bias
                t = t * cos_ref[...] + pltpu.roll(t, TURN_BACK, 1) * sa_ref[...] + pltpu.roll(t, TURN, 1) * sb_ref[...]
                buf_ref[b, h, :, LO] = t.astype(BF16)
                buf_ref[b, h, :, HI] = second.astype(BF16)
        if b == 0:
            pl.semaphore_wait(barrier, len(PEERS) + 1)
            send_heads(b)
        in_ref[b, me] = buf_ref[b, me]
        ctx_ref[rows, :] = (hat * row(g2_ref) + row(s2_ref)).astype(BF16)
        res_ref[rows, :] = x + row(bd_ref) + row(bo_ref)

    h2t_ref[...] = ctx_ref[...].T
    gt_ref[...] = g_ref[...].T
    b_in = row(bi_ref)
    for load in loads:
        load.wait()
    for c in range(N_CHUNK):
        cols = span(c, CHUNK)
        pre = dot(ctx_ref[...], wi_ref[:, cols]) + b_in[:, cols]
        d_act = dot_tb(g_ref[...], wo_ref[cols, :])
        cdf = 0.5 * (1.0 + lax.erf(pre * math.sqrt(0.5)))
        pdf = jnp.exp(-0.5 * pre * pre) * (1.0 / math.sqrt(2.0 * math.pi))
        act = (pre * cdf).astype(BF16)
        d_pre = d_act * (cdf + pre * pdf)
        d_pre_bf = d_pre.astype(BF16)
        gbi_ref[:, cols] = jnp.broadcast_to(col_sum(d_pre), (SUB, CHUNK))
        g_wi = dot(h2t_ref[...], d_pre_bf)
        for p in range(PARTS):
            sum_w[c // 2].put(p, span(c % 2, SLICE), g_wi[span(p, SLICE)])
        if c % 2:
            sum_w[c // 2].start(0)
        g_wo = dot(gt_ref[...], act)
        for q in range(CHUNK // LANES):
            where = sum_wo.place(PARTS // N_CHUNK * c + q)
            for k in range(D // LANES):
                sum_wo.buf[where + (slice(None), span(k, LANES))] = g_wo[span(k, LANES), span(q, LANES)]
        res_ref[...] += dot(act, wo_ref[cols, :])
        d_h = dot_tb(d_pre_bf, wi_ref[:, cols])
        if c == N_CHUNK - 2:
            send_heads(1)
        if c == 0:
            dh2_ref[...] = d_h
        else:
            dh2_ref[...] += d_h
    sum_wo.start(0)
    sum_w[0].step(0)
    zero_row = jnp.zeros((1, D), F32)
    g_ln2 = g_ln2_b = g_b_dense = zero_row
    for b in range(NB):
        rows = span(b, NT)
        hat, _ = layer_hat(x_ref[rows, :].astype(F32))
        d_h = dh2_ref[rows, :]
        g_ln2 += col_sum(d_h * hat)
        g_ln2_b += col_sum(d_h)
        g_b_dense += col_sum(g_ref[rows, :].astype(F32))
        dh2_ref[rows, :] = d_h * row(g2_ref)

    keep = lax.broadcasted_iota(jnp.int32, (NT, NT), 0) <= lane_iota(NT, NT)
    zero_t = jnp.zeros((HD, NT), BF16)
    s_cols, p_cols = span(0, NT), span(1, NT)

    def one_sequence(b, carry):
        for copy in exchange(at, b, buf_ref, in_ref, out_sems):
            copy.wait()
        for j in range(SP):
            xt_ref[:, span(j, NT)] = in_ref[b, j].T
        for i in reversed(range(SP)):
            cols = span(i, NT)
            q_t = xt_ref[span(0, HD), cols] * BF16(SCALE)
            dc_t = xt_ref[span(3, HD), cols]
            w_s = jnp.concatenate([zero_t, q_t, zero_t, zero_t], axis=0)
            w_p = jnp.concatenate([zero_t, zero_t, dc_t, zero_t], axis=0)
            w_sp = jnp.concatenate([w_s, w_p], axis=1)
            q_n = jnp.where(low, in_ref[b, i, :, LO] * BF16(SCALE), BF16(0.0))
            dc_n = jnp.where(low, BF16(0.0), in_ref[b, i, :, HI])
            w_acc = jnp.concatenate([q_n, dc_n], axis=0)
            tops = []
            for j in range(i + 1):
                kv = span(j, NT)
                both = dot(in_ref[b, j], w_sp)
                s = both[:, s_cols]
                if j == i:
                    s = jnp.where(keep, s, -1e30)
                sdp_ref[kv, s_cols] = s
                sdp_ref[kv, p_cols] = both[:, p_cols]
                part = fold(s, jnp.max)
                tops = [jnp.maximum(tops[0], part)] if tops else [part]
            top = jnp.max(tops[0], axis=0, keepdims=True)
            total = jnp.zeros((SUB, NT), F32)
            inner = jnp.zeros((SUB, NT), F32)
            for j in range(i + 1):
                kv = span(j, NT)
                e = jnp.exp(sdp_ref[kv, s_cols] - top)
                sdp_ref[kv, s_cols] = e
                total += fold(e, jnp.sum)
                inner += fold(e * sdp_ref[kv, p_cols], jnp.sum)
            inv = 1.0 / col_sum(total)
            delta = col_sum(inner) * inv
            ctx_t = jnp.zeros((HD, NT), F32)
            dq_t = jnp.zeros((HD, NT), F32)
            for j in range(i + 1):
                kv = span(j, NT)
                prob = sdp_ref[kv, s_cols] * inv
                prob_bf = prob.astype(BF16)
                ds_bf = (prob * (sdp_ref[kv, p_cols] - delta)).astype(BF16)
                ctx_t += dot(xt_ref[span(2, HD), kv], prob_bf)
                dq_t += dot(xt_ref[span(1, HD), kv], ds_bf)
                step = dot(jnp.concatenate([ds_bf, prob_bf], axis=1), w_acc)
                if i == SP - 1:
                    acc_ref[kv, :] = step
                else:
                    acc_ref[kv, :] += step
            nat = jnp.concatenate([dq_t * SCALE, ctx_t], axis=0).T
            acc = acc_ref[cols, :]
            buf_ref[b, i, :, LO] = jnp.where(low, nat, swap(acc)).astype(BF16)
            buf_ref[b, i, :, HI] = jnp.where(low, swap(nat), acc).astype(BF16)
            if i == SP - 3:
                @pl.when(b == 0)
                def _():
                    for s in early[1:]:
                        s.step(0)
                    send_heads(2)
        for copy in exchange(at, b, buf_ref, z_ref, back_sems):
            copy.start()
        z_ref[b, me] = buf_ref[b, me]
        return carry

    lax.fori_loop(0, NB, one_sequence, 0)

    def arrive(b):
        rows = span(b, NT)
        if b == NB - 1:
            for s in early:
                s.step(1)
        for copy in exchange(at, b, buf_ref, z_ref, back_sems):
            copy.wait()
        sums_qk, sums_v = [], []
        for p in range(PAIRS):
            seconds = []
            for h in (2 * p, 2 * p + 1):
                t = z_ref[b, h, :, LO].astype(F32)
                t = t * cos_ref[...] - pltpu.roll(t, TURN_BACK, 1) * sa_ref[...] - pltpu.roll(t, TURN, 1) * sb_ref[...]
                sums_qk.append(col_sum(t))
                dqkv_ref[rows, span(h, LANES)] = t.astype(BF16)
                seconds.append(z_ref[b, h, :, HI].astype(F32))
            ctx_ref[rows, span(p, LANES)] = jnp.where(low, seconds[0], swap(seconds[1])).astype(BF16)
            dv_pair = jnp.where(low, swap(seconds[0]), seconds[1])
            dqkv_ref[rows, span(2 * NH // 2 + p, LANES)] = dv_pair.astype(BF16)
            sums_v.append(col_sum(dv_pair))
        hat, inv_std = layer_hat(x_ref[rows, :].astype(F32))
        h1_t = (hat * row(g1_ref) + row(s1_ref)).astype(BF16).T
        ctx_t = ctx_ref[rows, :].T
        for k in range(4):
            block = span(k, D)
            term = dot(h1_t, dqkv_ref[rows, block]) if k < 3 else dot(ctx_t, g_ref[rows, :])
            if b:
                sdp_ref[block, :] += term
            else:
                sdp_ref[block, :] = term
        return hat, inv_std, jnp.concatenate(sums_qk, axis=1), jnp.concatenate(sums_v, axis=1)

    def finish(b, hat, inv_std):
        rows = span(b, NT)
        d_h1 = dot(dqkv_ref[rows, :], wp_ref[...])
        d_hat = d_h1 * row(g1_ref) + dh2_ref[rows, :]
        d_x = inv_std * (d_hat - jnp.mean(d_hat, axis=-1, keepdims=True) - hat * jnp.mean(d_hat * hat, axis=-1, keepdims=True))
        gx_ref[rows, :] = (g_ref[rows, :].astype(F32) + d_x).astype(BF16)
        return col_sum(d_h1 * hat), col_sum(d_h1)

    def forward(b):
        rows = span(b, NT)
        out_ref[rows, :] = (res_ref[rows, :] + dot(ctx_ref[rows, :], wd_ref[...])).astype(BF16)

    g_ln1 = g_ln1_b = zero_row
    gb_qk, gb_v = jnp.zeros((1, 2 * D), F32), zero_row
    for b in range(NB):
        hat, inv_std, part_qk, part_v = arrive(b)
        gb_qk += part_qk
        gb_v += part_v
        if b == NB - 1:
            for p in range(PARTS):
                for k in range(3):
                    tail[k].put(p, slice(None), sdp_ref[D * k + SLICE * p:D * k + SLICE * p + SLICE, :])
            for s in tail[:3]:
                s.start(0)
        part_g, part_b = finish(b, hat, inv_std)
        g_ln1 += part_g
        g_ln1_b += part_b
        if b < NB - 1:
            forward(b)

    store_gx = pltpu.make_async_copy(gx_ref, gx_hbm, store_sem.at[0])
    store_gx.start()
    five = jnp.concatenate([g_ln1, g_ln1_b, g_ln2, g_ln2_b, g_b_dense] + [zero_row] * 3, axis=0)
    g_bqkv = jnp.broadcast_to(pair_lanes(gb_qk, gb_v), (SUB, QKV))
    line = lax.broadcasted_iota(jnp.int32, (SUB, LANES), 0)
    for p in range(PARTS):
        tail[3].put(p, slice(None), sdp_ref[QKV + SLICE * p:QKV + SLICE * p + SLICE, :])
        small = jnp.where(line == ROW_B_IN, gbi_ref[:, span(p, LANES)], cut(five, SLICE * p))
        tail[4].put(p, slice(None), jnp.where(line == ROW_B_QKV, cut(g_bqkv, 3 * SLICE * p), small))
    for s in tail[3:]:
        s.start(0)
    forward(NB - 1)
    store_out = pltpu.make_async_copy(out_ref, out_hbm, store_sem.at[1])
    store_out.start()

    for s in tail:
        s.step(0)
    for s in early:
        s.step(2)
    for s in tail:
        s.step(1)
    for s in early:
        s.land(3)
    for c in range(N_CHUNK):
        gwi_ref[:, span(c, CHUNK)] = sum_w[c // 2].result()[span(c % 2, SLICE)]
    g_wo = sum_wo.result()
    for k in range(D // LANES):
        gwo_ref[:, span(k, LANES)] = g_wo[:, span(k, LANES)].T
    for s in tail:
        s.step(2)
    for s in tail:
        s.land(3)
    for k in range(3):
        gqkv_ref[:, span(k, D)] = tail[k].result()
    gwd_ref[...] = tail[3].result()
    tail_ref[...] = tail[4].result()
    store_gx.wait()
    store_out.wait()
    for s in sums:
        s.drain()


def write_out(out_in, gx_in, gwi_in, gwo_in, gqkv_in, gwd_in, tail_in,
              out_ref, gx_ref, g1_ref, s1_ref, g2_ref, s2_ref, gqkv_ref, gbqkv_ref, gwd_ref, gbd_ref, gwi_ref, gbi_ref, gwo_ref, gbo_ref):
    out_ref[...] = out_in[...]
    gx_ref[...] = gx_in[...]
    gwi_ref[...] = gwi_in[...]
    gwo_ref[...] = gwo_in[...]
    gwd_ref[...] = gwd_in[...]
    for h in range(NH):
        tile = gqkv_in[:, span(h, LANES)]
        gqkv_ref[:, 0, h, :] = tile[:, :HD]
        gqkv_ref[:, 1, h, :] = tile[:, HD:]
        gqkv_ref[:, 2, h, :] = gqkv_in[:, span(2 * NH + h, HD)]
    for n, ref in enumerate((g1_ref, s1_ref, g2_ref, s2_ref, gbd_ref)):
        ref[...] = tail_in[n, :SLICE]
    gbo_ref[...] = tail_in[n, :SLICE]
    gbi_ref[...] = tail_in[ROW_B_IN, :]
    gbqkv_ref[...] = tail_in[ROW_B_QKV, :3 * SLICE]


def sds(shape, dtype):
    return jax.ShapeDtypeStruct(shape, dtype)


def halving(shape):
    return tuple(pltpu.VMEM((2,) * n + shape, F32) for n in reversed(range(5)))


def vmem(rows, cols, dtype):
    return pltpu.VMEM((rows, cols), dtype)


def solution(mesh):
    grad_axes = ('dp', 'sp')

    def device_step(hidden, grad_out, ln1_gain, ln1_bias, ln2_gain, ln2_bias, w_qkv, b_qkv, w_dense, b_dense, w_in, b_in, w_out, b_out):
        x = hidden.reshape(ROWS, D)
        g = grad_out.reshape(ROWS, D)
        wt = jnp.moveaxis(w_qkv, 0, -1).reshape(QKV, D)
        near = jnp.asarray(angle_table(np.arange(NT)))
        far = jnp.asarray(angle_table(NT * np.arange(SP)))
        dma = pltpu.SemaphoreType.DMA
        whole = pl.BlockSpec(memory_space=pltpu.VMEM)
        in_specs = [whole] * 16
        in_specs[10] = in_specs[12] = pl.BlockSpec(memory_space=pl.ANY)
        block = pltpu.VMEM((NB, SP, NT, 2 * LANES), BF16)
        peer_sems = (dma((NB, len(PEERS))),) * 2
        results = pl.pallas_call(
            layer,
            out_shape=(sds((ROWS, D), BF16), sds((ROWS, D), BF16), sds((SLICE, FF), F32), sds((LANES, D), F32), sds((SLICE, QKV), F32), sds((SLICE, D), F32), sds((SUB, LANES), F32)),
            in_specs=in_specs,
            out_specs=(in_specs[10],) * 2 + (whole,) * 5,
            scratch_shapes=[
                vmem(ROWS, D, BF16), vmem(ROWS, D, BF16), vmem(NT, LANES, F32), vmem(NT, LANES, F32), vmem(NT, LANES, F32), vmem(D, FF, BF16), vmem(FF, D, BF16), vmem(QKV, D, BF16), vmem(ROWS, D, BF16), vmem(ROWS, QKV, BF16), vmem(D, ROWS, BF16), vmem(D, ROWS, BF16),
                block, block, block, vmem(ROWS, D, F32), vmem(ROWS, D, F32), vmem(SUB, FF, F32),
                vmem(2 * LANES, SEQ, BF16), vmem(SEQ, 2 * NT, F32), vmem(SEQ, LANES, F32),
                tuple(halving(shape) for shape in SUM_SHAPES),
                dma((2,)), dma((2,)), peer_sems, peer_sems, dma((8, 4)), dma((8, 4)),
            ],
            compiler_params=pltpu.CompilerParams(vmem_limit_bytes=VMEM_LIMIT, collective_id=0, has_side_effects=True),
            cost_estimate=pl.CostEstimate(flops=56_000_000_000, bytes_accessed=12_000_000, transcendentals=10_000_000),
            name='layer',
        )(x, g, ln1_gain, ln1_bias, ln2_gain, ln2_bias, wt, b_qkv, w_dense, b_dense, w_in, b_in, w_out, b_out, near, far)

        part = sds((SLICE,), F32)
        tokens = sds((ROWS, D), BF16)
        final = list(pl.pallas_call(
            write_out,
            out_shape=(tokens, tokens, part, part, part, part, sds((SLICE, 3, NH, HD), F32), sds((3 * SLICE,), F32), sds((SLICE, D), F32), part,
                       sds((SLICE, FF), F32), sds((LANES,), F32), sds((LANES, D), F32), part),
            in_specs=[whole] * 7,
            out_specs=(whole,) * 14,
            name='write_out',
        )(*results))
        final[0] = final[0].reshape(hidden.shape)
        final[1] = final[1].reshape(hidden.shape)
        final[6] = jnp.swapaxes(final[6], 1, 2)
        return tuple(final)

    tok_spec = P('dp', 'sp', None)
    grad_spec = P(grad_axes)
    return jax.shard_map(device_step, mesh=mesh, in_specs=(tok_spec, tok_spec) + (P(),) * 12, out_specs=(tok_spec, tok_spec) + (grad_spec,) * 12, check_vma=False)
```

```python
import math
import jax
import jax.numpy as jnp
import numpy as np
from jax import lax
from jax.experimental import pallas as pl
from jax.experimental.pallas import tpu as pltpu
from jax.sharding import PartitionSpec as P

LN_EPS = 1e-5
ROPE_BASE = 10000.0
F32 = jnp.float32
BF16 = jnp.bfloat16
MESH = pl.DeviceIdType.MESH
VMEM_LIMIT = 67_043_328

NB, NT, D, NH, HD, FF = 3, 256, 512, 8, 64, 2048
ROWS = NB * NT
SP = 8
PARTS = 16
SEQ = SP * NT
CHUNK = 512
N_CHUNK = FF // CHUNK
SUB = 8
ROW_B_IN, ROW_B_QKV = 5, 6
LANES = 2 * HD
PAIRS = NH // 2
SLICE = D // PARTS
QKV = 3 * D
ROT = HD // 4
TURN = ROT // 2
TURN_BACK = LANES - TURN
LO = slice(0, LANES)
HI = slice(LANES, 2 * LANES)
SCALE = 1.0 / math.sqrt(HD)


def dot(a, b):
    return lax.dot_general(a, b, (((1,), (0,)), ((), ())), preferred_element_type=F32)


def dot_tb(a, b):
    return lax.dot_general(a, b, (((1,), (1,)), ((), ())), preferred_element_type=F32)


def span(index, size):
    return slice(size * index, size * (index + 1))


def lane_iota(rows, cols):
    return lax.broadcasted_iota(jnp.int32, (rows, cols), 1)


def swap(x):
    return pltpu.roll(x, HD, 1)


def row(ref):
    return ref[...].reshape(1, ref.shape[0])


def col_sum(x):
    return jnp.sum(x, axis=0, keepdims=True)


def fold(x, op):
    return op(x.reshape(NT // SUB, SUB, NT), axis=0)


def layer_hat(x):
    mean_val = jnp.mean(x, axis=-1, keepdims=True)
    centered = x - mean_val
    var_val = jnp.mean(centered * centered, axis=-1, keepdims=True)
    inv_std = lax.rsqrt(var_val + LN_EPS)
    return centered * inv_std, inv_std


def fold_weights(wt_ref, wp_ref):
    for h in range(NH):
        base = 3 * HD * h
        wp_ref[span(h, LANES), :] = wt_ref[base:base + LANES, :]
        wp_ref[span(2 * NH + h, HD), :] = wt_ref[base + LANES:base + LANES + HD, :]


def pair_lanes(row_qk, row_v):
    low = lane_iota(1, LANES) < HD
    tiles = []
    for p in range(PAIRS):
        second = swap(row_qk[:, span(2 * p + 1, LANES)])
        v_pair = row_v[:, span(p, LANES)]
        tiles += [row_qk[:, span(2 * p, LANES)], jnp.where(low, v_pair, second), jnp.where(low, second, v_pair)]
    return jnp.concatenate(tiles, axis=1)


def pair_bias(b_all, p):
    low = lane_iota(1, LANES) < HD
    first, mid, last = (b_all[:, span(3 * p + n, LANES)] for n in range(3))
    return first, swap(jnp.where(low, last, mid)), jnp.where(low, mid, last)


def cut(x, shift):
    width = x.shape[1]
    return pltpu.roll(x, (width - shift) % width, 1)[:, LO]


def rotation(near_ref, far_ref, block, cos_ref, sa_ref, sb_ref):
    in_head = lane_iota(NT, LANES) % HD
    near, far = near_ref[...], far_ref[pl.ds(block, 1), :]
    near_s, far_s = pltpu.roll(near, LANES - ROT, 1), pltpu.roll(far, LANES - ROT, 1)
    sin_t = near_s * far + near * far_s
    cos_ref[...] = jnp.where(in_head < ROT, near * far - near_s * far_s, 1.0)
    sa_ref[...] = jnp.where(in_head < TURN, -sin_t, 0.0)
    sb_ref[...] = jnp.where((in_head >= TURN) & (in_head < ROT), sin_t, 0.0)


def angle_table(positions):
    lane = np.arange(LANES) % HD
    freq = ROPE_BASE ** (-(2.0 * (lane % TURN)) / ROT)
    angles = positions[:, None] * freq[None, :]
    return np.where(lane < ROT, np.cos(angles), np.sin(angles)).astype(np.float32)


def part_bits(p):
    return {'c': p % 2, 'x': p // 2 % 2, 'y': p // 4 % 2, 'z': p // 8}


class Where:
    def __init__(self):
        self.z = lax.axis_index('dp')
        self.me = lax.axis_index('sp')
        self.bit = part_bits(self.z * SP + self.me)

    def flip(self, names):
        step = {'c': 1, 'x': 2, 'y': 4}
        z, sp = self.z, self.me
        for n in names:
            if n == 'z':
                z = 1 - z
            else:
                sp = sp + step[n] * (1 - 2 * self.bit[n])
        return z, sp


class Summed:
    def __init__(self, at, order, refs, send_sem, recv_sem):
        self.at, self.order, self.buf, self.lands, self.send_sem, self.recv_sem = at, order, refs[0], refs[1:], send_sem, recv_sem

    def place(self, p):
        bits = part_bits(p)
        return tuple(bits[n] for n in self.order)

    def put(self, p, rows, value):
        self.buf[self.place(p) + (rows,)] = value

    def copy(self, k):
        mine = [self.at.bit[n] for n in self.order]
        return pltpu.make_async_remote_copy(src_ref=self.buf.at[tuple(mine[:k]) + (1 - mine[k],)], dst_ref=self.lands[k],
                                            send_sem=self.send_sem.at[k], recv_sem=self.recv_sem.at[k],
                                            device_id=self.at.flip(self.order[k]), device_id_type=MESH)

    def start(self, k):
        self.copy(k).start()

    def land(self, k):
        self.copy(k).wait_recv()
        mine = tuple(self.at.bit[n] for n in self.order[:k + 1])
        rest = len(self.order) - 1 - k
        for n in range(2 ** rest):
            sub = tuple((n >> m) % 2 for m in reversed(range(rest)))
            self.buf[mine + sub] = self.buf[mine + sub] + self.lands[k][sub if sub else ...]

    def step(self, k):
        self.land(k)
        self.start(k + 1)

    def result(self):
        return self.buf[tuple(self.at.bit[n] for n in self.order)]

    def drain(self):
        for k in range(len(self.order)):
            self.copy(k).wait_send()


PEERS = ('x', 'y', 'xc', 'yc', 'xy', 'xyc', 'c')
ORDERS = ('czxy', 'czxy', 'czyx', 'czxy', 'czyx', 'cxzy', 'cyzx', 'czxy')
SUM_SHAPES = ((2 * SLICE, D), (2 * SLICE, D), (LANES, D)) + ((SLICE, D),) * 4 + ((SUB, LANES),)


def exchange(at, b, src, dst, sems):
    out = []
    for k, names in enumerate(PEERS):
        z, sp = at.flip(names)
        out.append(pltpu.make_async_remote_copy(src_ref=src.at[b, sp], dst_ref=dst.at[b, at.me], send_sem=sems[0].at[b, k], recv_sem=sems[1].at[b, k],
                                                device_id=(z, sp), device_id_type=MESH))
    return out


def layer(x_ref, g_ref, g1_ref, s1_ref, g2_ref, s2_ref, wt_ref, bqkv_ref, wd_ref, bd_ref, wi_hbm, bi_ref, wo_hbm, bo_ref, near_ref, far_ref,
          out_hbm, gx_hbm, gwi_ref, gwo_ref, gqkv_ref, gwd_ref, tail_ref,
          out_ref, gx_ref, cos_ref, sa_ref, sb_ref, wi_ref, wo_ref, wp_ref, ctx_ref, dqkv_ref, h2t_ref, gt_ref, buf_ref, in_ref, z_ref, res_ref, dh2_ref, gbi_ref, xt_ref, sdp_ref, acc_ref,
          sums_refs, load_sem, store_sem, out_sems, back_sems, sum_send, sum_recv):
    at = Where()
    me = at.me
    loads = [pltpu.make_async_copy(src, dst, load_sem.at[n]) for n, (src, dst) in enumerate(((wi_hbm, wi_ref), (wo_hbm, wo_ref)))]
    for load in loads:
        load.start()
    barrier = pltpu.get_barrier_semaphore()
    for names in PEERS + ('z',):
        pl.semaphore_signal(barrier, inc=1, device_id=at.flip(names), device_id_type=MESH)
    sums = [Summed(at, order, refs, sum_send.at[n], sum_recv.at[n]) for n, (order, refs) in enumerate(zip(ORDERS, sums_refs))]
    early, tail = sums[:3], sums[3:]
    sum_w = sums[:2]
    sum_wo = sums[2]
    low = lane_iota(NT, LANES) < HD
    rotation(near_ref, far_ref, me, cos_ref, sa_ref, sb_ref)
    fold_weights(wt_ref, wp_ref)
    b_all = row(bqkv_ref)

    def send_heads(b):
        for copy in exchange(at, b, buf_ref, in_ref, out_sems):
            copy.start()

    def send_tokens(b):
        for copy in exchange(at, b, buf_ref, z_ref, back_sems):
            copy.start()

    for b in range(NB):
        rows = span(b, NT)
        x = x_ref[rows, :].astype(F32)
        hat, _ = layer_hat(x)
        h_b = (hat * row(g1_ref) + row(s1_ref)).astype(BF16)
        qk = dot_tb(h_b, wp_ref[:2 * D, :])
        vv = dot_tb(h_b, wp_ref[2 * D:, :])
        dc = dot_tb(g_ref[rows, :], wd_ref[...])
        for p in range(PAIRS):
            bias_a, bias_b, bias_v = pair_bias(b_all, p)
            v_pair = vv[:, span(p, LANES)] + bias_v
            d_pair = dc[:, span(p, LANES)]
            for h, bias, second in ((2 * p, bias_a, jnp.where(low, v_pair, swap(d_pair))), (2 * p + 1, bias_b, jnp.where(low, swap(v_pair), d_pair))):
                t = qk[:, span(h, LANES)] + bias
                t = t * cos_ref[...] + pltpu.roll(t, TURN_BACK, 1) * sa_ref[...] + pltpu.roll(t, TURN, 1) * sb_ref[...]
                buf_ref[b, h, :, LO] = t.astype(BF16)
                buf_ref[b, h, :, HI] = second.astype(BF16)
        if b == 0:
            pl.semaphore_wait(barrier, len(PEERS) + 1)
            send_heads(b)
        in_ref[b, me] = buf_ref[b, me]
        ctx_ref[rows, :] = (hat * row(g2_ref) + row(s2_ref)).astype(BF16)
        res_ref[rows, :] = x + row(bd_ref) + row(bo_ref)

    h2t_ref[...] = ctx_ref[...].T
    gt_ref[...] = g_ref[...].T
    b_in = row(bi_ref)
    for load in loads:
        load.wait()
    for c in range(N_CHUNK):
        cols = span(c, CHUNK)
        pre = dot(ctx_ref[...], wi_ref[:, cols]) + b_in[:, cols]
        d_act = dot_tb(g_ref[...], wo_ref[cols, :])
        cdf = 0.5 * (1.0 + lax.erf(pre * math.sqrt(0.5)))
        pdf = jnp.exp(-0.5 * pre * pre) * (1.0 / math.sqrt(2.0 * math.pi))
        act = (pre * cdf).astype(BF16)
        d_pre = d_act * (cdf + pre * pdf)
        d_pre_bf = d_pre.astype(BF16)
        gbi_ref[:, cols] = jnp.broadcast_to(col_sum(d_pre), (SUB, CHUNK))
        g_wi = dot(h2t_ref[...], d_pre_bf)
        for p in range(PARTS):
            sum_w[c // 2].put(p, span(c % 2, SLICE), g_wi[span(p, SLICE)])
        if c % 2:
            sum_w[c // 2].start(0)
        g_wo = dot(gt_ref[...], act)
        for q in range(CHUNK // LANES):
            where = sum_wo.place(PARTS // N_CHUNK * c + q)
            for k in range(D // LANES):
                sum_wo.buf[where + (slice(None), span(k, LANES))] = g_wo[span(k, LANES), span(q, LANES)]
        res_ref[...] += dot(act, wo_ref[cols, :])
        d_h = dot_tb(d_pre_bf, wi_ref[:, cols])
        if c == N_CHUNK - 2:
            send_heads(1)
        if c == 0:
            dh2_ref[...] = d_h
        else:
            dh2_ref[...] += d_h
    sum_wo.start(0)
    sum_w[0].step(0)
    zero_row = jnp.zeros((1, D), F32)
    g_ln2 = g_ln2_b = g_b_dense = zero_row
    for b in range(NB):
        rows = span(b, NT)
        hat, _ = layer_hat(x_ref[rows, :].astype(F32))
        d_h = dh2_ref[rows, :]
        g_ln2 += col_sum(d_h * hat)
        g_ln2_b += col_sum(d_h)
        g_b_dense += col_sum(g_ref[rows, :].astype(F32))
        dh2_ref[rows, :] = d_h * row(g2_ref)

    keep = lax.broadcasted_iota(jnp.int32, (NT, NT), 0) <= lane_iota(NT, NT)
    zero_t = jnp.zeros((HD, NT), BF16)
    s_cols, p_cols = span(0, NT), span(1, NT)

    def one_sequence(b, carry):
        for copy in exchange(at, b, buf_ref, in_ref, out_sems):
            copy.wait()
        for j in range(SP):
            xt_ref[:, span(j, NT)] = in_ref[b, j].T
        for i in reversed(range(SP)):
            cols = span(i, NT)
            q_t = xt_ref[span(0, HD), cols] * BF16(SCALE)
            dc_t = xt_ref[span(3, HD), cols]
            w_s = jnp.concatenate([zero_t, q_t, zero_t, zero_t], axis=0)
            w_p = jnp.concatenate([zero_t, zero_t, dc_t, zero_t], axis=0)
            w_sp = jnp.concatenate([w_s, w_p], axis=1)
            q_n = jnp.where(low, in_ref[b, i, :, LO] * BF16(SCALE), BF16(0.0))
            dc_n = jnp.where(low, BF16(0.0), in_ref[b, i, :, HI])
            w_acc = jnp.concatenate([q_n, dc_n], axis=0)
            tops = []
            for j in range(i + 1):
                kv = span(j, NT)
                both = dot(in_ref[b, j], w_sp)
                s = both[:, s_cols]
                if j == i:
                    s = jnp.where(keep, s, -1e30)
                sdp_ref[kv, s_cols] = s
                sdp_ref[kv, p_cols] = both[:, p_cols]
                part = fold(s, jnp.max)
                tops = [jnp.maximum(tops[0], part)] if tops else [part]
            top = jnp.max(tops[0], axis=0, keepdims=True)
            total = jnp.zeros((SUB, NT), F32)
            inner = jnp.zeros((SUB, NT), F32)
            for j in range(i + 1):
                kv = span(j, NT)
                e = jnp.exp(sdp_ref[kv, s_cols] - top)
                sdp_ref[kv, s_cols] = e
                total += fold(e, jnp.sum)
                inner += fold(e * sdp_ref[kv, p_cols], jnp.sum)
            inv = 1.0 / col_sum(total)
            delta = col_sum(inner) * inv
            ctx_t = jnp.zeros((HD, NT), F32)
            dq_t = jnp.zeros((HD, NT), F32)
            for j in range(i + 1):
                kv = span(j, NT)
                prob = sdp_ref[kv, s_cols] * inv
                prob_bf = prob.astype(BF16)
                ds_bf = (prob * (sdp_ref[kv, p_cols] - delta)).astype(BF16)
                ctx_t += dot(xt_ref[span(2, HD), kv], prob_bf)
                dq_t += dot(xt_ref[span(1, HD), kv], ds_bf)
                step = dot(jnp.concatenate([ds_bf, prob_bf], axis=1), w_acc)
                if i == SP - 1:
                    acc_ref[kv, :] = step
                else:
                    acc_ref[kv, :] += step
            nat = jnp.concatenate([dq_t * SCALE, ctx_t], axis=0).T
            acc = acc_ref[cols, :]
            buf_ref[b, i, :, LO] = jnp.where(low, nat, swap(acc)).astype(BF16)
            buf_ref[b, i, :, HI] = jnp.where(low, swap(nat), acc).astype(BF16)
            if i == SP - 3:
                @pl.when(b == 0)
                def _():
                    for s in early[1:]:
                        s.step(0)
                    send_heads(2)

                @pl.when(b > 0)
                def _():
                    send_tokens(b - 1)
        z_ref[b, me] = buf_ref[b, me]
        return carry

    lax.fori_loop(0, NB, one_sequence, 0)
    send_tokens(NB - 1)

    def arrive(b):
        rows = span(b, NT)
        if b == NB - 1:
            for s in early:
                s.step(1)
        for copy in exchange(at, b, buf_ref, z_ref, back_sems):
            copy.wait()
        sums_qk, sums_v = [], []
        for p in range(PAIRS):
            seconds = []
            for h in (2 * p, 2 * p + 1):
                t = z_ref[b, h, :, LO].astype(F32)
                t = t * cos_ref[...] - pltpu.roll(t, TURN_BACK, 1) * sa_ref[...] - pltpu.roll(t, TURN, 1) * sb_ref[...]
                sums_qk.append(col_sum(t))
                dqkv_ref[rows, span(h, LANES)] = t.astype(BF16)
                seconds.append(z_ref[b, h, :, HI].astype(F32))
            ctx_ref[rows, span(p, LANES)] = jnp.where(low, seconds[0], swap(seconds[1])).astype(BF16)
            dv_pair = jnp.where(low, swap(seconds[0]), seconds[1])
            dqkv_ref[rows, span(2 * NH // 2 + p, LANES)] = dv_pair.astype(BF16)
            sums_v.append(col_sum(dv_pair))
        hat, inv_std = layer_hat(x_ref[rows, :].astype(F32))
        h1_t = (hat * row(g1_ref) + row(s1_ref)).astype(BF16).T
        ctx_t = ctx_ref[rows, :].T
        for k in range(4):
            block = span(k, D)
            term = dot(h1_t, dqkv_ref[rows, block]) if k < 3 else dot(ctx_t, g_ref[rows, :])
            if b == 0:
                sdp_ref[block, :] = term
            elif b < NB - 1:
                sdp_ref[block, :] += term
            else:
                term = sdp_ref[block, :] + term
                for p in range(PARTS):
                    tail[k].put(p, slice(None), term[span(p, SLICE)])
                tail[k].start(0)
        return hat, inv_std, jnp.concatenate(sums_qk, axis=1), jnp.concatenate(sums_v, axis=1)

    def finish(b, hat, inv_std):
        rows = span(b, NT)
        d_h1 = dot(dqkv_ref[rows, :], wp_ref[...])
        d_hat = d_h1 * row(g1_ref) + dh2_ref[rows, :]
        d_x = inv_std * (d_hat - jnp.mean(d_hat, axis=-1, keepdims=True) - hat * jnp.mean(d_hat * hat, axis=-1, keepdims=True))
        gx_ref[rows, :] = (g_ref[rows, :].astype(F32) + d_x).astype(BF16)
        return col_sum(d_h1 * hat), col_sum(d_h1)

    def forward(b):
        rows = span(b, NT)
        out_ref[rows, :] = (res_ref[rows, :] + dot(ctx_ref[rows, :], wd_ref[...])).astype(BF16)

    g_ln1 = g_ln1_b = zero_row
    gb_qk, gb_v = jnp.zeros((1, 2 * D), F32), zero_row
    for b in range(NB):
        hat, inv_std, part_qk, part_v = arrive(b)
        gb_qk += part_qk
        gb_v += part_v
        if b == NB - 1:
            for s in tail[:4]:
                s.step(0)
        part_g, part_b = finish(b, hat, inv_std)
        g_ln1 += part_g
        g_ln1_b += part_b
        if b < NB - 1:
            forward(b)

    store_gx = pltpu.make_async_copy(gx_ref, gx_hbm, store_sem.at[0])
    store_gx.start()
    five = jnp.concatenate([g_ln1, g_ln1_b, g_ln2, g_ln2_b, g_b_dense] + [zero_row] * 3, axis=0)
    g_bqkv = jnp.broadcast_to(pair_lanes(gb_qk, gb_v), (SUB, QKV))
    line = lax.broadcasted_iota(jnp.int32, (SUB, LANES), 0)
    for p in range(PARTS):
        small = jnp.where(line == ROW_B_IN, gbi_ref[:, span(p, LANES)], cut(five, SLICE * p))
        tail[4].put(p, slice(None), jnp.where(line == ROW_B_QKV, cut(g_bqkv, 3 * SLICE * p), small))
    tail[4].start(0)
    forward(NB - 1)
    store_out = pltpu.make_async_copy(out_ref, out_hbm, store_sem.at[1])
    store_out.start()

    tail[4].step(0)
    for s in early:
        s.step(2)
    for s in tail:
        s.step(1)
    for s in early:
        s.land(3)
    for c in range(N_CHUNK):
        gwi_ref[:, span(c, CHUNK)] = sum_w[c // 2].result()[span(c % 2, SLICE)]
    g_wo = sum_wo.result()
    for k in range(D // LANES):
        gwo_ref[:, span(k, LANES)] = g_wo[:, span(k, LANES)].T
    for s in tail:
        s.step(2)
    for s in tail:
        s.land(3)
    for k in range(3):
        gqkv_ref[:, span(k, D)] = tail[k].result()
    gwd_ref[...] = tail[3].result()
    tail_ref[...] = tail[4].result()
    store_gx.wait()
    store_out.wait()
    for s in sums:
        s.drain()


def write_out(out_in, gx_in, gwi_in, gwo_in, gqkv_in, gwd_in, tail_in,
              out_ref, gx_ref, g1_ref, s1_ref, g2_ref, s2_ref, gqkv_ref, gbqkv_ref, gwd_ref, gbd_ref, gwi_ref, gbi_ref, gwo_ref, gbo_ref, out_buf, gx_buf, sems):
    loads = [pltpu.make_async_copy(out_in, out_buf, sems.at[0]), pltpu.make_async_copy(gx_in, gx_buf, sems.at[1])]
    stores = [pltpu.make_async_copy(out_buf, out_ref, sems.at[0]), pltpu.make_async_copy(gx_buf, gx_ref, sems.at[1])]
    for load in loads:
        load.start()
    gwi_ref[...] = gwi_in[...]
    for load, store in zip(loads, stores):
        load.wait()
        store.start()
    gwo_ref[...] = gwo_in[...]
    gwd_ref[...] = gwd_in[...]
    for h in range(NH):
        tile = gqkv_in[:, span(h, LANES)]
        gqkv_ref[:, 0, h, :] = tile[:, :HD]
        gqkv_ref[:, 1, h, :] = tile[:, HD:]
        gqkv_ref[:, 2, h, :] = gqkv_in[:, span(2 * NH + h, HD)]
    for n, ref in enumerate((g1_ref, s1_ref, g2_ref, s2_ref, gbd_ref)):
        ref[...] = tail_in[n, :SLICE]
    gbo_ref[...] = tail_in[n, :SLICE]
    gbi_ref[...] = tail_in[ROW_B_IN, :]
    gbqkv_ref[...] = tail_in[ROW_B_QKV, :3 * SLICE]
    for store in stores:
        store.wait()


def sds(shape, dtype):
    return jax.ShapeDtypeStruct(shape, dtype)


def halving(shape):
    return tuple(pltpu.VMEM((2,) * n + shape, F32) for n in reversed(range(5)))


def vmem(rows, cols, dtype):
    return pltpu.VMEM((rows, cols), dtype)


def solution(mesh):
    grad_axes = ('dp', 'sp')

    def device_step(hidden, grad_out, ln1_gain, ln1_bias, ln2_gain, ln2_bias, w_qkv, b_qkv, w_dense, b_dense, w_in, b_in, w_out, b_out):
        x = hidden.reshape(ROWS, D)
        g = grad_out.reshape(ROWS, D)
        wt = jnp.moveaxis(w_qkv, 0, -1).reshape(QKV, D)
        near = jnp.asarray(angle_table(np.arange(NT)))
        far = jnp.asarray(angle_table(NT * np.arange(SP)))
        dma = pltpu.SemaphoreType.DMA
        whole = pl.BlockSpec(memory_space=pltpu.VMEM)
        in_specs = [whole] * 16
        in_specs[10] = in_specs[12] = pl.BlockSpec(memory_space=pl.ANY)
        block = pltpu.VMEM((NB, SP, NT, 2 * LANES), BF16)
        peer_sems = (dma((NB, len(PEERS))),) * 2
        results = pl.pallas_call(
            layer,
            out_shape=(sds((ROWS, D), BF16), sds((ROWS, D), BF16), sds((SLICE, FF), F32), sds((LANES, D), F32), sds((SLICE, QKV), F32), sds((SLICE, D), F32), sds((SUB, LANES), F32)),
            in_specs=in_specs,
            out_specs=(in_specs[10],) * 2 + (whole,) * 5,
            scratch_shapes=[
                vmem(ROWS, D, BF16), vmem(ROWS, D, BF16), vmem(NT, LANES, F32), vmem(NT, LANES, F32), vmem(NT, LANES, F32), vmem(D, FF, BF16), vmem(FF, D, BF16), vmem(QKV, D, BF16), vmem(ROWS, D, BF16), vmem(ROWS, QKV, BF16), vmem(D, ROWS, BF16), vmem(D, ROWS, BF16),
                block, block, block, vmem(ROWS, D, F32), vmem(ROWS, D, F32), vmem(SUB, FF, F32),
                vmem(2 * LANES, SEQ, BF16), vmem(SEQ, 2 * NT, F32), vmem(SEQ, LANES, F32),
                tuple(halving(shape) for shape in SUM_SHAPES),
                dma((2,)), dma((2,)), peer_sems, peer_sems, dma((8, 4)), dma((8, 4)),
            ],
            compiler_params=pltpu.CompilerParams(vmem_limit_bytes=VMEM_LIMIT, collective_id=0, has_side_effects=True),
            cost_estimate=pl.CostEstimate(flops=56_000_000_000, bytes_accessed=12_000_000, transcendentals=10_000_000),
            name='layer',
        )(x, g, ln1_gain, ln1_bias, ln2_gain, ln2_bias, wt, b_qkv, w_dense, b_dense, w_in, b_in, w_out, b_out, near, far)

        part = sds((SLICE,), F32)
        tokens = sds((ROWS, D), BF16)
        final = list(pl.pallas_call(
            write_out,
            out_shape=(tokens, tokens, part, part, part, part, sds((SLICE, 3, NH, HD), F32), sds((3 * SLICE,), F32), sds((SLICE, D), F32), part,
                       sds((SLICE, FF), F32), sds((LANES,), F32), sds((LANES, D), F32), part),
            in_specs=[in_specs[10]] * 2 + [whole] * 5,
            out_specs=(in_specs[10],) * 2 + (whole,) * 12,
            scratch_shapes=[vmem(ROWS, D, BF16), vmem(ROWS, D, BF16), dma((2,))],
            name='write_out',
        )(*results))
        final[0] = final[0].reshape(hidden.shape)
        final[1] = final[1].reshape(hidden.shape)
        final[6] = jnp.swapaxes(final[6], 1, 2)
        return tuple(final)

    tok_spec = P('dp', 'sp', None)
    grad_spec = P(grad_axes)
    return jax.shard_map(device_step, mesh=mesh, in_specs=(tok_spec, tok_spec) + (P(),) * 12, out_specs=(tok_spec, tok_spec) + (grad_spec,) * 12, check_vma=False)
```

```python
import math
import jax
import jax.numpy as jnp
import numpy as np
from jax import lax
from jax.experimental import pallas as pl
from jax.experimental.pallas import tpu as pltpu
from jax.sharding import PartitionSpec as P

LN_EPS = 1e-5
ROPE_BASE = 10000.0
F32 = jnp.float32
BF16 = jnp.bfloat16
MESH = pl.DeviceIdType.MESH
VMEM_LIMIT = 67_043_328

NB, NT, D, NH, HD, FF = 3, 256, 512, 8, 64, 2048
ROWS = NB * NT
SP = 8
PARTS = 16
SEQ = SP * NT
CHUNK = 512
N_CHUNK = FF // CHUNK
SUB = 8
ROW_B_IN, ROW_B_QKV = 5, 6
LANES = 2 * HD
PAIRS = NH // 2
SLICE = D // PARTS
QKV = 3 * D
ROT = HD // 4
TURN = ROT // 2
TURN_BACK = LANES - TURN
LO = slice(0, LANES)
HI = slice(LANES, 2 * LANES)
SCALE = 1.0 / math.sqrt(HD)


def dot(a, b):
    return lax.dot_general(a, b, (((1,), (0,)), ((), ())), preferred_element_type=F32)


def dot_tb(a, b):
    return lax.dot_general(a, b, (((1,), (1,)), ((), ())), preferred_element_type=F32)


def span(index, size):
    return slice(size * index, size * (index + 1))


def lane_iota(rows, cols):
    return lax.broadcasted_iota(jnp.int32, (rows, cols), 1)


def swap(x):
    return pltpu.roll(x, HD, 1)


def row(ref):
    return ref[...].reshape(1, ref.shape[0])


def col_sum(x):
    return jnp.sum(x, axis=0, keepdims=True)


def fold(x, op):
    return op(x.reshape(NT // SUB, SUB, NT), axis=0)


def layer_hat(x):
    mean_val = jnp.mean(x, axis=-1, keepdims=True)
    centered = x - mean_val
    var_val = jnp.mean(centered * centered, axis=-1, keepdims=True)
    inv_std = lax.rsqrt(var_val + LN_EPS)
    return centered * inv_std, inv_std


def fold_weights(wt_ref, wp_ref):
    for h in range(NH):
        base = 3 * HD * h
        wp_ref[span(h, LANES), :] = wt_ref[base:base + LANES, :]
        wp_ref[span(2 * NH + h, HD), :] = wt_ref[base + LANES:base + LANES + HD, :]


def pair_lanes(row_qk, row_v):
    low = lane_iota(1, LANES) < HD
    tiles = []
    for p in range(PAIRS):
        second = swap(row_qk[:, span(2 * p + 1, LANES)])
        v_pair = row_v[:, span(p, LANES)]
        tiles += [row_qk[:, span(2 * p, LANES)], jnp.where(low, v_pair, second), jnp.where(low, second, v_pair)]
    return jnp.concatenate(tiles, axis=1)


def pair_bias(b_all, p):
    low = lane_iota(1, LANES) < HD
    first, mid, last = (b_all[:, span(3 * p + n, LANES)] for n in range(3))
    return first, swap(jnp.where(low, last, mid)), jnp.where(low, mid, last)


def cut(x, shift):
    width = x.shape[1]
    return pltpu.roll(x, (width - shift) % width, 1)[:, LO]


def rotation(near_ref, far_ref, block, cos_ref, sa_ref, sb_ref):
    in_head = lane_iota(NT, LANES) % HD
    near, far = near_ref[...], far_ref[pl.ds(block, 1), :]
    near_s, far_s = pltpu.roll(near, LANES - ROT, 1), pltpu.roll(far, LANES - ROT, 1)
    sin_t = near_s * far + near * far_s
    cos_ref[...] = jnp.where(in_head < ROT, near * far - near_s * far_s, 1.0)
    sa_ref[...] = jnp.where(in_head < TURN, -sin_t, 0.0)
    sb_ref[...] = jnp.where((in_head >= TURN) & (in_head < ROT), sin_t, 0.0)


def angle_table(positions):
    lane = np.arange(LANES) % HD
    freq = ROPE_BASE ** (-(2.0 * (lane % TURN)) / ROT)
    angles = positions[:, None] * freq[None, :]
    return np.where(lane < ROT, np.cos(angles), np.sin(angles)).astype(np.float32)


def part_bits(p):
    return {'c': p % 2, 'x': p // 2 % 2, 'y': p // 4 % 2, 'z': p // 8}


class Where:
    def __init__(self):
        self.z = lax.axis_index('dp')
        self.me = lax.axis_index('sp')
        self.bit = part_bits(self.z * SP + self.me)

    def flip(self, names):
        step = {'c': 1, 'x': 2, 'y': 4}
        z, sp = self.z, self.me
        for n in names:
            if n == 'z':
                z = 1 - z
            else:
                sp = sp + step[n] * (1 - 2 * self.bit[n])
        return z, sp


class Summed:
    def __init__(self, at, order, refs, send_sem, recv_sem):
        self.at, self.order, self.buf, self.lands, self.send_sem, self.recv_sem = at, order, refs[0], refs[1:], send_sem, recv_sem

    def place(self, p):
        bits = part_bits(p)
        return tuple(bits[n] for n in self.order)

    def put(self, p, rows, value):
        self.buf[self.place(p) + (rows,)] = value

    def copy(self, k):
        mine = [self.at.bit[n] for n in self.order]
        return pltpu.make_async_remote_copy(src_ref=self.buf.at[tuple(mine[:k]) + (1 - mine[k],)], dst_ref=self.lands[k],
                                            send_sem=self.send_sem.at[k], recv_sem=self.recv_sem.at[k],
                                            device_id=self.at.flip(self.order[k]), device_id_type=MESH)

    def start(self, k):
        self.copy(k).start()

    def land(self, k):
        self.copy(k).wait_recv()
        mine = tuple(self.at.bit[n] for n in self.order[:k + 1])
        rest = len(self.order) - 1 - k
        for n in range(2 ** rest):
            sub = tuple((n >> m) % 2 for m in reversed(range(rest)))
            self.buf[mine + sub] = self.buf[mine + sub] + self.lands[k][sub if sub else ...]

    def step(self, k):
        self.land(k)
        self.start(k + 1)

    def result(self):
        return self.buf[tuple(self.at.bit[n] for n in self.order)]

    def drain(self):
        for k in range(len(self.order)):
            self.copy(k).wait_send()


PEERS = ('x', 'y', 'xc', 'yc', 'xy', 'xyc', 'c')
ORDERS = ('czxy', 'czxy', 'czyx', 'czxy', 'czyx', 'cxzy', 'cyzx', 'czxy')
SUM_SHAPES = ((2 * SLICE, D), (2 * SLICE, D), (LANES, D)) + ((SLICE, D),) * 4 + ((SUB, LANES),)


def exchange(at, b, src, dst, sems):
    out = []
    for k, names in enumerate(PEERS):
        z, sp = at.flip(names)
        out.append(pltpu.make_async_remote_copy(src_ref=src.at[b, sp], dst_ref=dst.at[b, at.me], send_sem=sems[0].at[b, k], recv_sem=sems[1].at[b, k],
                                                device_id=(z, sp), device_id_type=MESH))
    return out


def layer(x_ref, g_ref, g1_ref, s1_ref, g2_ref, s2_ref, wt_ref, bqkv_ref, wd_ref, bd_ref, wi_hbm, bi_ref, wo_hbm, bo_ref, near_ref, far_ref,
          out_hbm, gx_hbm, gwi_ref, gwo_ref, gqkv_ref, gwd_ref, tail_ref,
          out_ref, gx_ref, cos_ref, sa_ref, sb_ref, wi_ref, wo_ref, wp_ref, ctx_ref, dqkv_ref, h2t_ref, gt_ref, buf_ref, in_ref, z_ref, res_ref, dh2_ref, gbi_ref, xt_ref, sdp_ref, acc_ref,
          sums_refs, load_sem, store_sem, out_sems, back_sems, sum_send, sum_recv):
    at = Where()
    me = at.me
    loads = [pltpu.make_async_copy(src, dst, load_sem.at[n]) for n, (src, dst) in enumerate(((wi_hbm, wi_ref), (wo_hbm, wo_ref)))]
    for load in loads:
        load.start()
    barrier = pltpu.get_barrier_semaphore()
    for names in PEERS + ('z',):
        pl.semaphore_signal(barrier, inc=1, device_id=at.flip(names), device_id_type=MESH)
    sums = [Summed(at, order, refs, sum_send.at[n], sum_recv.at[n]) for n, (order, refs) in enumerate(zip(ORDERS, sums_refs))]
    early, tail = sums[:3], sums[3:]
    sum_w = sums[:2]
    sum_wo = sums[2]
    low = lane_iota(NT, LANES) < HD
    rotation(near_ref, far_ref, me, cos_ref, sa_ref, sb_ref)
    fold_weights(wt_ref, wp_ref)
    b_all = row(bqkv_ref)

    def send_heads(b):
        for copy in exchange(at, b, buf_ref, in_ref, out_sems):
            copy.start()

    def send_tokens(b):
        for copy in exchange(at, b, buf_ref, z_ref, back_sems):
            copy.start()

    for b in range(NB):
        rows = span(b, NT)
        x = x_ref[rows, :].astype(F32)
        hat, _ = layer_hat(x)
        h_b = (hat * row(g1_ref) + row(s1_ref)).astype(BF16)
        qk = dot_tb(h_b, wp_ref[:2 * D, :])
        vv = dot_tb(h_b, wp_ref[2 * D:, :])
        dc = dot_tb(g_ref[rows, :], wd_ref[...])
        for p in range(PAIRS):
            bias_a, bias_b, bias_v = pair_bias(b_all, p)
            v_pair = vv[:, span(p, LANES)] + bias_v
            d_pair = dc[:, span(p, LANES)]
            for h, bias, second in ((2 * p, bias_a, jnp.where(low, v_pair, swap(d_pair))), (2 * p + 1, bias_b, jnp.where(low, swap(v_pair), d_pair))):
                t = qk[:, span(h, LANES)] + bias
                t = t * cos_ref[...] + pltpu.roll(t, TURN_BACK, 1) * sa_ref[...] + pltpu.roll(t, TURN, 1) * sb_ref[...]
                buf_ref[b, h, :, LO] = t.astype(BF16)
                buf_ref[b, h, :, HI] = second.astype(BF16)
        if b == 0:
            pl.semaphore_wait(barrier, len(PEERS) + 1)
            send_heads(b)
        in_ref[b, me] = buf_ref[b, me]
        ctx_ref[rows, :] = (hat * row(g2_ref) + row(s2_ref)).astype(BF16)
        res_ref[rows, :] = x + row(bd_ref) + row(bo_ref)

    h2t_ref[...] = ctx_ref[...].T
    gt_ref[...] = g_ref[...].T
    b_in = row(bi_ref)
    for load in loads:
        load.wait()
    for c in range(N_CHUNK):
        cols = span(c, CHUNK)
        pre = dot(ctx_ref[...], wi_ref[:, cols]) + b_in[:, cols]
        d_act = dot_tb(g_ref[...], wo_ref[cols, :])
        cdf = 0.5 * (1.0 + lax.erf(pre * math.sqrt(0.5)))
        pdf = jnp.exp(-0.5 * pre * pre) * (1.0 / math.sqrt(2.0 * math.pi))
        act = (pre * cdf).astype(BF16)
        d_pre = d_act * (cdf + pre * pdf)
        d_pre_bf = d_pre.astype(BF16)
        gbi_ref[:, cols] = jnp.broadcast_to(col_sum(d_pre), (SUB, CHUNK))
        g_wi = dot(h2t_ref[...], d_pre_bf)
        for p in range(PARTS):
            sum_w[c // 2].put(p, span(c % 2, SLICE), g_wi[span(p, SLICE)])
        if c % 2:
            sum_w[c // 2].start(0)
        g_wo = dot(gt_ref[...], act)
        for q in range(CHUNK // LANES):
            where = sum_wo.place(PARTS // N_CHUNK * c + q)
            for k in range(D // LANES):
                sum_wo.buf[where + (slice(None), span(k, LANES))] = g_wo[span(k, LANES), span(q, LANES)]
        res_ref[...] += dot(act, wo_ref[cols, :])
        d_h = dot_tb(d_pre_bf, wi_ref[:, cols])
        if c == N_CHUNK - 2:
            send_heads(1)
        if c == 0:
            dh2_ref[...] = d_h
        else:
            dh2_ref[...] += d_h
    sum_wo.start(0)
    sum_w[0].step(0)
    zero_row = jnp.zeros((1, D), F32)
    g_ln2 = g_ln2_b = g_b_dense = zero_row
    for b in range(NB):
        rows = span(b, NT)
        hat, _ = layer_hat(x_ref[rows, :].astype(F32))
        d_h = dh2_ref[rows, :]
        g_ln2 += col_sum(d_h * hat)
        g_ln2_b += col_sum(d_h)
        g_b_dense += col_sum(g_ref[rows, :].astype(F32))
        dh2_ref[rows, :] = d_h * row(g2_ref)

    keep = lax.broadcasted_iota(jnp.int32, (NT, NT), 0) <= lane_iota(NT, NT)
    zero_t = jnp.zeros((HD, NT), BF16)
    s_cols, p_cols = span(0, NT), span(1, NT)

    def one_sequence(b, carry):
        for copy in exchange(at, b, buf_ref, in_ref, out_sems):
            copy.wait()
        for j in range(SP):
            xt_ref[:, span(j, NT)] = in_ref[b, j].T
        for i in reversed(range(SP)):
            cols = span(i, NT)
            q_t = xt_ref[span(0, HD), cols] * BF16(SCALE)
            dc_t = xt_ref[span(3, HD), cols]
            w_s = jnp.concatenate([zero_t, q_t, zero_t, zero_t], axis=0)
            w_p = jnp.concatenate([zero_t, zero_t, dc_t, zero_t], axis=0)
            w_sp = jnp.concatenate([w_s, w_p], axis=1)
            q_n = jnp.where(low, in_ref[b, i, :, LO] * BF16(SCALE), BF16(0.0))
            dc_n = jnp.where(low, BF16(0.0), in_ref[b, i, :, HI])
            w_acc = jnp.concatenate([q_n, dc_n], axis=0)
            tops = []
            for j in range(i + 1):
                kv = span(j, NT)
                both = dot(in_ref[b, j], w_sp)
                s = both[:, s_cols]
                if j == i:
                    s = jnp.where(keep, s, -1e30)
                sdp_ref[kv, s_cols] = s
                sdp_ref[kv, p_cols] = both[:, p_cols]
                part = fold(s, jnp.max)
                tops = [jnp.maximum(tops[0], part)] if tops else [part]
            top = jnp.max(tops[0], axis=0, keepdims=True)
            total = jnp.zeros((SUB, NT), F32)
            inner = jnp.zeros((SUB, NT), F32)
            for j in range(i + 1):
                kv = span(j, NT)
                e = jnp.exp(sdp_ref[kv, s_cols] - top)
                sdp_ref[kv, s_cols] = e
                total += fold(e, jnp.sum)
                inner += fold(e * sdp_ref[kv, p_cols], jnp.sum)
            inv = 1.0 / col_sum(total)
            delta = col_sum(inner) * inv
            ctx_t = jnp.zeros((HD, NT), F32)
            dq_t = jnp.zeros((HD, NT), F32)
            for j in range(i + 1):
                kv = span(j, NT)
                prob = sdp_ref[kv, s_cols] * inv
                prob_bf = prob.astype(BF16)
                ds_bf = (prob * (sdp_ref[kv, p_cols] - delta)).astype(BF16)
                ctx_t += dot(xt_ref[span(2, HD), kv], prob_bf)
                dq_t += dot(xt_ref[span(1, HD), kv], ds_bf)
                step = dot(jnp.concatenate([ds_bf, prob_bf], axis=1), w_acc)
                if i == SP - 1:
                    acc_ref[kv, :] = step
                else:
                    acc_ref[kv, :] += step
            nat = jnp.concatenate([dq_t * SCALE, ctx_t], axis=0).T
            acc = acc_ref[cols, :]
            buf_ref[b, i, :, LO] = jnp.where(low, nat, swap(acc)).astype(BF16)
            buf_ref[b, i, :, HI] = jnp.where(low, swap(nat), acc).astype(BF16)
            if i == SP - 3:
                @pl.when(b == 0)
                def _():
                    for s in early[1:]:
                        s.step(0)
                    send_heads(2)
        send_tokens(b)
        z_ref[b, me] = buf_ref[b, me]
        return carry

    lax.fori_loop(0, NB, one_sequence, 0)

    def arrive(b):
        rows = span(b, NT)
        if b == NB - 1:
            for s in early:
                s.step(1)
        for copy in exchange(at, b, buf_ref, z_ref, back_sems):
            copy.wait()
        sums_qk, sums_v = [], []
        for p in range(PAIRS):
            seconds = []
            for h in (2 * p, 2 * p + 1):
                t = z_ref[b, h, :, LO].astype(F32)
                t = t * cos_ref[...] - pltpu.roll(t, TURN_BACK, 1) * sa_ref[...] - pltpu.roll(t, TURN, 1) * sb_ref[...]
                sums_qk.append(col_sum(t))
                dqkv_ref[rows, span(h, LANES)] = t.astype(BF16)
                seconds.append(z_ref[b, h, :, HI].astype(F32))
            ctx_ref[rows, span(p, LANES)] = jnp.where(low, seconds[0], swap(seconds[1])).astype(BF16)
            dv_pair = jnp.where(low, swap(seconds[0]), seconds[1])
            dqkv_ref[rows, span(2 * NH // 2 + p, LANES)] = dv_pair.astype(BF16)
            sums_v.append(col_sum(dv_pair))
        hat, inv_std = layer_hat(x_ref[rows, :].astype(F32))
        h1_t = (hat * row(g1_ref) + row(s1_ref)).astype(BF16).T
        ctx_t = ctx_ref[rows, :].T
        for k in range(4):
            block = span(k, D)
            term = dot(h1_t, dqkv_ref[rows, block]) if k < 3 else dot(ctx_t, g_ref[rows, :])
            if b == 0:
                sdp_ref[block, :] = term
            elif b < NB - 1:
                sdp_ref[block, :] += term
            else:
                term = sdp_ref[block, :] + term
                for p in range(PARTS):
                    tail[k].put(p, slice(None), term[span(p, SLICE)])
                tail[k].start(0)
        return hat, inv_std, jnp.concatenate(sums_qk, axis=1), jnp.concatenate(sums_v, axis=1)

    def finish(b, hat, inv_std):
        rows = span(b, NT)
        d_h1 = dot(dqkv_ref[rows, :], wp_ref[...])
        d_hat = d_h1 * row(g1_ref) + dh2_ref[rows, :]
        d_x = inv_std * (d_hat - jnp.mean(d_hat, axis=-1, keepdims=True) - hat * jnp.mean(d_hat * hat, axis=-1, keepdims=True))
        gx_ref[rows, :] = (g_ref[rows, :].astype(F32) + d_x).astype(BF16)
        return col_sum(d_h1 * hat), col_sum(d_h1)

    def forward(b):
        rows = span(b, NT)
        out_ref[rows, :] = (res_ref[rows, :] + dot(ctx_ref[rows, :], wd_ref[...])).astype(BF16)

    g_ln1 = g_ln1_b = zero_row
    gb_qk, gb_v = jnp.zeros((1, 2 * D), F32), zero_row
    for b in range(NB):
        hat, inv_std, part_qk, part_v = arrive(b)
        gb_qk += part_qk
        gb_v += part_v
        if b == NB - 1:
            for s in tail[:4]:
                s.step(0)
        part_g, part_b = finish(b, hat, inv_std)
        g_ln1 += part_g
        g_ln1_b += part_b
        if b < NB - 1:
            forward(b)

    store_gx = pltpu.make_async_copy(gx_ref, gx_hbm, store_sem.at[0])
    store_gx.start()
    five = jnp.concatenate([g_ln1, g_ln1_b, g_ln2, g_ln2_b, g_b_dense] + [zero_row] * 3, axis=0)
    g_bqkv = jnp.broadcast_to(pair_lanes(gb_qk, gb_v), (SUB, QKV))
    line = lax.broadcasted_iota(jnp.int32, (SUB, LANES), 0)
    for p in range(PARTS):
        small = jnp.where(line == ROW_B_IN, gbi_ref[:, span(p, LANES)], cut(five, SLICE * p))
        tail[4].put(p, slice(None), jnp.where(line == ROW_B_QKV, cut(g_bqkv, 3 * SLICE * p), small))
    tail[4].start(0)
    forward(NB - 1)
    store_out = pltpu.make_async_copy(out_ref, out_hbm, store_sem.at[1])
    store_out.start()

    tail[4].step(0)
    for s in tail:
        s.step(1)
    for s in early:
        s.step(2)
    for s in tail:
        s.step(2)
    for s in early:
        s.land(3)
    for c in range(N_CHUNK):
        gwi_ref[:, span(c, CHUNK)] = sum_w[c // 2].result()[span(c % 2, SLICE)]
    g_wo = sum_wo.result()
    for k in range(D // LANES):
        gwo_ref[:, span(k, LANES)] = g_wo[:, span(k, LANES)].T
    for s in tail:
        s.land(3)
    for k in range(3):
        gqkv_ref[:, span(k, D)] = tail[k].result()
    gwd_ref[...] = tail[3].result()
    tail_ref[...] = tail[4].result()
    store_gx.wait()
    store_out.wait()
    for s in sums:
        s.drain()


def write_out(out_in, gx_in, gwi_in, gwo_in, gqkv_in, gwd_in, tail_in,
              out_ref, gx_ref, g1_ref, s1_ref, g2_ref, s2_ref, gqkv_ref, gbqkv_ref, gwd_ref, gbd_ref, gwi_ref, gbi_ref, gwo_ref, gbo_ref):
    out_ref[...] = out_in[...]
    gx_ref[...] = gx_in[...]
    gwi_ref[...] = gwi_in[...]
    gwo_ref[...] = gwo_in[...]
    gwd_ref[...] = gwd_in[...]
    for h in range(NH):
        tile = gqkv_in[:, span(h, LANES)]
        gqkv_ref[:, 0, h, :] = tile[:, :HD]
        gqkv_ref[:, 1, h, :] = tile[:, HD:]
        gqkv_ref[:, 2, h, :] = gqkv_in[:, span(2 * NH + h, HD)]
    for n, ref in enumerate((g1_ref, s1_ref, g2_ref, s2_ref, gbd_ref)):
        ref[...] = tail_in[n, :SLICE]
    gbo_ref[...] = tail_in[n, :SLICE]
    gbi_ref[...] = tail_in[ROW_B_IN, :]
    gbqkv_ref[...] = tail_in[ROW_B_QKV, :3 * SLICE]


def sds(shape, dtype):
    return jax.ShapeDtypeStruct(shape, dtype)


def halving(shape):
    return tuple(pltpu.VMEM((2,) * n + shape, F32) for n in reversed(range(5)))


def vmem(rows, cols, dtype):
    return pltpu.VMEM((rows, cols), dtype)


def solution(mesh):
    grad_axes = ('dp', 'sp')

    def device_step(hidden, grad_out, ln1_gain, ln1_bias, ln2_gain, ln2_bias, w_qkv, b_qkv, w_dense, b_dense, w_in, b_in, w_out, b_out):
        x = hidden.reshape(ROWS, D)
        g = grad_out.reshape(ROWS, D)
        wt = jnp.moveaxis(w_qkv, 0, -1).reshape(QKV, D)
        near = jnp.asarray(angle_table(np.arange(NT)))
        far = jnp.asarray(angle_table(NT * np.arange(SP)))
        dma = pltpu.SemaphoreType.DMA
        whole = pl.BlockSpec(memory_space=pltpu.VMEM)
        in_specs = [whole] * 16
        in_specs[10] = in_specs[12] = pl.BlockSpec(memory_space=pl.ANY)
        block = pltpu.VMEM((NB, SP, NT, 2 * LANES), BF16)
        peer_sems = (dma((NB, len(PEERS))),) * 2
        results = pl.pallas_call(
            layer,
            out_shape=(sds((ROWS, D), BF16), sds((ROWS, D), BF16), sds((SLICE, FF), F32), sds((LANES, D), F32), sds((SLICE, QKV), F32), sds((SLICE, D), F32), sds((SUB, LANES), F32)),
            in_specs=in_specs,
            out_specs=(in_specs[10],) * 2 + (whole,) * 5,
            scratch_shapes=[
                vmem(ROWS, D, BF16), vmem(ROWS, D, BF16), vmem(NT, LANES, F32), vmem(NT, LANES, F32), vmem(NT, LANES, F32), vmem(D, FF, BF16), vmem(FF, D, BF16), vmem(QKV, D, BF16), vmem(ROWS, D, BF16), vmem(ROWS, QKV, BF16), vmem(D, ROWS, BF16), vmem(D, ROWS, BF16),
                block, block, block, vmem(ROWS, D, F32), vmem(ROWS, D, F32), vmem(SUB, FF, F32),
                vmem(2 * LANES, SEQ, BF16), vmem(SEQ, 2 * NT, F32), vmem(SEQ, LANES, F32),
                tuple(halving(shape) for shape in SUM_SHAPES),
                dma((2,)), dma((2,)), peer_sems, peer_sems, dma((8, 4)), dma((8, 4)),
            ],
            compiler_params=pltpu.CompilerParams(vmem_limit_bytes=VMEM_LIMIT, collective_id=0, has_side_effects=True),
            cost_estimate=pl.CostEstimate(flops=56_000_000_000, bytes_accessed=12_000_000, transcendentals=10_000_000),
            name='layer',
        )(x, g, ln1_gain, ln1_bias, ln2_gain, ln2_bias, wt, b_qkv, w_dense, b_dense, w_in, b_in, w_out, b_out, near, far)

        part = sds((SLICE,), F32)
        tokens = sds((ROWS, D), BF16)
        final = list(pl.pallas_call(
            write_out,
            out_shape=(tokens, tokens, part, part, part, part, sds((SLICE, 3, NH, HD), F32), sds((3 * SLICE,), F32), sds((SLICE, D), F32), part,
                       sds((SLICE, FF), F32), sds((LANES,), F32), sds((LANES, D), F32), part),
            in_specs=[whole] * 7,
            out_specs=(whole,) * 14,
            name='write_out',
        )(*results))
        final[0] = final[0].reshape(hidden.shape)
        final[1] = final[1].reshape(hidden.shape)
        final[6] = jnp.swapaxes(final[6], 1, 2)
        return tuple(final)

    tok_spec = P('dp', 'sp', None)
    grad_spec = P(grad_axes)
    return jax.shard_map(device_step, mesh=mesh, in_specs=(tok_spec, tok_spec) + (P(),) * 12, out_specs=(tok_spec, tok_spec) + (grad_spec,) * 12, check_vma=False)
```

```python
import math
import jax
import jax.numpy as jnp
import numpy as np
from jax import lax
from jax.experimental import pallas as pl
from jax.experimental.pallas import tpu as pltpu
from jax.sharding import PartitionSpec as P

LN_EPS = 1e-5
ROPE_BASE = 10000.0
F32 = jnp.float32
BF16 = jnp.bfloat16
MESH = pl.DeviceIdType.MESH
VMEM_LIMIT = 67_043_328

NB, NT, D, NH, HD, FF = 3, 256, 512, 8, 64, 2048
ROWS = NB * NT
SP = 8
PARTS = 16
SEQ = SP * NT
CHUNK = 512
N_CHUNK = FF // CHUNK
SUB = 8
ROW_B_IN, ROW_B_QKV = 5, 6
LANES = 2 * HD
PAIRS = NH // 2
SLICE = D // PARTS
QKV = 3 * D
ROT = HD // 4
TURN = ROT // 2
TURN_BACK = LANES - TURN
LO = slice(0, LANES)
HI = slice(LANES, 2 * LANES)
SCALE = 1.0 / math.sqrt(HD)


def dot(a, b):
    return lax.dot_general(a, b, (((1,), (0,)), ((), ())), preferred_element_type=F32)


def dot_tb(a, b):
    return lax.dot_general(a, b, (((1,), (1,)), ((), ())), preferred_element_type=F32)


def span(index, size):
    return slice(size * index, size * (index + 1))


def lane_iota(rows, cols):
    return lax.broadcasted_iota(jnp.int32, (rows, cols), 1)


def swap(x):
    return pltpu.roll(x, HD, 1)


def row(ref):
    return ref[...].reshape(1, ref.shape[0])


def col_sum(x):
    return jnp.sum(x, axis=0, keepdims=True)


def fold(x, op):
    return op(x.reshape(NT // SUB, SUB, NT), axis=0)


def layer_hat(x):
    mean_val = jnp.mean(x, axis=-1, keepdims=True)
    centered = x - mean_val
    var_val = jnp.mean(centered * centered, axis=-1, keepdims=True)
    inv_std = lax.rsqrt(var_val + LN_EPS)
    return centered * inv_std, inv_std


def fold_weights(wt_ref, wp_ref):
    for h in range(NH):
        base = 3 * HD * h
        wp_ref[span(h, LANES), :] = wt_ref[base:base + LANES, :]
        wp_ref[span(2 * NH + h, HD), :] = wt_ref[base + LANES:base + LANES + HD, :]


def pair_lanes(row_qk, row_v):
    low = lane_iota(1, LANES) < HD
    tiles = []
    for p in range(PAIRS):
        second = swap(row_qk[:, span(2 * p + 1, LANES)])
        v_pair = row_v[:, span(p, LANES)]
        tiles += [row_qk[:, span(2 * p, LANES)], jnp.where(low, v_pair, second), jnp.where(low, second, v_pair)]
    return jnp.concatenate(tiles, axis=1)


def pair_bias(b_all, p):
    low = lane_iota(1, LANES) < HD
    first, mid, last = (b_all[:, span(3 * p + n, LANES)] for n in range(3))
    return first, swap(jnp.where(low, last, mid)), jnp.where(low, mid, last)


def cut(x, shift):
    width = x.shape[1]
    return pltpu.roll(x, (width - shift) % width, 1)[:, LO]


def rotation(near_ref, far_ref, block, cos_ref, sa_ref, sb_ref):
    in_head = lane_iota(NT, LANES) % HD
    near, far = near_ref[...], far_ref[pl.ds(block, 1), :]
    near_s, far_s = pltpu.roll(near, LANES - ROT, 1), pltpu.roll(far, LANES - ROT, 1)
    sin_t = near_s * far + near * far_s
    cos_ref[...] = jnp.where(in_head < ROT, near * far - near_s * far_s, 1.0)
    sa_ref[...] = jnp.where(in_head < TURN, -sin_t, 0.0)
    sb_ref[...] = jnp.where((in_head >= TURN) & (in_head < ROT), sin_t, 0.0)


def angle_table(positions):
    lane = np.arange(LANES) % HD
    freq = ROPE_BASE ** (-(2.0 * (lane % TURN)) / ROT)
    angles = positions[:, None] * freq[None, :]
    return np.where(lane < ROT, np.cos(angles), np.sin(angles)).astype(np.float32)


def part_bits(p):
    return {'c': p % 2, 'x': p // 2 % 2, 'y': p // 4 % 2, 'z': p // 8}


class Where:
    def __init__(self):
        self.z = lax.axis_index('dp')
        self.me = lax.axis_index('sp')
        self.bit = part_bits(self.z * SP + self.me)

    def flip(self, names):
        step = {'c': 1, 'x': 2, 'y': 4}
        z, sp = self.z, self.me
        for n in names:
            if n == 'z':
                z = 1 - z
            else:
                sp = sp + step[n] * (1 - 2 * self.bit[n])
        return z, sp


class Summed:
    def __init__(self, at, order, refs, send_sem, recv_sem):
        self.at, self.order, self.buf, self.lands, self.send_sem, self.recv_sem = at, order, refs[0], refs[1:], send_sem, recv_sem

    def place(self, p):
        bits = part_bits(p)
        return tuple(bits[n] for n in self.order)

    def put(self, p, rows, value):
        self.buf[self.place(p) + (rows,)] = value

    def copy(self, k):
        mine = [self.at.bit[n] for n in self.order]
        return pltpu.make_async_remote_copy(src_ref=self.buf.at[tuple(mine[:k]) + (1 - mine[k],)], dst_ref=self.lands[k],
                                            send_sem=self.send_sem.at[k], recv_sem=self.recv_sem.at[k],
                                            device_id=self.at.flip(self.order[k]), device_id_type=MESH)

    def start(self, k):
        self.copy(k).start()

    def land(self, k):
        self.copy(k).wait_recv()
        mine = tuple(self.at.bit[n] for n in self.order[:k + 1])
        rest = len(self.order) - 1 - k
        for n in range(2 ** rest):
            sub = tuple((n >> m) % 2 for m in reversed(range(rest)))
            self.buf[mine + sub] = self.buf[mine + sub] + self.lands[k][sub if sub else ...]

    def step(self, k):
        self.land(k)
        self.start(k + 1)

    def result(self):
        return self.buf[tuple(self.at.bit[n] for n in self.order)]

    def drain(self):
        for k in range(len(self.order)):
            self.copy(k).wait_send()


PEERS = ('x', 'y', 'xc', 'yc', 'xy', 'xyc', 'c')
ORDERS = ('czxy', 'czyx', 'czxy', 'czyx', 'czxy', 'czyx', 'cxzy', 'cyzx', 'czxy')
SUM_SHAPES = ((HD, D),) * 4 + ((SLICE, D),) * 4 + ((SUB, LANES),)


def exchange(at, b, src, dst, sems):
    out = []
    for k, names in enumerate(PEERS):
        z, sp = at.flip(names)
        out.append(pltpu.make_async_remote_copy(src_ref=src.at[b, sp], dst_ref=dst.at[b, at.me], send_sem=sems[0].at[b, k], recv_sem=sems[1].at[b, k],
                                                device_id=(z, sp), device_id_type=MESH))
    return out


def layer(x_ref, g_ref, g1_ref, s1_ref, g2_ref, s2_ref, wt_ref, bqkv_ref, wd_ref, bd_ref, wi_hbm, bi_ref, wo_hbm, bo_ref, near_ref, far_ref,
          out_hbm, gx_hbm, gwi_ref, gwo_ref, gqkv_ref, gwd_ref, tail_ref,
          out_ref, gx_ref, cos_ref, sa_ref, sb_ref, wi_ref, wo_ref, wp_ref, ctx_ref, dqkv_ref, h2t_ref, gt_ref, buf_ref, in_ref, z_ref, res_ref, dh2_ref, gbi_ref, xt_ref, sdp_ref, acc_ref,
          sums_refs, load_sem, store_sem, out_sems, back_sems, sum_send, sum_recv):
    at = Where()
    me = at.me
    loads = [pltpu.make_async_copy(src, dst, load_sem.at[n]) for n, (src, dst) in enumerate(((wi_hbm, wi_ref), (wo_hbm, wo_ref)))]
    for load in loads:
        load.start()
    barrier = pltpu.get_barrier_semaphore()
    for names in PEERS + ('z',):
        pl.semaphore_signal(barrier, inc=1, device_id=at.flip(names), device_id_type=MESH)
    sums = [Summed(at, order, refs, sum_send.at[n], sum_recv.at[n]) for n, (order, refs) in enumerate(zip(ORDERS, sums_refs))]
    early, tail = sums[:4], sums[4:]
    sum_w, sum_wo = sums[:2], sums[2:4]
    low = lane_iota(NT, LANES) < HD
    rotation(near_ref, far_ref, me, cos_ref, sa_ref, sb_ref)
    fold_weights(wt_ref, wp_ref)
    b_all = row(bqkv_ref)

    def send_heads(b):
        for copy in exchange(at, b, buf_ref, in_ref, out_sems):
            copy.start()

    def send_tokens(b):
        for copy in exchange(at, b, buf_ref, z_ref, back_sems):
            copy.start()

    for b in range(NB):
        rows = span(b, NT)
        x = x_ref[rows, :].astype(F32)
        hat, _ = layer_hat(x)
        h_b = (hat * row(g1_ref) + row(s1_ref)).astype(BF16)
        qk = dot_tb(h_b, wp_ref[:2 * D, :])
        vv = dot_tb(h_b, wp_ref[2 * D:, :])
        dc = dot_tb(g_ref[rows, :], wd_ref[...])
        for p in range(PAIRS):
            bias_a, bias_b, bias_v = pair_bias(b_all, p)
            v_pair = vv[:, span(p, LANES)] + bias_v
            d_pair = dc[:, span(p, LANES)]
            for h, bias, second in ((2 * p, bias_a, jnp.where(low, v_pair, swap(d_pair))), (2 * p + 1, bias_b, jnp.where(low, swap(v_pair), d_pair))):
                t = qk[:, span(h, LANES)] + bias
                t = t * cos_ref[...] + pltpu.roll(t, TURN_BACK, 1) * sa_ref[...] + pltpu.roll(t, TURN, 1) * sb_ref[...]
                buf_ref[b, h, :, LO] = t.astype(BF16)
                buf_ref[b, h, :, HI] = second.astype(BF16)
        if b == 0:
            pl.semaphore_wait(barrier, len(PEERS) + 1)
            send_heads(b)
        in_ref[b, me] = buf_ref[b, me]
        ctx_ref[rows, :] = (hat * row(g2_ref) + row(s2_ref)).astype(BF16)
        res_ref[rows, :] = x + row(bd_ref) + row(bo_ref)

    h2t_ref[...] = ctx_ref[...].T
    gt_ref[...] = g_ref[...].T
    b_in = row(bi_ref)
    for load in loads:
        load.wait()
    for c in range(N_CHUNK):
        cols = span(c, CHUNK)
        pre = dot(ctx_ref[...], wi_ref[:, cols]) + b_in[:, cols]
        d_act = dot_tb(g_ref[...], wo_ref[cols, :])
        cdf = 0.5 * (1.0 + lax.erf(pre * math.sqrt(0.5)))
        pdf = jnp.exp(-0.5 * pre * pre) * (1.0 / math.sqrt(2.0 * math.pi))
        act = (pre * cdf).astype(BF16)
        d_pre = d_act * (cdf + pre * pdf)
        d_pre_bf = d_pre.astype(BF16)
        gbi_ref[:, cols] = jnp.broadcast_to(col_sum(d_pre), (SUB, CHUNK))
        g_wi = dot(h2t_ref[...], d_pre_bf)
        for p in range(PARTS):
            sum_w[c // 2].put(p, span(c % 2, SLICE), g_wi[span(p, SLICE)])
        if c % 2:
            sum_w[c // 2].start(0)
        g_wo = dot(gt_ref[...], act)
        for q in range(CHUNK // LANES):
            for n, s in enumerate(sum_wo):
                where = s.place(PARTS // N_CHUNK * c + q)
                for k in range(D // LANES):
                    s.buf[where + (slice(None), span(k, LANES))] = g_wo[span(2 * k + n, HD), span(q, LANES)]
        res_ref[...] += dot(act, wo_ref[cols, :])
        d_h = dot_tb(d_pre_bf, wi_ref[:, cols])
        if c == N_CHUNK - 2:
            send_heads(1)
        if c == 0:
            dh2_ref[...] = d_h
        else:
            dh2_ref[...] += d_h
    for s in sum_wo:
        s.start(0)
    sum_w[0].step(0)
    zero_row = jnp.zeros((1, D), F32)
    g_ln2 = g_ln2_b = g_b_dense = zero_row
    for b in range(NB):
        rows = span(b, NT)
        hat, _ = layer_hat(x_ref[rows, :].astype(F32))
        d_h = dh2_ref[rows, :]
        g_ln2 += col_sum(d_h * hat)
        g_ln2_b += col_sum(d_h)
        g_b_dense += col_sum(g_ref[rows, :].astype(F32))
        dh2_ref[rows, :] = d_h * row(g2_ref)

    keep = lax.broadcasted_iota(jnp.int32, (NT, NT), 0) <= lane_iota(NT, NT)
    zero_t = jnp.zeros((HD, NT), BF16)
    s_cols, p_cols = span(0, NT), span(1, NT)

    def one_sequence(b, carry):
        for copy in exchange(at, b, buf_ref, in_ref, out_sems):
            copy.wait()
        for j in range(SP):
            xt_ref[:, span(j, NT)] = in_ref[b, j].T
        for i in reversed(range(SP)):
            cols = span(i, NT)
            q_t = xt_ref[span(0, HD), cols] * BF16(SCALE)
            dc_t = xt_ref[span(3, HD), cols]
            w_s = jnp.concatenate([zero_t, q_t, zero_t, zero_t], axis=0)
            w_p = jnp.concatenate([zero_t, zero_t, dc_t, zero_t], axis=0)
            w_sp = jnp.concatenate([w_s, w_p], axis=1)
            q_n = jnp.where(low, in_ref[b, i, :, LO] * BF16(SCALE), BF16(0.0))
            dc_n = jnp.where(low, BF16(0.0), in_ref[b, i, :, HI])
            w_acc = jnp.concatenate([q_n, dc_n], axis=0)
            tops = []
            for j in range(i + 1):
                kv = span(j, NT)
                both = dot(in_ref[b, j], w_sp)
                s = both[:, s_cols]
                if j == i:
                    s = jnp.where(keep, s, -1e30)
                sdp_ref[kv, s_cols] = s
                sdp_ref[kv, p_cols] = both[:, p_cols]
                part = fold(s, jnp.max)
                tops = [jnp.maximum(tops[0], part)] if tops else [part]
            top = jnp.max(tops[0], axis=0, keepdims=True)
            total = jnp.zeros((SUB, NT), F32)
            inner = jnp.zeros((SUB, NT), F32)
            for j in range(i + 1):
                kv = span(j, NT)
                e = jnp.exp(sdp_ref[kv, s_cols] - top)
                sdp_ref[kv, s_cols] = e
                total += fold(e, jnp.sum)
                inner += fold(e * sdp_ref[kv, p_cols], jnp.sum)
            inv = 1.0 / col_sum(total)
            delta = col_sum(inner) * inv
            ctx_t = jnp.zeros((HD, NT), F32)
            dq_t = jnp.zeros((HD, NT), F32)
            for j in range(i + 1):
                kv = span(j, NT)
                prob = sdp_ref[kv, s_cols] * inv
                prob_bf = prob.astype(BF16)
                ds_bf = (prob * (sdp_ref[kv, p_cols] - delta)).astype(BF16)
                ctx_t += dot(xt_ref[span(2, HD), kv], prob_bf)
                dq_t += dot(xt_ref[span(1, HD), kv], ds_bf)
                step = dot(jnp.concatenate([ds_bf, prob_bf], axis=1), w_acc)
                if i == SP - 1:
                    acc_ref[kv, :] = step
                else:
                    acc_ref[kv, :] += step
            nat = jnp.concatenate([dq_t * SCALE, ctx_t], axis=0).T
            acc = acc_ref[cols, :]
            buf_ref[b, i, :, LO] = jnp.where(low, nat, swap(acc)).astype(BF16)
            buf_ref[b, i, :, HI] = jnp.where(low, swap(nat), acc).astype(BF16)
            if i == SP - 3:
                @pl.when(b == 0)
                def _():
                    for s in early[1:]:
                        s.step(0)
                    send_heads(2)

                @pl.when(b == 1)
                def _():
                    sum_w[0].step(1)
        send_tokens(b)
        z_ref[b, me] = buf_ref[b, me]
        return carry

    lax.fori_loop(0, NB, one_sequence, 0)
    sum_w[0].step(2)
    sum_w[1].step(1)
    sum_wo[0].step(1)

    def arrive(b):
        rows = span(b, NT)
        if b == NB - 1:
            sum_wo[1].step(1)
        for copy in exchange(at, b, buf_ref, z_ref, back_sems):
            copy.wait()
        sums_qk, sums_v = [], []
        for p in range(PAIRS):
            seconds = []
            for h in (2 * p, 2 * p + 1):
                t = z_ref[b, h, :, LO].astype(F32)
                t = t * cos_ref[...] - pltpu.roll(t, TURN_BACK, 1) * sa_ref[...] - pltpu.roll(t, TURN, 1) * sb_ref[...]
                sums_qk.append(col_sum(t))
                dqkv_ref[rows, span(h, LANES)] = t.astype(BF16)
                seconds.append(z_ref[b, h, :, HI].astype(F32))
            ctx_ref[rows, span(p, LANES)] = jnp.where(low, seconds[0], swap(seconds[1])).astype(BF16)
            dv_pair = jnp.where(low, swap(seconds[0]), seconds[1])
            dqkv_ref[rows, span(2 * NH // 2 + p, LANES)] = dv_pair.astype(BF16)
            sums_v.append(col_sum(dv_pair))
        hat, inv_std = layer_hat(x_ref[rows, :].astype(F32))
        h1_t = (hat * row(g1_ref) + row(s1_ref)).astype(BF16).T
        ctx_t = ctx_ref[rows, :].T
        for k in range(4):
            block = span(k, D)
            term = dot(h1_t, dqkv_ref[rows, block]) if k < 3 else dot(ctx_t, g_ref[rows, :])
            if b == 0:
                sdp_ref[block, :] = term
            elif b < NB - 1:
                sdp_ref[block, :] += term
            else:
                term = sdp_ref[block, :] + term
                for p in range(PARTS):
                    tail[k].put(p, slice(None), term[span(p, SLICE)])
                tail[k].start(0)
        return hat, inv_std, jnp.concatenate(sums_qk, axis=1), jnp.concatenate(sums_v, axis=1)

    def finish(b, hat, inv_std):
        rows = span(b, NT)
        d_h1 = dot(dqkv_ref[rows, :], wp_ref[...])
        d_hat = d_h1 * row(g1_ref) + dh2_ref[rows, :]
        d_x = inv_std * (d_hat - jnp.mean(d_hat, axis=-1, keepdims=True) - hat * jnp.mean(d_hat * hat, axis=-1, keepdims=True))
        gx_ref[rows, :] = (g_ref[rows, :].astype(F32) + d_x).astype(BF16)
        return col_sum(d_h1 * hat), col_sum(d_h1)

    def forward(b):
        rows = span(b, NT)
        out_ref[rows, :] = (res_ref[rows, :] + dot(ctx_ref[rows, :], wd_ref[...])).astype(BF16)

    g_ln1 = g_ln1_b = zero_row
    gb_qk, gb_v = jnp.zeros((1, 2 * D), F32), zero_row
    for b in range(NB):
        hat, inv_std, part_qk, part_v = arrive(b)
        gb_qk += part_qk
        gb_v += part_v
        if b == NB - 1:
            for s in tail[:4]:
                s.step(0)
        part_g, part_b = finish(b, hat, inv_std)
        g_ln1 += part_g
        g_ln1_b += part_b
        if b < NB - 1:
            forward(b)

    store_gx = pltpu.make_async_copy(gx_ref, gx_hbm, store_sem.at[0])
    store_gx.start()
    five = jnp.concatenate([g_ln1, g_ln1_b, g_ln2, g_ln2_b, g_b_dense] + [zero_row] * 3, axis=0)
    g_bqkv = jnp.broadcast_to(pair_lanes(gb_qk, gb_v), (SUB, QKV))
    line = lax.broadcasted_iota(jnp.int32, (SUB, LANES), 0)
    for p in range(PARTS):
        small = jnp.where(line == ROW_B_IN, gbi_ref[:, span(p, LANES)], cut(five, SLICE * p))
        tail[4].put(p, slice(None), jnp.where(line == ROW_B_QKV, cut(g_bqkv, 3 * SLICE * p), small))
    tail[4].start(0)
    forward(NB - 1)
    store_out = pltpu.make_async_copy(out_ref, out_hbm, store_sem.at[1])
    store_out.start()

    tail[4].step(0)
    for s in tail:
        s.step(1)
    for s in early[1:]:
        s.step(2)
    for s in tail:
        s.step(2)
    for s in early:
        s.land(3)
    for c in range(N_CHUNK):
        gwi_ref[:, span(c, CHUNK)] = sum_w[c // 2].result()[span(c % 2, SLICE)]
    g_wo = jnp.concatenate([s.result() for s in sum_wo], axis=0)
    for k in range(D // LANES):
        gwo_ref[:, span(k, LANES)] = g_wo[:, span(k, LANES)].T
    for s in tail:
        s.land(3)
    for k in range(3):
        gqkv_ref[:, span(k, D)] = tail[k].result()
    gwd_ref[...] = tail[3].result()
    tail_ref[...] = tail[4].result()
    store_gx.wait()
    store_out.wait()
    for s in sums:
        s.drain()


def write_out(out_in, gx_in, gwi_in, gwo_in, gqkv_in, gwd_in, tail_in,
              out_ref, gx_ref, g1_ref, s1_ref, g2_ref, s2_ref, gqkv_ref, gbqkv_ref, gwd_ref, gbd_ref, gwi_ref, gbi_ref, gwo_ref, gbo_ref):
    out_ref[...] = out_in[...]
    gx_ref[...] = gx_in[...]
    gwi_ref[...] = gwi_in[...]
    gwo_ref[...] = gwo_in[...]
    gwd_ref[...] = gwd_in[...]
    for h in range(NH):
        tile = gqkv_in[:, span(h, LANES)]
        gqkv_ref[:, 0, h, :] = tile[:, :HD]
        gqkv_ref[:, 1, h, :] = tile[:, HD:]
        gqkv_ref[:, 2, h, :] = gqkv_in[:, span(2 * NH + h, HD)]
    for n, ref in enumerate((g1_ref, s1_ref, g2_ref, s2_ref, gbd_ref)):
        ref[...] = tail_in[n, :SLICE]
    gbo_ref[...] = tail_in[n, :SLICE]
    gbi_ref[...] = tail_in[ROW_B_IN, :]
    gbqkv_ref[...] = tail_in[ROW_B_QKV, :3 * SLICE]


def sds(shape, dtype):
    return jax.ShapeDtypeStruct(shape, dtype)


def halving(shape):
    return tuple(pltpu.VMEM((2,) * n + shape, F32) for n in reversed(range(5)))


def vmem(rows, cols, dtype):
    return pltpu.VMEM((rows, cols), dtype)


def solution(mesh):
    grad_axes = ('dp', 'sp')

    def device_step(hidden, grad_out, ln1_gain, ln1_bias, ln2_gain, ln2_bias, w_qkv, b_qkv, w_dense, b_dense, w_in, b_in, w_out, b_out):
        x = hidden.reshape(ROWS, D)
        g = grad_out.reshape(ROWS, D)
        wt = jnp.moveaxis(w_qkv, 0, -1).reshape(QKV, D)
        near = jnp.asarray(angle_table(np.arange(NT)))
        far = jnp.asarray(angle_table(NT * np.arange(SP)))
        dma = pltpu.SemaphoreType.DMA
        whole = pl.BlockSpec(memory_space=pltpu.VMEM)
        in_specs = [whole] * 16
        in_specs[10] = in_specs[12] = pl.BlockSpec(memory_space=pl.ANY)
        block = pltpu.VMEM((NB, SP, NT, 2 * LANES), BF16)
        peer_sems = (dma((NB, len(PEERS))),) * 2
        results = pl.pallas_call(
            layer,
            out_shape=(sds((ROWS, D), BF16), sds((ROWS, D), BF16), sds((SLICE, FF), F32), sds((LANES, D), F32), sds((SLICE, QKV), F32), sds((SLICE, D), F32), sds((SUB, LANES), F32)),
            in_specs=in_specs,
            out_specs=(in_specs[10],) * 2 + (whole,) * 5,
            scratch_shapes=[
                vmem(ROWS, D, BF16), vmem(ROWS, D, BF16), vmem(NT, LANES, F32), vmem(NT, LANES, F32), vmem(NT, LANES, F32), vmem(D, FF, BF16), vmem(FF, D, BF16), vmem(QKV, D, BF16), vmem(ROWS, D, BF16), vmem(ROWS, QKV, BF16), vmem(D, ROWS, BF16), vmem(D, ROWS, BF16),
                block, block, block, vmem(ROWS, D, F32), vmem(ROWS, D, F32), vmem(SUB, FF, F32),
                vmem(2 * LANES, SEQ, BF16), vmem(SEQ, 2 * NT, F32), vmem(SEQ, LANES, F32),
                tuple(halving(shape) for shape in SUM_SHAPES),
                dma((2,)), dma((2,)), peer_sems, peer_sems, dma((9, 4)), dma((9, 4)),
            ],
            compiler_params=pltpu.CompilerParams(vmem_limit_bytes=VMEM_LIMIT, collective_id=0, has_side_effects=True),
            cost_estimate=pl.CostEstimate(flops=56_000_000_000, bytes_accessed=12_000_000, transcendentals=10_000_000),
            name='layer',
        )(x, g, ln1_gain, ln1_bias, ln2_gain, ln2_bias, wt, b_qkv, w_dense, b_dense, w_in, b_in, w_out, b_out, near, far)

        part = sds((SLICE,), F32)
        tokens = sds((ROWS, D), BF16)
        final = list(pl.pallas_call(
            write_out,
            out_shape=(tokens, tokens, part, part, part, part, sds((SLICE, 3, NH, HD), F32), sds((3 * SLICE,), F32), sds((SLICE, D), F32), part,
                       sds((SLICE, FF), F32), sds((LANES,), F32), sds((LANES, D), F32), part),
            in_specs=[whole] * 7,
            out_specs=(whole,) * 14,
            name='write_out',
        )(*results))
        final[0] = final[0].reshape(hidden.shape)
        final[1] = final[1].reshape(hidden.shape)
        final[6] = jnp.swapaxes(final[6], 1, 2)
        return tuple(final)

    tok_spec = P('dp', 'sp', None)
    grad_spec = P(grad_axes)
    return jax.shard_map(device_step, mesh=mesh, in_specs=(tok_spec, tok_spec) + (P(),) * 12, out_specs=(tok_spec, tok_spec) + (grad_spec,) * 12, check_vma=False)
```

```python
import math
import jax
import jax.numpy as jnp
import numpy as np
from jax import lax
from jax.experimental import pallas as pl
from jax.experimental.pallas import tpu as pltpu
from jax.sharding import PartitionSpec as P

LN_EPS = 1e-5
ROPE_BASE = 10000.0
F32 = jnp.float32
BF16 = jnp.bfloat16
MESH = pl.DeviceIdType.MESH
VMEM_LIMIT = 67_043_328

NB, NT, D, NH, HD, FF = 3, 256, 512, 8, 64, 2048
ROWS = NB * NT
SP = 8
PARTS = 16
SEQ = SP * NT
CHUNK = 512
N_CHUNK = FF // CHUNK
SUB = 8
ROW_B_IN, ROW_B_QKV = 5, 6
LANES = 2 * HD
PAIRS = NH // 2
SLICE = D // PARTS
QKV = 3 * D
ROT = HD // 4
TURN = ROT // 2
TURN_BACK = LANES - TURN
LO = slice(0, LANES)
HI = slice(LANES, 2 * LANES)
SCALE = 1.0 / math.sqrt(HD)


def dot(a, b):
    return lax.dot_general(a, b, (((1,), (0,)), ((), ())), preferred_element_type=F32)


def dot_tb(a, b):
    return lax.dot_general(a, b, (((1,), (1,)), ((), ())), preferred_element_type=F32)


def span(index, size):
    return slice(size * index, size * (index + 1))


def lane_iota(rows, cols):
    return lax.broadcasted_iota(jnp.int32, (rows, cols), 1)


def swap(x):
    return pltpu.roll(x, HD, 1)


def row(ref):
    return ref[...].reshape(1, ref.shape[0])


def col_sum(x):
    return jnp.sum(x, axis=0, keepdims=True)


def fold(x, op):
    return op(x.reshape(NT // SUB, SUB, NT), axis=0)


def layer_hat(x):
    mean_val = jnp.mean(x, axis=-1, keepdims=True)
    centered = x - mean_val
    var_val = jnp.mean(centered * centered, axis=-1, keepdims=True)
    inv_std = lax.rsqrt(var_val + LN_EPS)
    return centered * inv_std, inv_std


def fold_weights(wt_ref, wp_ref):
    for h in range(NH):
        base = 3 * HD * h
        wp_ref[span(h, LANES), :] = wt_ref[base:base + LANES, :]
        wp_ref[span(2 * NH + h, HD), :] = wt_ref[base + LANES:base + LANES + HD, :]


def pair_lanes(row_qk, row_v):
    low = lane_iota(1, LANES) < HD
    tiles = []
    for p in range(PAIRS):
        second = swap(row_qk[:, span(2 * p + 1, LANES)])
        v_pair = row_v[:, span(p, LANES)]
        tiles += [row_qk[:, span(2 * p, LANES)], jnp.where(low, v_pair, second), jnp.where(low, second, v_pair)]
    return jnp.concatenate(tiles, axis=1)


def pair_bias(b_all, p):
    low = lane_iota(1, LANES) < HD
    first, mid, last = (b_all[:, span(3 * p + n, LANES)] for n in range(3))
    return first, swap(jnp.where(low, last, mid)), jnp.where(low, mid, last)


def cut(x, shift):
    width = x.shape[1]
    return pltpu.roll(x, (width - shift) % width, 1)[:, LO]


def rotation(near_ref, far_ref, block, cos_ref, sa_ref, sb_ref):
    in_head = lane_iota(NT, LANES) % HD
    near, far = near_ref[...], far_ref[pl.ds(block, 1), :]
    near_s, far_s = pltpu.roll(near, LANES - ROT, 1), pltpu.roll(far, LANES - ROT, 1)
    sin_t = near_s * far + near * far_s
    cos_ref[...] = jnp.where(in_head < ROT, near * far - near_s * far_s, 1.0)
    sa_ref[...] = jnp.where(in_head < TURN, -sin_t, 0.0)
    sb_ref[...] = jnp.where((in_head >= TURN) & (in_head < ROT), sin_t, 0.0)


def angle_table(positions):
    lane = np.arange(LANES) % HD
    freq = ROPE_BASE ** (-(2.0 * (lane % TURN)) / ROT)
    angles = positions[:, None] * freq[None, :]
    return np.where(lane < ROT, np.cos(angles), np.sin(angles)).astype(np.float32)


def part_bits(p):
    return {'c': p % 2, 'x': p // 2 % 2, 'y': p // 4 % 2, 'z': p // 8}


class Where:
    def __init__(self):
        self.z = lax.axis_index('dp')
        self.me = lax.axis_index('sp')
        self.bit = part_bits(self.z * SP + self.me)

    def flip(self, names):
        step = {'c': 1, 'x': 2, 'y': 4}
        z, sp = self.z, self.me
        for n in names:
            if n == 'z':
                z = 1 - z
            else:
                sp = sp + step[n] * (1 - 2 * self.bit[n])
        return z, sp


class Summed:
    def __init__(self, at, order, refs, send_sem, recv_sem):
        self.at, self.order, self.buf, self.lands, self.send_sem, self.recv_sem = at, order, refs[0], refs[1:], send_sem, recv_sem

    def place(self, p):
        bits = part_bits(p)
        return tuple(bits[n] for n in self.order)

    def put(self, p, rows, value):
        self.buf[self.place(p) + (rows,)] = value

    def copy(self, k):
        mine = [self.at.bit[n] for n in self.order]
        return pltpu.make_async_remote_copy(src_ref=self.buf.at[tuple(mine[:k]) + (1 - mine[k],)], dst_ref=self.lands[k],
                                            send_sem=self.send_sem.at[k], recv_sem=self.recv_sem.at[k],
                                            device_id=self.at.flip(self.order[k]), device_id_type=MESH)

    def start(self, k):
        self.copy(k).start()

    def land(self, k):
        self.copy(k).wait_recv()
        mine = tuple(self.at.bit[n] for n in self.order[:k + 1])
        rest = len(self.order) - 1 - k
        for n in range(2 ** rest):
            sub = tuple((n >> m) % 2 for m in reversed(range(rest)))
            self.buf[mine + sub] = self.buf[mine + sub] + self.lands[k][sub if sub else ...]

    def step(self, k):
        self.land(k)
        self.start(k + 1)

    def result(self):
        return self.buf[tuple(self.at.bit[n] for n in self.order)]

    def drain(self):
        for k in range(len(self.order)):
            self.copy(k).wait_send()


PEERS = ('x', 'y', 'xc', 'yc', 'xy', 'xyc', 'c')
ORDERS = ('czxy', 'czxy', 'czyx', 'czxy', 'czyx', 'cxzy', 'cyzx', 'czxy')
SUM_SHAPES = ((2 * SLICE, D), (2 * SLICE, D), (LANES, D)) + ((SLICE, D),) * 4 + ((SUB, LANES),)


def exchange(at, b, src, dst, sems):
    out = []
    for k, names in enumerate(PEERS):
        z, sp = at.flip(names)
        out.append(pltpu.make_async_remote_copy(src_ref=src.at[b, sp], dst_ref=dst.at[b, at.me], send_sem=sems[0].at[b, k], recv_sem=sems[1].at[b, k],
                                                device_id=(z, sp), device_id_type=MESH))
    return out


def layer(x_ref, g_ref, g1_ref, s1_ref, g2_ref, s2_ref, wt_ref, bqkv_ref, wd_ref, bd_ref, wi_hbm, bi_ref, wo_hbm, bo_ref, near_ref, far_ref,
          out_hbm, gx_hbm, gwi_ref, gwo_ref, gqkv_ref, gwd_ref, tail_ref,
          out_ref, gx_ref, cos_ref, sa_ref, sb_ref, wi_ref, wo_ref, wp_ref, ctx_ref, dqkv_ref, h2t_ref, gt_ref, buf_ref, in_ref, z_ref, res_ref, dh2_ref, gbi_ref, xt_ref, sdp_ref, acc_ref,
          sums_refs, load_sem, store_sem, out_sems, back_sems, sum_send, sum_recv):
    at = Where()
    me = at.me
    loads = [pltpu.make_async_copy(src, dst, load_sem.at[n]) for n, (src, dst) in enumerate(((wi_hbm, wi_ref), (wo_hbm, wo_ref)))]
    for load in loads:
        load.start()
    barrier = pltpu.get_barrier_semaphore()
    for names in PEERS + ('z',):
        pl.semaphore_signal(barrier, inc=1, device_id=at.flip(names), device_id_type=MESH)
    sums = [Summed(at, order, refs, sum_send.at[n], sum_recv.at[n]) for n, (order, refs) in enumerate(zip(ORDERS, sums_refs))]
    early, tail = sums[:3], sums[3:]
    sum_w = sums[:2]
    sum_wo = sums[2]
    low = lane_iota(NT, LANES) < HD
    rotation(near_ref, far_ref, me, cos_ref, sa_ref, sb_ref)
    fold_weights(wt_ref, wp_ref)
    b_all = row(bqkv_ref)

    def send_heads(b):
        for copy in exchange(at, b, buf_ref, in_ref, out_sems):
            copy.start()

    def send_tokens(b):
        for copy in exchange(at, b, buf_ref, z_ref, back_sems):
            copy.start()

    for b in range(NB):
        rows = span(b, NT)
        x = x_ref[rows, :].astype(F32)
        hat, _ = layer_hat(x)
        h_b = (hat * row(g1_ref) + row(s1_ref)).astype(BF16)
        qk = dot_tb(h_b, wp_ref[:2 * D, :])
        vv = dot_tb(h_b, wp_ref[2 * D:, :])
        dc = dot_tb(g_ref[rows, :], wd_ref[...])
        for p in range(PAIRS):
            bias_a, bias_b, bias_v = pair_bias(b_all, p)
            v_pair = vv[:, span(p, LANES)] + bias_v
            d_pair = dc[:, span(p, LANES)]
            for h, bias, second in ((2 * p, bias_a, jnp.where(low, v_pair, swap(d_pair))), (2 * p + 1, bias_b, jnp.where(low, swap(v_pair), d_pair))):
                t = qk[:, span(h, LANES)] + bias
                t = t * cos_ref[...] + pltpu.roll(t, TURN_BACK, 1) * sa_ref[...] + pltpu.roll(t, TURN, 1) * sb_ref[...]
                buf_ref[b, h, :, LO] = t.astype(BF16)
                buf_ref[b, h, :, HI] = second.astype(BF16)
        if b == 0:
            pl.semaphore_wait(barrier, len(PEERS) + 1)
            send_heads(b)
        in_ref[b, me] = buf_ref[b, me]
        ctx_ref[rows, :] = (hat * row(g2_ref) + row(s2_ref)).astype(BF16)
        res_ref[rows, :] = x + row(bd_ref) + row(bo_ref)

    h2t_ref[...] = ctx_ref[...].T
    gt_ref[...] = g_ref[...].T
    b_in = row(bi_ref)
    for load in loads:
        load.wait()
    for c in range(N_CHUNK):
        cols = span(c, CHUNK)
        pre = dot(ctx_ref[...], wi_ref[:, cols]) + b_in[:, cols]
        d_act = dot_tb(g_ref[...], wo_ref[cols, :])
        cdf = 0.5 * (1.0 + lax.erf(pre * math.sqrt(0.5)))
        pdf = jnp.exp(-0.5 * pre * pre) * (1.0 / math.sqrt(2.0 * math.pi))
        act = (pre * cdf).astype(BF16)
        d_pre = d_act * (cdf + pre * pdf)
        d_pre_bf = d_pre.astype(BF16)
        gbi_ref[:, cols] = jnp.broadcast_to(col_sum(d_pre), (SUB, CHUNK))
        g_wi = dot(h2t_ref[...], d_pre_bf)
        for p in range(PARTS):
            sum_w[c // 2].put(p, span(c % 2, SLICE), g_wi[span(p, SLICE)])
        if c % 2:
            sum_w[c // 2].start(0)
        g_wo = dot(gt_ref[...], act)
        for q in range(CHUNK // LANES):
            where = sum_wo.place(PARTS // N_CHUNK * c + q)
            for k in range(D // LANES):
                sum_wo.buf[where + (slice(None), span(k, LANES))] = g_wo[span(k, LANES), span(q, LANES)]
        res_ref[...] += dot(act, wo_ref[cols, :])
        d_h = dot_tb(d_pre_bf, wi_ref[:, cols])
        if c == N_CHUNK - 2:
            send_heads(1)
        if c == 0:
            dh2_ref[...] = d_h
        else:
            dh2_ref[...] += d_h
    sum_wo.start(0)
    sum_w[0].step(0)
    zero_row = jnp.zeros((1, D), F32)
    g_ln2 = g_ln2_b = g_b_dense = zero_row
    for b in range(NB):
        rows = span(b, NT)
        hat, _ = layer_hat(x_ref[rows, :].astype(F32))
        d_h = dh2_ref[rows, :]
        g_ln2 += col_sum(d_h * hat)
        g_ln2_b += col_sum(d_h)
        g_b_dense += col_sum(g_ref[rows, :].astype(F32))
        dh2_ref[rows, :] = d_h * row(g2_ref)

    keep = lax.broadcasted_iota(jnp.int32, (NT, NT), 0) <= lane_iota(NT, NT)
    zero_t = jnp.zeros((HD, NT), BF16)
    s_cols, p_cols = span(0, NT), span(1, NT)

    def one_sequence(b, carry):
        for copy in exchange(at, b, buf_ref, in_ref, out_sems):
            copy.wait()
        for j in range(SP):
            xt_ref[:, span(j, NT)] = in_ref[b, j].T
        for i in reversed(range(SP)):
            cols = span(i, NT)
            q_t = xt_ref[span(0, HD), cols] * BF16(SCALE)
            dc_t = xt_ref[span(3, HD), cols]
            w_s = jnp.concatenate([zero_t, q_t, zero_t, zero_t], axis=0)
            w_p = jnp.concatenate([zero_t, zero_t, dc_t, zero_t], axis=0)
            w_sp = jnp.concatenate([w_s, w_p], axis=1)
            q_n = jnp.where(low, in_ref[b, i, :, LO] * BF16(SCALE), BF16(0.0))
            dc_n = jnp.where(low, BF16(0.0), in_ref[b, i, :, HI])
            w_acc = jnp.concatenate([q_n, dc_n], axis=0)
            tops = []
            for j in range(i + 1):
                kv = span(j, NT)
                both = dot(in_ref[b, j], w_sp)
                s = both[:, s_cols]
                if j == i:
                    s = jnp.where(keep, s, -1e30)
                sdp_ref[kv, s_cols] = s
                sdp_ref[kv, p_cols] = both[:, p_cols]
                part = fold(s, jnp.max)
                tops = [jnp.maximum(tops[0], part)] if tops else [part]
            top = jnp.max(tops[0], axis=0, keepdims=True)
            total = jnp.zeros((SUB, NT), F32)
            inner = jnp.zeros((SUB, NT), F32)
            for j in range(i + 1):
                kv = span(j, NT)
                e = jnp.exp(sdp_ref[kv, s_cols] - top)
                sdp_ref[kv, s_cols] = e
                total += fold(e, jnp.sum)
                inner += fold(e * sdp_ref[kv, p_cols], jnp.sum)
            inv = 1.0 / col_sum(total)
            delta = col_sum(inner) * inv
            ctx_t = jnp.zeros((HD, NT), F32)
            dq_t = jnp.zeros((HD, NT), F32)
            for j in range(i + 1):
                kv = span(j, NT)
                prob = sdp_ref[kv, s_cols] * inv
                prob_bf = prob.astype(BF16)
                ds_bf = (prob * (sdp_ref[kv, p_cols] - delta)).astype(BF16)
                ctx_t += dot(xt_ref[span(2, HD), kv], prob_bf)
                dq_t += dot(xt_ref[span(1, HD), kv], ds_bf)
                step = dot(jnp.concatenate([ds_bf, prob_bf], axis=1), w_acc)
                if i == SP - 1:
                    acc_ref[kv, :] = step
                else:
                    acc_ref[kv, :] += step
            nat = jnp.concatenate([dq_t * SCALE, ctx_t], axis=0).T
            acc = acc_ref[cols, :]
            buf_ref[b, i, :, LO] = jnp.where(low, nat, swap(acc)).astype(BF16)
            buf_ref[b, i, :, HI] = jnp.where(low, swap(nat), acc).astype(BF16)
            if i == SP - 3:
                @pl.when(b == 0)
                def _():
                    for s in early[1:]:
                        s.step(0)
                    send_heads(2)
        send_tokens(b)
        z_ref[b, me] = buf_ref[b, me]
        return carry

    lax.fori_loop(0, NB, one_sequence, 0)

    def arrive(b):
        rows = span(b, NT)
        for copy in exchange(at, b, buf_ref, z_ref, back_sems):
            copy.wait()
        if b == NB - 1:
            for s in early:
                s.step(1)
        sums_qk, sums_v = [], []
        for p in range(PAIRS):
            seconds = []
            for h in (2 * p, 2 * p + 1):
                t = z_ref[b, h, :, LO].astype(F32)
                t = t * cos_ref[...] - pltpu.roll(t, TURN_BACK, 1) * sa_ref[...] - pltpu.roll(t, TURN, 1) * sb_ref[...]
                sums_qk.append(col_sum(t))
                dqkv_ref[rows, span(h, LANES)] = t.astype(BF16)
                seconds.append(z_ref[b, h, :, HI].astype(F32))
            ctx_ref[rows, span(p, LANES)] = jnp.where(low, seconds[0], swap(seconds[1])).astype(BF16)
            dv_pair = jnp.where(low, swap(seconds[0]), seconds[1])
            dqkv_ref[rows, span(2 * NH // 2 + p, LANES)] = dv_pair.astype(BF16)
            sums_v.append(col_sum(dv_pair))
        hat, inv_std = layer_hat(x_ref[rows, :].astype(F32))
        h1_t = (hat * row(g1_ref) + row(s1_ref)).astype(BF16).T
        ctx_t = ctx_ref[rows, :].T
        for k in range(4):
            block = span(k, D)
            term = dot(h1_t, dqkv_ref[rows, block]) if k < 3 else dot(ctx_t, g_ref[rows, :])
            if b == 0:
                sdp_ref[block, :] = term
            elif b < NB - 1:
                sdp_ref[block, :] += term
            else:
                term = sdp_ref[block, :] + term
                for p in range(PARTS):
                    tail[k].put(p, slice(None), term[span(p, SLICE)])
                tail[k].start(0)
        return hat, inv_std, jnp.concatenate(sums_qk, axis=1), jnp.concatenate(sums_v, axis=1)

    def finish(b, hat, inv_std):
        rows = span(b, NT)
        d_h1 = dot(dqkv_ref[rows, :], wp_ref[...])
        d_hat = d_h1 * row(g1_ref) + dh2_ref[rows, :]
        d_x = inv_std * (d_hat - jnp.mean(d_hat, axis=-1, keepdims=True) - hat * jnp.mean(d_hat * hat, axis=-1, keepdims=True))
        gx_ref[rows, :] = (g_ref[rows, :].astype(F32) + d_x).astype(BF16)
        return col_sum(d_h1 * hat), col_sum(d_h1)

    def forward(b):
        rows = span(b, NT)
        out_ref[rows, :] = (res_ref[rows, :] + dot(ctx_ref[rows, :], wd_ref[...])).astype(BF16)

    g_ln1 = g_ln1_b = zero_row
    gb_qk, gb_v = jnp.zeros((1, 2 * D), F32), zero_row
    for b in range(NB):
        hat, inv_std, part_qk, part_v = arrive(b)
        gb_qk += part_qk
        gb_v += part_v
        if b == NB - 1:
            for s in tail[:4]:
                s.step(0)
        part_g, part_b = finish(b, hat, inv_std)
        g_ln1 += part_g
        g_ln1_b += part_b
        if b < NB - 1:
            forward(b)

    store_gx = pltpu.make_async_copy(gx_ref, gx_hbm, store_sem.at[0])
    store_gx.start()
    five = jnp.concatenate([g_ln1, g_ln1_b, g_ln2, g_ln2_b, g_b_dense] + [zero_row] * 3, axis=0)
    g_bqkv = jnp.broadcast_to(pair_lanes(gb_qk, gb_v), (SUB, QKV))
    line = lax.broadcasted_iota(jnp.int32, (SUB, LANES), 0)
    for p in range(PARTS):
        small = jnp.where(line == ROW_B_IN, gbi_ref[:, span(p, LANES)], cut(five, SLICE * p))
        tail[4].put(p, slice(None), jnp.where(line == ROW_B_QKV, cut(g_bqkv, 3 * SLICE * p), small))
    tail[4].start(0)
    forward(NB - 1)
    store_out = pltpu.make_async_copy(out_ref, out_hbm, store_sem.at[1])
    store_out.start()

    tail[4].step(0)
    for s in tail:
        s.step(1)
    for s in early:
        s.step(2)
    for s in tail:
        s.step(2)
    for s in early:
        s.land(3)
    for c in range(N_CHUNK):
        gwi_ref[:, span(c, CHUNK)] = sum_w[c // 2].result()[span(c % 2, SLICE)]
    g_wo = sum_wo.result()
    for k in range(D // LANES):
        gwo_ref[:, span(k, LANES)] = g_wo[:, span(k, LANES)].T
    for s in tail:
        s.land(3)
    for k in range(3):
        gqkv_ref[:, span(k, D)] = tail[k].result()
    gwd_ref[...] = tail[3].result()
    tail_ref[...] = tail[4].result()
    store_gx.wait()
    store_out.wait()
    for s in sums:
        s.drain()


def write_out(out_in, gx_in, gwi_in, gwo_in, gqkv_in, gwd_in, tail_in,
              out_ref, gx_ref, g1_ref, s1_ref, g2_ref, s2_ref, gqkv_ref, gbqkv_ref, gwd_ref, gbd_ref, gwi_ref, gbi_ref, gwo_ref, gbo_ref):
    out_ref[...] = out_in[...]
    gx_ref[...] = gx_in[...]
    gwi_ref[...] = gwi_in[...]
    gwo_ref[...] = gwo_in[...]
    gwd_ref[...] = gwd_in[...]
    for h in range(NH):
        tile = gqkv_in[:, span(h, LANES)]
        gqkv_ref[:, 0, h, :] = tile[:, :HD]
        gqkv_ref[:, 1, h, :] = tile[:, HD:]
        gqkv_ref[:, 2, h, :] = gqkv_in[:, span(2 * NH + h, HD)]
    for n, ref in enumerate((g1_ref, s1_ref, g2_ref, s2_ref, gbd_ref)):
        ref[...] = tail_in[n, :SLICE]
    gbo_ref[...] = tail_in[n, :SLICE]
    gbi_ref[...] = tail_in[ROW_B_IN, :]
    gbqkv_ref[...] = tail_in[ROW_B_QKV, :3 * SLICE]


def sds(shape, dtype):
    return jax.ShapeDtypeStruct(shape, dtype)


def halving(shape):
    return tuple(pltpu.VMEM((2,) * n + shape, F32) for n in reversed(range(5)))


def vmem(rows, cols, dtype):
    return pltpu.VMEM((rows, cols), dtype)


def solution(mesh):
    grad_axes = ('dp', 'sp')

    def device_step(hidden, grad_out, ln1_gain, ln1_bias, ln2_gain, ln2_bias, w_qkv, b_qkv, w_dense, b_dense, w_in, b_in, w_out, b_out):
        x = hidden.reshape(ROWS, D)
        g = grad_out.reshape(ROWS, D)
        wt = jnp.moveaxis(w_qkv, 0, -1).reshape(QKV, D)
        near = jnp.asarray(angle_table(np.arange(NT)))
        far = jnp.asarray(angle_table(NT * np.arange(SP)))
        dma = pltpu.SemaphoreType.DMA
        whole = pl.BlockSpec(memory_space=pltpu.VMEM)
        in_specs = [whole] * 16
        in_specs[10] = in_specs[12] = pl.BlockSpec(memory_space=pl.ANY)
        block = pltpu.VMEM((NB, SP, NT, 2 * LANES), BF16)
        peer_sems = (dma((NB, len(PEERS))),) * 2
        results = pl.pallas_call(
            layer,
            out_shape=(sds((ROWS, D), BF16), sds((ROWS, D), BF16), sds((SLICE, FF), F32), sds((LANES, D), F32), sds((SLICE, QKV), F32), sds((SLICE, D), F32), sds((SUB, LANES), F32)),
            in_specs=in_specs,
            out_specs=(in_specs[10],) * 2 + (whole,) * 5,
            scratch_shapes=[
                vmem(ROWS, D, BF16), vmem(ROWS, D, BF16), vmem(NT, LANES, F32), vmem(NT, LANES, F32), vmem(NT, LANES, F32), vmem(D, FF, BF16), vmem(FF, D, BF16), vmem(QKV, D, BF16), vmem(ROWS, D, BF16), vmem(ROWS, QKV, BF16), vmem(D, ROWS, BF16), vmem(D, ROWS, BF16),
                block, block, block, vmem(ROWS, D, F32), vmem(ROWS, D, F32), vmem(SUB, FF, F32),
                vmem(2 * LANES, SEQ, BF16), vmem(SEQ, 2 * NT, F32), vmem(SEQ, LANES, F32),
                tuple(halving(shape) for shape in SUM_SHAPES),
                dma((2,)), dma((2,)), peer_sems, peer_sems, dma((8, 4)), dma((8, 4)),
            ],
            compiler_params=pltpu.CompilerParams(vmem_limit_bytes=VMEM_LIMIT, collective_id=0, has_side_effects=True),
            cost_estimate=pl.CostEstimate(flops=56_000_000_000, bytes_accessed=12_000_000, transcendentals=10_000_000),
            name='layer',
        )(x, g, ln1_gain, ln1_bias, ln2_gain, ln2_bias, wt, b_qkv, w_dense, b_dense, w_in, b_in, w_out, b_out, near, far)

        part = sds((SLICE,), F32)
        tokens = sds((ROWS, D), BF16)
        final = list(pl.pallas_call(
            write_out,
            out_shape=(tokens, tokens, part, part, part, part, sds((SLICE, 3, NH, HD), F32), sds((3 * SLICE,), F32), sds((SLICE, D), F32), part,
                       sds((SLICE, FF), F32), sds((LANES,), F32), sds((LANES, D), F32), part),
            in_specs=[whole] * 7,
            out_specs=(whole,) * 14,
            name='write_out',
        )(*results))
        final[0] = final[0].reshape(hidden.shape)
        final[1] = final[1].reshape(hidden.shape)
        final[6] = jnp.swapaxes(final[6], 1, 2)
        return tuple(final)

    tok_spec = P('dp', 'sp', None)
    grad_spec = P(grad_axes)
    return jax.shard_map(device_step, mesh=mesh, in_specs=(tok_spec, tok_spec) + (P(),) * 12, out_specs=(tok_spec, tok_spec) + (grad_spec,) * 12, check_vma=False)
```
